128 devices in a mesh: dp: 128 (over z, y, x, core).
Axes of the slice: x: 4, y: 4, z: 4, core: 2. Of those that a mesh axis runs over, the one named last changes fastest.
Arguments:
- attended: bfloat16 [65536, 1152], P('dp'), may hold values from -24 to 24, as said below
- proj_cot: bfloat16 [65536, 1152], P('dp'), may hold values from -0.00036621094 to 0.00036621094
- timesteps: float32 [256], P('dp'), may hold values from 0 to 1
- embed_cot: bfloat16 [256, 1152], P('dp'), may hold values from -0.015625 to 0.015625
- master_proj: float32 [1327104], P('dp'), may hold values from -0.1875 to 0.1875
- moment_proj: float32 [1327104], P('dp'), may hold values from -0.013671875 to 0.013671875
- second_proj: float32 [1327104], P('dp'), may hold values from 1.8838011e-07 to 3.0140818e-06
- master_embed: float32 [294912], P('dp'), may hold values from -0.375 to 0.375
- moment_embed: float32 [294912], P('dp'), may hold values from -0.02734375 to 0.02734375
- squared_moment_layer: float32 [294912], P('dp'), may hold values from 8.477105e-07 to 1.3563368e-05
- attended_next: bfloat16 [65536, 1152], P('dp'), may hold values from -6 to 6
- timesteps_next: float32 [256], P('dp'), may hold values from 0 to 1
Outputs:
- next_proj: bfloat16 [65536, 1152], P('dp')
- next_embed: bfloat16 [256, 1152], P('dp')
- move_direction_output: float32 [1327104], P('dp')
- step_embed: float32 [294912], P('dp')
- master_proj_new: float32 [1327104], P('dp')
- master_embed_new: float32 [294912], P('dp')
- grad_norm: float32 [], replicated
The draws below stay inside these ranges and needn't reach their ends.
Inputs may be any that keep to these rules, and one draw needn't show every extreme that they name: attended has entries of mean zero whose scale differs between feature columns by up to a factor of 16.
All inputs are finite; a program needn't handle non-finite values.
Results may differ from the reference program's by a relative error of at most 0.0025.
Values may be sent and summed in bfloat16 or wider, within the bound.
A program may use at most 64 MiB of HBM per device.

```python
import math
import jax
import jax.numpy as jnp

MODEL_BREADTH = 1152
WAVE_EMBED_SPAN = 256
IMG_DEV = 2
TOK_DEV = 512
TOKENS = 65536
IMAGES = 256
N_DP = 128


def draw_attended(key, part):
    scale_key = jax.random.fold_in(key, 11)
    value_key = jax.random.fold_in(key, 12)
    log_scale = jax.random.uniform(scale_key, (MODEL_BREADTH,), jnp.float32, math.log(0.25), math.log(4.0))
    column_scale = jnp.exp(log_scale)
    values = jax.random.truncated_normal(value_key, -6.0, 6.0, (TOKENS, MODEL_BREADTH), jnp.float32)
    return (values * column_scale[None, :]).astype(jnp.bfloat16)


def level_of(rng, shape, shards, smallest, high):
    factor_of, own = 1.0, jax.random.fold_in(rng, 6)
    for dim, blocks in shards:
        heights = jnp.exp(jax.random.uniform(jax.random.fold_in(own, dim), (blocks,), jnp.float32, smallest / len(shards), high / len(shards)))
        factor_of = factor_of * jnp.repeat(heights, shape[dim] // blocks).reshape([-1 if axis == dim else 1 for axis in range(len(shape))])
    return factor_of


def centred(rng, dims, scale, reach, split=(), kind=jnp.bfloat16):
    level = level_of(rng, dims, split, -0.22, 0.18) if split else 1.0
    entries = jax.random.normal(rng, dims, jnp.float32) * scale * level
    return jnp.minimum(jnp.maximum(entries, -reach), reach).astype(kind)


def setup_inputs(seed: int = 0) -> dict:
    seeds = jax.random.split(jax.random.key(seed), 13)
    attended = draw_attended(jax.random.fold_in(seeds[12], 71), 0)
    proj_cot = centred(seeds[1], (TOKENS, MODEL_BREADTH), (7.0 / (MODEL_BREADTH * (TOK_DEV * N_DP) ** 0.5)), 0.00036621094, ((0, 128),))
    timesteps = jnp.clip(1.0 * jax.random.uniform(seeds[2], (IMAGES,), jnp.float32) ** level_of(seeds[2], (IMAGES,), ((0, 128),), -0.2, 0.2), 0.0, 1.0)
    embed_cot = centred(seeds[3], (IMAGES, MODEL_BREADTH), (10.0 / (WAVE_EMBED_SPAN * MODEL_BREADTH * IMG_DEV * N_DP) ** 0.5), 0.015625, ((0, 128),))
    master_proj = centred(seeds[4], (MODEL_BREADTH * MODEL_BREADTH,), MODEL_BREADTH ** -0.5, 0.1875, ((0, 128),), jnp.float32)
    moment_proj = centred(seeds[5], (MODEL_BREADTH * MODEL_BREADTH,), (1.0 / MODEL_BREADTH), 0.013671875, ((0, 128),), jnp.float32)
    second_proj = jnp.clip(jnp.exp(math.log(3.014081812580116e-06) - 2.7725887 * jax.random.uniform(seeds[6], (MODEL_BREADTH * MODEL_BREADTH,), jnp.float32) ** level_of(seeds[6], (MODEL_BREADTH * MODEL_BREADTH,), ((0, 128),), -0.2, 0.2)), 1.8838011328625726e-07, 3.014081812580116e-06)
    master_embed = centred(seeds[7], (WAVE_EMBED_SPAN * MODEL_BREADTH,), WAVE_EMBED_SPAN ** -0.5, 0.375, ((0, 128),), jnp.float32)
    moment_embed = centred(seeds[8], (WAVE_EMBED_SPAN * MODEL_BREADTH,), (1.0 / (WAVE_EMBED_SPAN * MODEL_BREADTH) ** 0.5), 0.02734375, ((0, 128),), jnp.float32)
    squared_moment_layer = jnp.clip(jnp.exp(math.log(1.3563368156610522e-05) - 2.7725887 * jax.random.uniform(seeds[9], (WAVE_EMBED_SPAN * MODEL_BREADTH,), jnp.float32) ** level_of(seeds[9], (WAVE_EMBED_SPAN * MODEL_BREADTH,), ((0, 128),), -0.2, 0.2)), 8.477105097881577e-07, 1.3563368156610522e-05)
    attended_next = centred(seeds[10], (TOKENS, MODEL_BREADTH), 1.0, 6.0, ((0, 128),))
    timesteps_next = jnp.clip(1.0 * jax.random.uniform(seeds[11], (IMAGES,), jnp.float32) ** level_of(seeds[11], (IMAGES,), ((0, 128),), -0.2, 0.2), 0.0, 1.0)
    return dict(attended=attended, proj_cot=proj_cot, timesteps=timesteps, embed_cot=embed_cot, master_proj=master_proj, moment_proj=moment_proj, second_proj=second_proj, master_embed=master_embed, moment_embed=moment_embed, squared_moment_layer=squared_moment_layer, attended_next=attended_next, timesteps_next=timesteps_next)


beta_one = 0.9
beta_two = 0.999
step_count = 1000.0
learn_rate = 0.0001
shrink_factor = 0.01
epsilon = 1e-08
max_norm = 1.0

def freq_embed(moments):
    half_width = WAVE_EMBED_SPAN // 2
    ladder = jnp.arange(half_width, dtype=jnp.float32)
    freqs = jnp.exp(-math.log(10000.0) * ladder / half_width)
    phase_values = (moments * 1000.0)[:, None] * freqs[None, :]
    return jnp.concatenate([jnp.cos(phase_values), jnp.sin(phase_values)], axis=1).astype(jnp.bfloat16)

def adamw_update(gradient, clip, master, moment, second):
    scaled = clip * gradient
    first_new = beta_one * moment + (1.0 - beta_one) * scaled
    second_new = beta_two * second + (1.0 - beta_two) * scaled * scaled
    first_hat = first_new / (1.0 - beta_one ** step_count)
    second_hat = second_new / (1.0 - beta_two ** step_count)
    direction = first_hat / (jnp.sqrt(second_hat) + epsilon)
    freshened_values = master - learn_rate * (direction + shrink_factor * master)
    return (direction, freshened_values)

def reference(attended, proj_cot, timesteps, embed_cot, master_proj, moment_proj, second_proj, master_embed, moment_embed, squared_moment_layer, attended_next, timesteps_next):
    grad_proj = jnp.dot(attended.T, proj_cot, preferred_element_type=jnp.float32).reshape(-1)
    freq_now = freq_embed(timesteps)
    grad_embed = jnp.dot(freq_now.T, embed_cot, preferred_element_type=jnp.float32).reshape(-1)
    total = jnp.sum(grad_proj * grad_proj) + jnp.sum(grad_embed * grad_embed)
    grad_norm = jnp.sqrt(total)
    clip = jnp.minimum(jnp.float32(1.0), max_norm / (grad_norm + 1e-06))
    move_direction_output, master_proj_new = adamw_update(grad_proj, clip, master_proj, moment_proj, second_proj)
    step_embed, master_embed_new = adamw_update(grad_embed, clip, master_embed, moment_embed, squared_moment_layer)
    weight_proj = master_proj_new.astype(jnp.bfloat16).reshape(MODEL_BREADTH, MODEL_BREADTH)
    weight_embed = master_embed_new.astype(jnp.bfloat16).reshape(WAVE_EMBED_SPAN, MODEL_BREADTH)
    next_proj = jnp.dot(attended_next, weight_proj, preferred_element_type=jnp.float32).astype(jnp.bfloat16)
    next_embed = jnp.dot(freq_embed(timesteps_next), weight_embed, preferred_element_type=jnp.float32).astype(jnp.bfloat16)
    return (next_proj, next_embed, move_direction_output, step_embed, master_proj_new, master_embed_new, grad_norm)
```

```python
import functools
import math

import jax
import jax.numpy as jnp
from jax import lax
from jax.experimental import pallas as pl
from jax.experimental.pallas import tpu as pltpu
from jax.sharding import Mesh
from jax.sharding import PartitionSpec as P

AXES = ("z", "y", "x", "c")
MESH = pl.DeviceIdType.MESH
F32 = jnp.float32
BF16 = jnp.bfloat16

beta_one = 0.9
beta_two = 0.999
step_count = 1000.0
learn_rate = 0.0001
shrink_factor = 0.01
epsilon = 1e-08
max_norm = 1.0

TILES = 9
MINE = {0: (0, 5), 1: (5, 4)}
UNITS = {
    0: ((0, 0, 2), (1, 2, 2), (2, 4, 1)),
    1: ((0, 0, 1), (1, 1, 1), (2, 2, 2)),
}
EUNIT = {0: (2, 0, 5), 1: (0, 0, 4)}
SLOTS = 5


def adamw_update(gradient, clip, master, moment, second):
    scaled = clip * gradient
    first_new = beta_one * moment + (1.0 - beta_one) * scaled
    second_new = beta_two * second + (1.0 - beta_two) * scaled * scaled
    first_hat = first_new / (1.0 - beta_one**step_count)
    second_hat = second_new / (1.0 - beta_two**step_count)
    direction = first_hat / (jnp.sqrt(second_hat) + epsilon)
    freshened_values = master - learn_rate * (direction + shrink_factor * master)
    return (direction, freshened_values)


def body(core, hbm, vm, outs, sc):
    (att_h, cot_h, nxt_h, mp_h, op_h, sp_h, me_h, oe_h, se_h) = hbm
    (t_now, t_next, ecot) = vm
    (o_np, o_ne, o_dir, o_dire, o_mst, o_mste, o_norm) = outs
    s = sc
    pos = [lax.axis_index(a) for a in AXES]
    other = 1 - core
    first, count = MINE[core]
    ofirst, ocount = MINE[other]
    units = UNITS[core]
    eunit = EUNIT[core]

    def at(axis, d):
        spot = list(pos)
        spot[axis] = lax.rem(pos[axis] + d, 4)
        return spot

    def in_plane(q, a, b):
        i, j = [k for k in range(3) if k != q]
        spot = list(pos)
        spot[i] = lax.rem(pos[i] + a, 4)
        spot[j] = lax.rem(pos[j] + b, 4)
        return spot

    def plane_of(q, spot):
        return [spot[k] for k in range(3) if k != q]

    def cut(q, p):
        index = [slice(None)] * 3
        index[q] = p
        return tuple(index)

    partner = tuple(pos[:3]) + (other,)

    def remote(src, dst, send, recv, spot):
        copy = pltpu.make_async_remote_copy(
            src_ref=src, dst_ref=dst, send_sem=send, recv_sem=recv,
            device_id=tuple(spot), device_id_type=MESH,
        )
        copy.start()

    def got(ref, sem):
        pltpu.make_async_remote_copy(
            src_ref=ref, dst_ref=ref, send_sem=sem, recv_sem=sem,
            device_id=partner, device_id_type=MESH,
        ).wait_recv()

    loads = []
    for k, (src, dst) in enumerate((
        (att_h, s.att), (cot_h, s.cot), (mp_h, s.st.at[core, 0]), (op_h, s.st.at[core, 1]),
        (sp_h, s.st.at[core, 2]), (me_h, s.ste.at[core, 0]), (oe_h, s.ste.at[core, 1]),
        (se_h, s.ste.at[core, 2]), (nxt_h, s.nxt),
    )):
        copy = pltpu.make_async_copy(src, dst, s.load_sem.at[k])
        copy.start()
        loads.append(copy)

    barrier = pltpu.get_barrier_semaphore()
    peers = {}
    for q in range(3):
        for a in range(4):
            for b in range(4):
                if (a, b) != (0, 0):
                    key = [0, 0, 0]
                    i, j = [k for k in range(3) if k != q]
                    key[i], key[j] = a, b
                    peers[tuple(key)] = in_plane(q, a, b)
    everyone = [tuple(p) for _, p in sorted(peers.items())] + [partner]
    for spot in everyone:
        pl.semaphore_signal(barrier, inc=1, device_id=spot, device_id_type=MESH)

    ladder = lax.broadcasted_iota(jnp.int32, (8, 128), 1).astype(F32)
    line = lax.broadcasted_iota(jnp.int32, (8, 128), 0)
    freqs = jnp.exp(-math.log(10000.0) * ladder / 128)
    moments = jnp.where(
        line == 0, t_now[0], jnp.where(line == 1, t_now[1], jnp.where(line == 2, t_next[0], t_next[1]))
    )
    phases = (moments * 1000.0) * freqs
    waves = jnp.concatenate([jnp.cos(phases), jnp.sin(phases)], axis=1).astype(BF16)
    columns = jnp.transpose(waves.astype(F32), (1, 0))

    loads[0].wait()
    s.attT[...] = jnp.transpose(s.att[...], (1, 0))
    loads[1].wait()

    def term(t):
        return jnp.dot(s.attT[...], s.cot[:, t * 128 : t * 128 + 128], preferred_element_type=F32)

    cots = ecot[...].astype(F32)

    def eterm(t):
        c = cots[:, t * 128 : t * 128 + 128]
        return columns[:, 0:1] * c[0:1] + columns[:, 1:2] * c[1:2]

    for j in range(ocount):
        s.psE[j] = eterm(ofirst + j).astype(BF16)
    pl.semaphore_wait(barrier, len(everyone))
    for k, src in enumerate((mp_h, op_h, sp_h)):
        remote(src, s.st.at[core, k], s.dsend.at[k], s.drecv.at[k], partner)
    for k, src in enumerate((me_h, oe_h, se_h)):
        remote(src, s.ste.at[core, k], s.dsend.at[3 + k], s.drecv.at[3 + k], partner)
    remote(s.psE.at[pl.ds(0, ocount)], s.prE.at[pl.ds(0, ocount)], s.dsend.at[6], s.drecv.at[6], partner)
    for j in range(ocount):
        s.ps[j] = term(ofirst + j).astype(BF16)
        remote(s.ps.at[j], s.pr.at[j], s.psend.at[j], s.precv.at[j], partner)
    for j in range(count):
        s.acc[j] = term(first + j)

    x2 = s.x.reshape(SLOTS, 1152, 128)
    xe2 = s.xE.reshape(SLOTS, 256, 128)

    def stage_one(u, x, r1, q, j0, n):
        for d in (1, 2, 3):
            spot = at(q, d)
            remote(
                x.at[(pl.ds(j0, n),) + cut(q, spot[q])],
                r1.at[pl.ds(j0, n), d],
                s.send1.at[u], s.recv1.at[u], spot,
            )
        for j in range(j0, j0 + n):
            r1[j, 0] = x[(j,) + cut(q, pos[q])]

    got(s.prE.at[pl.ds(0, count)], s.drecv.at[6])
    for j in range(count):
        xe2[j] = (eterm(first + j) + s.prE[j].astype(F32)).astype(BF16)
    stage_one(3, s.xE, s.r1E, *eunit)
    for u, (q, j0, n) in enumerate(units):
        for j in range(j0, j0 + n):
            got(s.pr.at[j], s.precv.at[j])
            x2[j] = (s.acc[j] + s.pr[j].astype(F32)).astype(BF16)
        stage_one(u, s.x, s.r1, q, j0, n)

    for k in range(6):
        loads[2 + k].wait()
    for k in range(3):
        got(s.st.at[other, k], s.drecv.at[k])
        got(s.ste.at[other, k], s.drecv.at[3 + k])
    for k in range(3):
        for j in range(count):
            t = first + j
            for half in range(2):
                s.reg[k, j, 9 * half : 9 * half + 9] = s.st[half, k, pl.ds(t, 9, stride=9), :]
                s.regE[k, j, 2 * half : 2 * half + 2] = s.ste[half, k, pl.ds(t, 2, stride=9), :]

    r1v = s.r1.reshape(SLOTS, 4, 288, 128)
    y2 = s.y.reshape(SLOTS, 288, 128)
    r1ve = s.r1E.reshape(SLOTS, 4, 64, 128)
    y2e = s.yE.reshape(SLOTS, 64, 128)

    def stage_two(u, r1, r1v, y, y2, r2, words, q, j0, n):
        got(r1.at[pl.ds(j0, n), pl.ds(1, 3)], s.recv1.at[u])
        for j in range(j0, j0 + n):
            total = r1v[j, 0].astype(F32)
            for d in (1, 2, 3):
                total = total + r1v[j, d].astype(F32)
            y2[j] = total.astype(BF16)
        for a in range(4):
            for b in range(4):
                if (a, b) == (0, 0):
                    continue
                spot = in_plane(q, a, b)
                p1, p2 = plane_of(q, spot)
                remote(
                    y.at[pl.ds(j0, n), p1, p2],
                    r2.at[pl.ds(j0, n), a * 4 + b, pl.ds(0, words)],
                    s.send2.at[u], s.recv2.at[u], spot,
                )
        p1, p2 = plane_of(q, pos)
        for j in range(j0, j0 + n):
            r2[j, 0, 0:words] = y[j, p1, p2]

    stage_two(3, s.r1E, r1ve, s.yE, y2e, s.r2E, 2, *eunit)
    for u, unit in enumerate(units):
        stage_two(u, s.r1, r1v, s.y, y2, s.r2, 9, *unit)

    r2v = s.r2.reshape(SLOTS, 16, 24, 128)
    r2ve = s.r2E.reshape(SLOTS, 16, 8, 128)
    squares = jnp.zeros((24, 128), F32)
    squares_e = jnp.zeros((8, 128), F32)

    q, j0, n = eunit
    got(s.r2E.at[pl.ds(j0, n), pl.ds(1, 15), pl.ds(0, 2)], s.recv2.at[3])
    for j in range(j0, j0 + n):
        total = r2ve[j, 0].astype(F32)
        for k in range(1, 16):
            total = total + r2ve[j, k].astype(F32)
        s.gE[j] = total
        squares_e = squares_e + total * total
    for u, (q, j0, n) in enumerate(units):
        got(s.r2.at[pl.ds(j0, n), pl.ds(1, 15), pl.ds(0, 9)], s.recv2.at[u])
        for j in range(j0, j0 + n):
            total = r2v[j, 0].astype(F32)
            for k in range(1, 16):
                total = total + r2v[j, k].astype(F32)
            s.g[j] = total
            squares = squares + total * total

    rows = lax.broadcasted_iota(jnp.int32, (24, 128), 0)
    rows_e = lax.broadcasted_iota(jnp.int32, (8, 128), 0)
    squares = jnp.sum(jnp.where(rows < 18, squares, 0.0), axis=0, keepdims=True)
    squares = squares + jnp.sum(jnp.where(rows_e < 4, squares_e, 0.0), axis=0, keepdims=True)
    s.na[core] = squares
    remote(s.na.at[core], s.na.at[core], s.nsend.at[0], s.nrecv.at[0], partner)
    got(s.na.at[other], s.nrecv.at[0])
    pz, py, px = pos[:3]
    s.nb[pz, py] = s.na[0] + s.na[1]
    for a in range(4):
        for b in range(4):
            if (a, b) != (0, 0):
                remote(s.nb.at[pz, py], s.nb.at[pz, py], s.nsend.at[1], s.nrecv.at[1], in_plane(2, a, b))
    got(s.nw.at[pl.ds(0, 15)], s.nrecv.at[1])
    total = s.nb[0, 0]
    for k in range(1, 16):
        total = total + s.nb[k // 4, k % 4]
    s.nc[px] = total
    for d in (1, 2, 3):
        remote(s.nc.at[px], s.nc.at[px], s.nsend.at[2], s.nrecv.at[2], at(2, d))
    got(s.nw.at[pl.ds(0, 3)], s.nrecv.at[2])
    total = s.nc[0] + s.nc[1] + s.nc[2] + s.nc[3]
    grad_norm = jnp.sqrt(jnp.sum(total, axis=1, keepdims=True))
    clip = jnp.minimum(jnp.float32(1.0), max_norm / (grad_norm + 1e-06))
    o_norm[...] = jnp.broadcast_to(grad_norm, (1, 128))

    z2 = s.zz.reshape(SLOTS, 24, 128)
    z2e = s.zE.reshape(SLOTS, 8, 128)

    def update(u, g, reg, zz, z2, dirs, v, words, q, j0, n):
        for j in range(j0, j0 + n):
            direction, fresh = adamw_update(g[j], clip, reg[0, j], reg[1, j], reg[2, j])
            dirs[0, j] = direction
            dirs[1, j] = fresh
            z2[j] = fresh.astype(BF16)
        p1, p2 = plane_of(q, pos)
        for a in range(4):
            for b in range(4):
                if (a, b) == (0, 0):
                    continue
                remote(
                    zz.at[pl.ds(j0, n), pl.ds(0, words)],
                    v.at[pl.ds(j0, n), p1, p2],
                    s.send3.at[u], s.recv3.at[u], in_plane(q, a, b),
                )
        for j in range(j0, j0 + n):
            v[j, p1, p2] = zz[j, 0:words]

    for u, unit in enumerate(units):
        update(u, s.g, s.reg, s.zz, z2, s.dirs, s.v, 9, *unit)
    update(3, s.gE, s.regE, s.zE, z2e, s.dirsE, s.vE, 2, *eunit)

    for k in range(2):
        for j in range(count):
            s.os[k, j, 0:9] = s.dirs[k, j, 9 * other : 9 * other + 9]
            s.osE[k, j, 0:2] = s.dirsE[k, j, 2 * other : 2 * other + 2]
    remote(s.os, s.orr, s.dsend.at[7], s.drecv.at[7], partner)
    remote(s.osE, s.orrE, s.dsend.at[8], s.drecv.at[8], partner)
    for k, (out, oute) in enumerate(((o_dir, o_dire), (o_mst, o_mste))):
        for j in range(count):
            out[pl.ds(first + j, 9, stride=9), :] = s.dirs[k, j, 9 * core : 9 * core + 9]
            oute[pl.ds(first + j, 2, stride=9), :] = s.dirsE[k, j, 2 * core : 2 * core + 2]

    def ring(u, r2, v, w, words, q, j0, n):
        got(r2.at[pl.ds(j0, n), pl.ds(1, 15), pl.ds(0, words)], s.recv3.at[u])
        for d in (1, 2, 3):
            remote(
                v.at[pl.ds(j0, n)],
                w.at[(pl.ds(first + j0, n),) + cut(q, pos[q])],
                s.send4.at[u], s.recv4.at[u], at(q, d),
            )
        for j in range(j0, j0 + n):
            w[(first + j,) + cut(q, pos[q])] = v[j]

    for u, unit in enumerate(units):
        ring(u, s.r2, s.v, s.w, 9, *unit)
    ring(3, s.r2E, s.vE, s.wE, 2, *eunit)

    got(s.orr, s.drecv.at[7])
    got(s.orrE, s.drecv.at[8])
    for k, (out, oute) in enumerate(((o_dir, o_dire), (o_mst, o_mste))):
        for j in range(ocount):
            out[pl.ds(ofirst + j, 9, stride=9), :] = s.orr[k, j, 0:9]
            oute[pl.ds(ofirst + j, 2, stride=9), :] = s.orrE[k, j, 0:2]

    loads[8].wait()
    w2 = s.w.reshape(TILES, 1152, 128)
    we2 = s.wE.reshape(TILES, 256, 128)

    def product(t):
        o_np[:, t * 128 : t * 128 + 128] = jnp.dot(
            s.nxt[...], w2[t], preferred_element_type=F32
        ).astype(BF16)

    for u, (q, j0, n) in enumerate(units):
        got(s.r1.at[pl.ds(j0, n), pl.ds(1, 3)], s.recv4.at[u])
        whole = s.w.at[pl.ds(first + j0, n)]
        remote(whole, whole, s.send5.at[u], s.recv5.at[u], partner)
        for j in range(j0, j0 + n):
            product(first + j)
    q, j0, n = eunit
    got(s.r1E.at[pl.ds(j0, n), pl.ds(1, 3)], s.recv4.at[3])
    whole = s.wE.at[pl.ds(first, count)]
    remote(whole, whole, s.send5.at[3], s.recv5.at[3], partner)
    for u, (q, j0, n) in enumerate(UNITS[other]):
        got(s.w.at[pl.ds(ofirst + j0, n)], s.recv5.at[u])
        for j in range(j0, j0 + n):
            product(ofirst + j)
    got(s.wE.at[pl.ds(ofirst, ocount)], s.recv5.at[3])
    for t in range(TILES):
        mixed = jnp.dot(waves, we2[t], preferred_element_type=F32)
        o_ne[:, t * 128 : t * 128 + 128] = mixed[2:4].astype(BF16)

    def sent(ref, sem):
        pltpu.make_async_remote_copy(
            src_ref=ref, dst_ref=ref, send_sem=sem, recv_sem=sem,
            device_id=partner, device_id_type=MESH,
        ).wait_send()

    for k in range(3):
        sent(s.st.at[core, k], s.dsend.at[k])
        sent(s.ste.at[core, k], s.dsend.at[3 + k])
    sent(s.psE.at[pl.ds(0, ocount)], s.dsend.at[6])
    sent(s.os, s.dsend.at[7])
    sent(s.osE, s.dsend.at[8])
    for j in range(ocount):
        sent(s.ps.at[j], s.psend.at[j])
    sent(s.na.at[core], s.nsend.at[0])
    sent(s.nw.at[pl.ds(0, 15)], s.nsend.at[1])
    sent(s.nw.at[pl.ds(0, 3)], s.nsend.at[2])
    for u, (q, j0, n) in enumerate(units):
        sent(s.r1.at[pl.ds(j0, n), pl.ds(1, 3)], s.send1.at[u])
        sent(s.r2.at[pl.ds(j0, n), pl.ds(1, 15), pl.ds(0, 9)], s.send2.at[u])
        sent(s.r2.at[pl.ds(j0, n), pl.ds(1, 15), pl.ds(0, 9)], s.send3.at[u])
        sent(s.r1.at[pl.ds(j0, n), pl.ds(1, 3)], s.send4.at[u])
        sent(s.w.at[pl.ds(first + j0, n)], s.send5.at[u])
    q, j0, n = eunit
    sent(s.r1E.at[pl.ds(j0, n), pl.ds(1, 3)], s.send1.at[3])
    sent(s.r2E.at[pl.ds(j0, n), pl.ds(1, 15), pl.ds(0, 2)], s.send2.at[3])
    sent(s.r2E.at[pl.ds(j0, n), pl.ds(1, 15), pl.ds(0, 2)], s.send3.at[3])
    sent(s.r1E.at[pl.ds(j0, n), pl.ds(1, 3)], s.send4.at[3])
    sent(s.wE.at[pl.ds(first, count)], s.send5.at[3])


class Names:
    pass


DMA = pltpu.SemaphoreType.DMA
SCRATCH = dict(
    att=pltpu.VMEM((512, 1152), BF16),
    cot=pltpu.VMEM((512, 1152), BF16),
    nxt=pltpu.VMEM((512, 1152), BF16),
    attT=pltpu.VMEM((1152, 512), BF16),
    st=pltpu.VMEM((2, 3, 81, 128), F32),
    ste=pltpu.VMEM((2, 3, 18, 128), F32),
    ps=pltpu.VMEM((SLOTS, 1152, 128), BF16),
    pr=pltpu.VMEM((SLOTS, 1152, 128), BF16),
    psE=pltpu.VMEM((SLOTS, 256, 128), BF16),
    prE=pltpu.VMEM((SLOTS, 256, 128), BF16),
    acc=pltpu.VMEM((SLOTS, 1152, 128), F32),
    x=pltpu.VMEM((SLOTS, 4, 4, 4, 9, 2, 128), BF16),
    xE=pltpu.VMEM((SLOTS, 4, 4, 4, 2, 2, 128), BF16),
    r1=pltpu.VMEM((SLOTS, 4, 4, 4, 9, 2, 128), BF16),
    r1E=pltpu.VMEM((SLOTS, 4, 4, 4, 2, 2, 128), BF16),
    y=pltpu.VMEM((SLOTS, 4, 4, 9, 2, 128), BF16),
    yE=pltpu.VMEM((SLOTS, 4, 4, 2, 2, 128), BF16),
    r2=pltpu.VMEM((SLOTS, 16, 12, 2, 128), BF16),
    r2E=pltpu.VMEM((SLOTS, 16, 4, 2, 128), BF16),
    reg=pltpu.VMEM((3, SLOTS, 24, 128), F32),
    regE=pltpu.VMEM((3, SLOTS, 8, 128), F32),
    g=pltpu.VMEM((SLOTS, 24, 128), F32),
    gE=pltpu.VMEM((SLOTS, 8, 128), F32),
    dirs=pltpu.VMEM((2, SLOTS, 24, 128), F32),
    dirsE=pltpu.VMEM((2, SLOTS, 8, 128), F32),
    zz=pltpu.VMEM((SLOTS, 12, 2, 128), BF16),
    zE=pltpu.VMEM((SLOTS, 4, 2, 128), BF16),
    v=pltpu.VMEM((SLOTS, 4, 4, 9, 2, 128), BF16),
    vE=pltpu.VMEM((SLOTS, 4, 4, 2, 2, 128), BF16),
    w=pltpu.VMEM((TILES, 4, 4, 4, 9, 2, 128), BF16),
    wE=pltpu.VMEM((TILES, 4, 4, 4, 2, 2, 128), BF16),
    os=pltpu.VMEM((2, SLOTS, 16, 128), F32),
    osE=pltpu.VMEM((2, SLOTS, 8, 128), F32),
    orr=pltpu.VMEM((2, SLOTS, 16, 128), F32),
    orrE=pltpu.VMEM((2, SLOTS, 8, 128), F32),
    na=pltpu.VMEM((2, 1, 128), F32),
    nb=pltpu.VMEM((4, 4, 1, 128), F32),
    nc=pltpu.VMEM((4, 1, 128), F32),
    nw=pltpu.VMEM((15, 1, 128), F32),
    load_sem=DMA((9,)),
    dsend=DMA((9,)),
    drecv=DMA((9,)),
    psend=DMA((SLOTS,)),
    precv=DMA((SLOTS,)),
    send1=DMA((4,)),
    recv1=DMA((4,)),
    send2=DMA((4,)),
    recv2=DMA((4,)),
    send3=DMA((4,)),
    recv3=DMA((4,)),
    send4=DMA((4,)),
    recv4=DMA((4,)),
    send5=DMA((4,)),
    recv5=DMA((4,)),
    nsend=DMA((3,)),
    nrecv=DMA((3,)),
)


def kernel(*refs):
    hbm, vm, outs, scratch = refs[:9], refs[9:12], refs[12:19], refs[19:]
    s = Names()
    for name, ref in zip(SCRATCH, scratch, strict=True):
        setattr(s, name, ref)
    core = lax.axis_index("c")
    for k in (0, 1):

        @pl.when(core == k)
        def _():
            body(k, hbm, vm, outs, s)


def shards(
    attended, proj_cot, timesteps, embed_cot, master_proj, moment_proj, second_proj,
    master_embed, moment_embed, squared_moment_layer, attended_next, timesteps_next,
):
    flat = [a.reshape(-1, 128) for a in (master_proj, moment_proj, second_proj)]
    flat_e = [a.reshape(-1, 128) for a in (master_embed, moment_embed, squared_moment_layer)]
    anywhere = pl.BlockSpec(memory_space=pl.ANY)
    smem = pl.BlockSpec(memory_space=pltpu.SMEM)
    vmem = pl.BlockSpec(memory_space=pltpu.VMEM)
    shape = jax.ShapeDtypeStruct
    nproj, nembed, d, de, m, mste, norm = pl.pallas_call(
        kernel,
        out_shape=(
            shape((512, 1152), BF16), shape((2, 1152), BF16), shape((81, 128), F32),
            shape((18, 128), F32), shape((81, 128), F32), shape((18, 128), F32), shape((1, 128), F32),
        ),
        in_specs=[anywhere] * 9 + [smem, smem, vmem],
        out_specs=[vmem] * 7,
        scratch_shapes=list(SCRATCH.values()),
        compiler_params=pltpu.CompilerParams(
            collective_id=0, has_side_effects=True, vmem_limit_bytes=48 * 2**20
        ),
    )(attended, proj_cot, attended_next, *flat, *flat_e, timesteps, timesteps_next, embed_cot)
    return (
        nproj, nembed, d.reshape(-1), de.reshape(-1), m.reshape(-1), mste.reshape(-1), norm[0, 0],
    )


def solution(mesh):
    finer = Mesh(mesh.devices.reshape(4, 4, 4, 2), AXES)
    dp = P(AXES)
    wide = P(AXES, None)
    return jax.shard_map(
        shards,
        mesh=finer,
        in_specs=(wide, wide, dp, wide, dp, dp, dp, dp, dp, dp, wide, dp),
        out_specs=(wide, wide, dp, dp, dp, dp, P()),
        check_vma=False,
    )
```

```python
import functools
import math

import jax
import jax.numpy as jnp
from jax import lax
from jax.experimental import pallas as pl
from jax.experimental.pallas import tpu as pltpu
from jax.sharding import Mesh
from jax.sharding import PartitionSpec as P

AXES = ("z", "y", "x", "c")
MESH = pl.DeviceIdType.MESH
F32 = jnp.float32
BF16 = jnp.bfloat16

beta_one = 0.9
beta_two = 0.999
step_count = 1000.0
learn_rate = 0.0001
shrink_factor = 0.01
epsilon = 1e-08
max_norm = 1.0

TILES = 9
MINE = {0: (0, 5), 1: (5, 4)}
UNITS = {
    0: ((0, 0, 2), (1, 2, 2), (2, 4, 1)),
    1: ((0, 0, 1), (1, 1, 1), (2, 2, 2)),
}
EUNIT = {0: (2, 0, 5), 1: (0, 0, 4)}
SLOTS = 5
PHASES = False


def adamw_update(gradient, clip, master, moment, second):
    scaled = clip * gradient
    first_new = beta_one * moment + (1.0 - beta_one) * scaled
    second_new = beta_two * second + (1.0 - beta_two) * scaled * scaled
    first_hat = first_new / (1.0 - beta_one**step_count)
    second_hat = second_new / (1.0 - beta_two**step_count)
    direction = first_hat / (jnp.sqrt(second_hat) + epsilon)
    freshened_values = master - learn_rate * (direction + shrink_factor * master)
    return (direction, freshened_values)


def body(core, hbm, outs, sc):
    (att_h, cot_h, nxt_h, mp_h, op_h, sp_h, me_h, oe_h, se_h, tn_h, tx_h, ec_h) = hbm
    (o_np, o_ne, o_dir, o_dire, o_mst, o_mste, o_norm) = outs
    s = sc
    pos = [lax.axis_index(a) for a in AXES]
    other = 1 - core
    first, count = MINE[core]
    ofirst, ocount = MINE[other]
    units = UNITS[core]
    eunit = EUNIT[core]

    def at(axis, d):
        spot = list(pos)
        spot[axis] = lax.rem(pos[axis] + d, 4)
        return spot

    def in_plane(q, a, b):
        i, j = [k for k in range(3) if k != q]
        spot = list(pos)
        spot[i] = lax.rem(pos[i] + a, 4)
        spot[j] = lax.rem(pos[j] + b, 4)
        return spot

    def plane_of(q, spot):
        return [spot[k] for k in range(3) if k != q]

    def cut(q, p):
        index = [slice(None)] * 3
        index[q] = p
        return tuple(index)

    partner = tuple(pos[:3]) + (other,)

    def remote(src, dst, send, recv, spot):
        copy = pltpu.make_async_remote_copy(
            src_ref=src, dst_ref=dst, send_sem=send, recv_sem=recv,
            device_id=tuple(spot), device_id_type=MESH,
        )
        copy.start()

    def got(ref, sem):
        pltpu.make_async_remote_copy(
            src_ref=ref, dst_ref=ref, send_sem=sem, recv_sem=sem,
            device_id=partner, device_id_type=MESH,
        ).wait_recv()

    phase = Phase()
    phase("start")
    loads = []
    for k, (src, dst) in enumerate((
        (att_h, s.att), (cot_h, s.cot), (mp_h, s.st.at[core, 0]), (op_h, s.st.at[core, 1]),
        (sp_h, s.st.at[core, 2]), (me_h, s.ste.at[core, 0]), (oe_h, s.ste.at[core, 1]),
        (se_h, s.ste.at[core, 2]), (nxt_h, s.nxt), (tn_h, s.now), (tx_h, s.later), (ec_h, s.ecot),
    )):
        copy = pltpu.make_async_copy(src, dst, s.load_sem.at[k])
        copy.start()
        loads.append(copy)

    phase("signal")
    barrier = pltpu.get_barrier_semaphore()
    peers = {}
    for q in range(3):
        for a in range(4):
            for b in range(4):
                if (a, b) != (0, 0):
                    key = [0, 0, 0]
                    i, j = [k for k in range(3) if k != q]
                    key[i], key[j] = a, b
                    peers[tuple(key)] = in_plane(q, a, b)
    everyone = [tuple(p) for _, p in sorted(peers.items())] + [partner]
    for spot in everyone:
        pl.semaphore_signal(barrier, inc=1, device_id=spot, device_id_type=MESH)

    phase("freqs")
    for k in (9, 10, 11):
        loads[k].wait()
    t_now, t_next, ecot = s.now, s.later, s.ecot
    ladder = lax.broadcasted_iota(jnp.int32, (8, 128), 1).astype(F32)
    line = lax.broadcasted_iota(jnp.int32, (8, 128), 0)
    freqs = jnp.exp(-math.log(10000.0) * ladder / 128)
    moments = jnp.where(
        line == 0, t_now[0], jnp.where(line == 1, t_now[1], jnp.where(line == 2, t_next[0], t_next[1]))
    )
    phases = (moments * 1000.0) * freqs
    waves = jnp.concatenate([jnp.cos(phases), jnp.sin(phases)], axis=1).astype(BF16)
    columns = jnp.transpose(waves.astype(F32), (1, 0))

    phase("transpose")
    loads[0].wait()
    s.attT[...] = jnp.transpose(s.att[...], (1, 0))
    loads[1].wait()

    phase("eterms")
    def term(t):
        return jnp.dot(s.attT[...], s.cot[:, t * 128 : t * 128 + 128], preferred_element_type=F32)

    cots = ecot[...].astype(F32)

    def eterm(t):
        c = cots[:, t * 128 : t * 128 + 128]
        return columns[:, 0:1] * c[0:1] + columns[:, 1:2] * c[1:2]

    for j in range(ocount):
        s.psE[j] = eterm(ofirst + j).astype(BF16)
    phase("barrier")
    pl.semaphore_wait(barrier, len(everyone))
    phase("partner_terms")
    for k, src in enumerate((mp_h, op_h, sp_h)):
        remote(src, s.st.at[core, k], s.dsend.at[k], s.drecv.at[k], partner)
    for k, src in enumerate((me_h, oe_h, se_h)):
        remote(src, s.ste.at[core, k], s.dsend.at[3 + k], s.drecv.at[3 + k], partner)
    remote(s.psE.at[pl.ds(0, ocount)], s.prE.at[pl.ds(0, ocount)], s.dsend.at[6], s.drecv.at[6], partner)
    for j in range(ocount):
        s.ps[j] = term(ofirst + j).astype(BF16)
        remote(s.ps.at[j], s.pr.at[j], s.psend.at[j], s.precv.at[j], partner)
    phase("own_terms")
    for j in range(count):
        s.acc[j] = term(first + j)

    x2 = s.x.reshape(SLOTS, 1152, 128)
    xe2 = s.xE.reshape(SLOTS, 256, 128)

    def stage_one(u, x, r1, q, j0, n):
        for d in (1, 2, 3):
            spot = at(q, d)
            remote(
                x.at[(pl.ds(j0, n),) + cut(q, spot[q])],
                r1.at[pl.ds(j0, n), d],
                s.send1.at[u], s.recv1.at[u], spot,
            )
        for j in range(j0, j0 + n):
            r1[j, 0] = x[(j,) + cut(q, pos[q])]

    phase("chip_e")
    got(s.prE.at[pl.ds(0, count)], s.drecv.at[6])
    for j in range(count):
        xe2[j] = (eterm(first + j) + s.prE[j].astype(F32)).astype(BF16)
    stage_one(3, s.xE, s.r1E, *eunit)
    for u, (q, j0, n) in enumerate(units):
        phase(f"chip{u}")
        for j in range(j0, j0 + n):
            got(s.pr.at[j], s.precv.at[j])
            x2[j] = (s.acc[j] + s.pr[j].astype(F32)).astype(BF16)
        stage_one(u, s.x, s.r1, q, j0, n)

    phase("state")
    for k in range(6):
        loads[2 + k].wait()
    for k in range(3):
        got(s.st.at[other, k], s.drecv.at[k])
        got(s.ste.at[other, k], s.drecv.at[3 + k])
    for k in range(3):
        for j in range(count):
            t = first + j
            for half in range(2):
                s.reg[k, j, 9 * half : 9 * half + 9] = s.st[half, k, pl.ds(t, 9, stride=9), :]
                s.regE[k, j, 2 * half : 2 * half + 2] = s.ste[half, k, pl.ds(t, 2, stride=9), :]

    r1v = s.r1.reshape(SLOTS, 4, 288, 128)
    y2 = s.y.reshape(SLOTS, 288, 128)
    r1ve = s.r1E.reshape(SLOTS, 4, 64, 128)
    y2e = s.yE.reshape(SLOTS, 64, 128)

    def stage_two(u, r1, r1v, y, y2, r2, words, q, j0, n):
        got(r1.at[pl.ds(j0, n), pl.ds(1, 3)], s.recv1.at[u])
        for j in range(j0, j0 + n):
            total = r1v[j, 0].astype(F32)
            for d in (1, 2, 3):
                total = total + r1v[j, d].astype(F32)
            y2[j] = total.astype(BF16)
        for a in range(4):
            for b in range(4):
                if (a, b) == (0, 0):
                    continue
                spot = in_plane(q, a, b)
                p1, p2 = plane_of(q, spot)
                remote(
                    y.at[pl.ds(j0, n), p1, p2],
                    r2.at[pl.ds(j0, n), a * 4 + b, pl.ds(0, words)],
                    s.send2.at[u], s.recv2.at[u], spot,
                )
        p1, p2 = plane_of(q, pos)
        for j in range(j0, j0 + n):
            r2[j, 0, 0:words] = y[j, p1, p2]

    phase("two_e")
    stage_two(3, s.r1E, r1ve, s.yE, y2e, s.r2E, 2, *eunit)
    for u, unit in enumerate(units):
        phase(f"two{u}")
        stage_two(u, s.r1, r1v, s.y, y2, s.r2, 9, *unit)

    r2v = s.r2.reshape(SLOTS, 16, 24, 128)
    r2ve = s.r2E.reshape(SLOTS, 16, 8, 128)
    squares = jnp.zeros((24, 128), F32)
    squares_e = jnp.zeros((8, 128), F32)

    phase("sum_e")
    q, j0, n = eunit
    got(s.r2E.at[pl.ds(j0, n), pl.ds(1, 15), pl.ds(0, 2)], s.recv2.at[3])
    for j in range(j0, j0 + n):
        total = r2ve[j, 0].astype(F32)
        for k in range(1, 16):
            total = total + r2ve[j, k].astype(F32)
        s.gE[j] = total
        squares_e = squares_e + total * total
    for u, (q, j0, n) in enumerate(units):
        phase(f"sum{u}")
        got(s.r2.at[pl.ds(j0, n), pl.ds(1, 15), pl.ds(0, 9)], s.recv2.at[u])
        for j in range(j0, j0 + n):
            total = r2v[j, 0].astype(F32)
            for k in range(1, 16):
                total = total + r2v[j, k].astype(F32)
            s.g[j] = total
            squares = squares + total * total

    phase("squares")
    rows = lax.broadcasted_iota(jnp.int32, (24, 128), 0)
    rows_e = lax.broadcasted_iota(jnp.int32, (8, 128), 0)
    squares = jnp.sum(jnp.where(rows < 18, squares, 0.0), axis=0, keepdims=True)
    squares = squares + jnp.sum(jnp.where(rows_e < 4, squares_e, 0.0), axis=0, keepdims=True)
    s.na[core] = squares
    remote(s.na.at[core], s.na.at[core], s.nsend.at[0], s.nrecv.at[0], partner)
    phase("norm_a")
    got(s.na.at[other], s.nrecv.at[0])
    pz, py, px = pos[:3]
    s.nb[pz, py] = s.na[0] + s.na[1]
    for a in range(4):
        for b in range(4):
            if (a, b) != (0, 0):
                remote(s.nb.at[pz, py], s.nb.at[pz, py], s.nsend.at[1], s.nrecv.at[1], in_plane(2, a, b))
    phase("norm_b")
    got(s.nw.at[pl.ds(0, 15)], s.nrecv.at[1])
    total = s.nb[0, 0]
    for k in range(1, 16):
        total = total + s.nb[k // 4, k % 4]
    s.nc[px] = total
    for d in (1, 2, 3):
        remote(s.nc.at[px], s.nc.at[px], s.nsend.at[2], s.nrecv.at[2], at(2, d))
    phase("norm_c")
    got(s.nw.at[pl.ds(0, 3)], s.nrecv.at[2])
    total = s.nc[0] + s.nc[1] + s.nc[2] + s.nc[3]
    grad_norm = jnp.sqrt(jnp.sum(total, axis=1, keepdims=True))
    clip = jnp.minimum(jnp.float32(1.0), max_norm / (grad_norm + 1e-06))
    o_norm[...] = jnp.broadcast_to(grad_norm, (1, 128))

    z2 = s.zz.reshape(SLOTS, 24, 128)
    z2e = s.zE.reshape(SLOTS, 8, 128)

    def update(u, g, reg, zz, z2, dirs, v, words, q, j0, n):
        for j in range(j0, j0 + n):
            direction, fresh = adamw_update(g[j], clip, reg[0, j], reg[1, j], reg[2, j])
            dirs[0, j] = direction
            dirs[1, j] = fresh
            z2[j] = fresh.astype(BF16)
        p1, p2 = plane_of(q, pos)
        for a in range(4):
            for b in range(4):
                if (a, b) == (0, 0):
                    continue
                remote(
                    zz.at[pl.ds(j0, n), pl.ds(0, words)],
                    v.at[pl.ds(j0, n), p1, p2],
                    s.send3.at[u], s.recv3.at[u], in_plane(q, a, b),
                )
        for j in range(j0, j0 + n):
            v[j, p1, p2] = zz[j, 0:words]

    phase("update")
    for u, unit in enumerate(units):
        update(u, s.g, s.reg, s.zz, z2, s.dirs, s.v, 9, *unit)
    update(3, s.gE, s.regE, s.zE, z2e, s.dirsE, s.vE, 2, *eunit)

    phase("outs")
    for k in range(2):
        for j in range(count):
            s.os[k, j, 0:9] = s.dirs[k, j, 9 * other : 9 * other + 9]
            s.osE[k, j, 0:2] = s.dirsE[k, j, 2 * other : 2 * other + 2]
    remote(s.os, s.orr, s.dsend.at[7], s.drecv.at[7], partner)
    remote(s.osE, s.orrE, s.dsend.at[8], s.drecv.at[8], partner)
    for k, (out, oute) in enumerate(((o_dir, o_dire), (o_mst, o_mste))):
        for j in range(count):
            out[pl.ds(first + j, 9, stride=9), :] = s.dirs[k, j, 9 * core : 9 * core + 9]
            oute[pl.ds(first + j, 2, stride=9), :] = s.dirsE[k, j, 2 * core : 2 * core + 2]

    def ring(u, r2, v, w, words, q, j0, n):
        got(r2.at[pl.ds(j0, n), pl.ds(1, 15), pl.ds(0, words)], s.recv3.at[u])
        for d in (1, 2, 3):
            remote(
                v.at[pl.ds(j0, n)],
                w.at[(pl.ds(first + j0, n),) + cut(q, pos[q])],
                s.send4.at[u], s.recv4.at[u], at(q, d),
            )
        for j in range(j0, j0 + n):
            w[(first + j,) + cut(q, pos[q])] = v[j]

    for u, unit in enumerate(units):
        phase(f"ring{u}")
        ring(u, s.r2, s.v, s.w, 9, *unit)
    phase("ring_e")
    ring(3, s.r2E, s.vE, s.wE, 2, *eunit)

    phase("outs2")
    got(s.orr, s.drecv.at[7])
    got(s.orrE, s.drecv.at[8])
    for k, (out, oute) in enumerate(((o_dir, o_dire), (o_mst, o_mste))):
        for j in range(ocount):
            out[pl.ds(ofirst + j, 9, stride=9), :] = s.orr[k, j, 0:9]
            oute[pl.ds(ofirst + j, 2, stride=9), :] = s.orrE[k, j, 0:2]

    loads[8].wait()
    w2 = s.w.reshape(TILES, 1152, 128)
    we2 = s.wE.reshape(TILES, 256, 128)

    def product(t):
        o_np[:, t * 128 : t * 128 + 128] = jnp.dot(
            s.nxt[...], w2[t], preferred_element_type=F32
        ).astype(BF16)

    for u, (q, j0, n) in enumerate(units):
        phase(f"own{u}")
        got(s.r1.at[pl.ds(j0, n), pl.ds(1, 3)], s.recv4.at[u])
        whole = s.w.at[pl.ds(first + j0, n)]
        remote(whole, whole, s.send5.at[u], s.recv5.at[u], partner)
        for j in range(j0, j0 + n):
            product(first + j)
    phase("own_e")
    q, j0, n = eunit
    got(s.r1E.at[pl.ds(j0, n), pl.ds(1, 3)], s.recv4.at[3])
    whole = s.wE.at[pl.ds(first, count)]
    remote(whole, whole, s.send5.at[3], s.recv5.at[3], partner)
    for u, (q, j0, n) in enumerate(UNITS[other]):
        phase(f"theirs{u}")
        got(s.w.at[pl.ds(ofirst + j0, n)], s.recv5.at[u])
        for j in range(j0, j0 + n):
            product(ofirst + j)
    phase("last_e")
    got(s.wE.at[pl.ds(ofirst, ocount)], s.recv5.at[3])
    for t in range(TILES):
        mixed = jnp.dot(waves, we2[t], preferred_element_type=F32)
        o_ne[:, t * 128 : t * 128 + 128] = mixed[2:4].astype(BF16)

    phase("drain")
    def sent(ref, sem):
        pltpu.make_async_remote_copy(
            src_ref=ref, dst_ref=ref, send_sem=sem, recv_sem=sem,
            device_id=partner, device_id_type=MESH,
        ).wait_send()

    for k in range(3):
        sent(s.st.at[core, k], s.dsend.at[k])
        sent(s.ste.at[core, k], s.dsend.at[3 + k])
    sent(s.psE.at[pl.ds(0, ocount)], s.dsend.at[6])
    sent(s.os, s.dsend.at[7])
    sent(s.osE, s.dsend.at[8])
    for j in range(ocount):
        sent(s.ps.at[j], s.psend.at[j])
    sent(s.na.at[core], s.nsend.at[0])
    sent(s.nw.at[pl.ds(0, 15)], s.nsend.at[1])
    sent(s.nw.at[pl.ds(0, 3)], s.nsend.at[2])
    for u, (q, j0, n) in enumerate(units):
        sent(s.r1.at[pl.ds(j0, n), pl.ds(1, 3)], s.send1.at[u])
        sent(s.r2.at[pl.ds(j0, n), pl.ds(1, 15), pl.ds(0, 9)], s.send2.at[u])
        sent(s.r2.at[pl.ds(j0, n), pl.ds(1, 15), pl.ds(0, 9)], s.send3.at[u])
        sent(s.r1.at[pl.ds(j0, n), pl.ds(1, 3)], s.send4.at[u])
        sent(s.w.at[pl.ds(first + j0, n)], s.send5.at[u])
    q, j0, n = eunit
    sent(s.r1E.at[pl.ds(j0, n), pl.ds(1, 3)], s.send1.at[3])
    sent(s.r2E.at[pl.ds(j0, n), pl.ds(1, 15), pl.ds(0, 2)], s.send2.at[3])
    sent(s.r2E.at[pl.ds(j0, n), pl.ds(1, 15), pl.ds(0, 2)], s.send3.at[3])
    sent(s.r1E.at[pl.ds(j0, n), pl.ds(1, 3)], s.send4.at[3])
    sent(s.wE.at[pl.ds(first, count)], s.send5.at[3])
    phase(None)


class Names:
    pass


class Phase:
    def __init__(self):
        self.open = None

    def __call__(self, name):
        if self.open is not None:
            self.open.__exit__(None, None, None)
            self.open = None
        if name is not None and PHASES:
            self.open = jax.named_scope(name)
            self.open.__enter__()


DMA = pltpu.SemaphoreType.DMA
SCRATCH = dict(
    att=pltpu.VMEM((512, 1152), BF16),
    cot=pltpu.VMEM((512, 1152), BF16),
    nxt=pltpu.VMEM((512, 1152), BF16),
    ecot=pltpu.VMEM((2, 1152), BF16),
    now=pltpu.SMEM((2,), F32),
    later=pltpu.SMEM((2,), F32),
    attT=pltpu.VMEM((1152, 512), BF16),
    st=pltpu.VMEM((2, 3, 81, 128), F32),
    ste=pltpu.VMEM((2, 3, 18, 128), F32),
    ps=pltpu.VMEM((SLOTS, 1152, 128), BF16),
    pr=pltpu.VMEM((SLOTS, 1152, 128), BF16),
    psE=pltpu.VMEM((SLOTS, 256, 128), BF16),
    prE=pltpu.VMEM((SLOTS, 256, 128), BF16),
    acc=pltpu.VMEM((SLOTS, 1152, 128), F32),
    x=pltpu.VMEM((SLOTS, 4, 4, 4, 9, 2, 128), BF16),
    xE=pltpu.VMEM((SLOTS, 4, 4, 4, 2, 2, 128), BF16),
    r1=pltpu.VMEM((SLOTS, 4, 4, 4, 9, 2, 128), BF16),
    r1E=pltpu.VMEM((SLOTS, 4, 4, 4, 2, 2, 128), BF16),
    y=pltpu.VMEM((SLOTS, 4, 4, 9, 2, 128), BF16),
    yE=pltpu.VMEM((SLOTS, 4, 4, 2, 2, 128), BF16),
    r2=pltpu.VMEM((SLOTS, 16, 12, 2, 128), BF16),
    r2E=pltpu.VMEM((SLOTS, 16, 4, 2, 128), BF16),
    reg=pltpu.VMEM((3, SLOTS, 24, 128), F32),
    regE=pltpu.VMEM((3, SLOTS, 8, 128), F32),
    g=pltpu.VMEM((SLOTS, 24, 128), F32),
    gE=pltpu.VMEM((SLOTS, 8, 128), F32),
    dirs=pltpu.VMEM((2, SLOTS, 24, 128), F32),
    dirsE=pltpu.VMEM((2, SLOTS, 8, 128), F32),
    zz=pltpu.VMEM((SLOTS, 12, 2, 128), BF16),
    zE=pltpu.VMEM((SLOTS, 4, 2, 128), BF16),
    v=pltpu.VMEM((SLOTS, 4, 4, 9, 2, 128), BF16),
    vE=pltpu.VMEM((SLOTS, 4, 4, 2, 2, 128), BF16),
    w=pltpu.VMEM((TILES, 4, 4, 4, 9, 2, 128), BF16),
    wE=pltpu.VMEM((TILES, 4, 4, 4, 2, 2, 128), BF16),
    os=pltpu.VMEM((2, SLOTS, 16, 128), F32),
    osE=pltpu.VMEM((2, SLOTS, 8, 128), F32),
    orr=pltpu.VMEM((2, SLOTS, 16, 128), F32),
    orrE=pltpu.VMEM((2, SLOTS, 8, 128), F32),
    na=pltpu.VMEM((2, 1, 128), F32),
    nb=pltpu.VMEM((4, 4, 1, 128), F32),
    nc=pltpu.VMEM((4, 1, 128), F32),
    nw=pltpu.VMEM((15, 1, 128), F32),
    load_sem=DMA((12,)),
    dsend=DMA((9,)),
    drecv=DMA((9,)),
    psend=DMA((SLOTS,)),
    precv=DMA((SLOTS,)),
    send1=DMA((4,)),
    recv1=DMA((4,)),
    send2=DMA((4,)),
    recv2=DMA((4,)),
    send3=DMA((4,)),
    recv3=DMA((4,)),
    send4=DMA((4,)),
    recv4=DMA((4,)),
    send5=DMA((4,)),
    recv5=DMA((4,)),
    nsend=DMA((3,)),
    nrecv=DMA((3,)),
)


def kernel(*refs):
    hbm, outs, scratch = refs[:12], refs[12:19], refs[19:]
    s = Names()
    for name, ref in zip(SCRATCH, scratch, strict=True):
        setattr(s, name, ref)
    core = lax.axis_index("c")
    for k in (0, 1):

        @pl.when(core == k)
        def _():
            body(k, hbm, outs, s)


def write_out(*refs):
    sems = refs[14]
    copies = [pltpu.make_async_copy(refs[k], refs[7 + k], sems.at[k]) for k in range(7)]
    for copy in copies:
        copy.start()
    for copy in copies:
        copy.wait()


def shards(
    attended, proj_cot, timesteps, embed_cot, master_proj, moment_proj, second_proj,
    master_embed, moment_embed, squared_moment_layer, attended_next, timesteps_next,
):
    flat = [a.reshape(-1, 128) for a in (master_proj, moment_proj, second_proj)]
    flat_e = [a.reshape(-1, 128) for a in (master_embed, moment_embed, squared_moment_layer)]
    anywhere = pl.BlockSpec(memory_space=pl.ANY)
    large = pl.BlockSpec(memory_space=pltpu.HBM)
    vmem = pl.BlockSpec(memory_space=pltpu.VMEM)
    shape = jax.ShapeDtypeStruct
    results = (
        shape((512, 1152), BF16), shape((2, 1152), BF16), shape((81, 128), F32),
        shape((18, 128), F32), shape((81, 128), F32), shape((18, 128), F32), shape((1, 128), F32),
    )
    inside = pl.pallas_call(
        kernel,
        out_shape=[pltpu.VMEM(r.shape, r.dtype) for r in results],
        in_specs=[large] * 12,
        out_specs=[vmem] * 7,
        scratch_shapes=list(SCRATCH.values()),
        compiler_params=pltpu.CompilerParams(
            collective_id=0, has_side_effects=True, vmem_limit_bytes=60 * 2**20
        ),
        name="step",
    )(attended, proj_cot, attended_next, *flat, *flat_e, timesteps, timesteps_next, embed_cot)
    nproj, nembed, d, de, m, mste, norm = pl.pallas_call(
        write_out,
        out_shape=results,
        in_specs=[vmem] * 7,
        out_specs=[large] * 7,
        scratch_shapes=[DMA((7,))],
        compiler_params=pltpu.CompilerParams(vmem_limit_bytes=8 * 2**20),
        name="write_out",
    )(*inside)
    return (
        nproj, nembed, d.reshape(-1), de.reshape(-1), m.reshape(-1), mste.reshape(-1), norm[0, 0],
    )


def solution(mesh):
    finer = Mesh(mesh.devices.reshape(4, 4, 4, 2), AXES)
    dp = P(AXES)
    wide = P(AXES, None)
    return jax.shard_map(
        shards,
        mesh=finer,
        in_specs=(wide, wide, dp, wide, dp, dp, dp, dp, dp, dp, wide, dp),
        out_specs=(wide, wide, dp, dp, dp, dp, P()),
        check_vma=False,
    )
```

```python
import functools
import math

import jax
import jax.numpy as jnp
from jax import lax
from jax.experimental import pallas as pl
from jax.experimental.pallas import tpu as pltpu
from jax.sharding import Mesh
from jax.sharding import PartitionSpec as P

AXES = ("z", "y", "x", "c")
MESH = pl.DeviceIdType.MESH
F32 = jnp.float32
BF16 = jnp.bfloat16

beta_one = 0.9
beta_two = 0.999
step_count = 1000.0
learn_rate = 0.0001
shrink_factor = 0.01
epsilon = 1e-08
max_norm = 1.0

TILES = 9
MINE = {0: (0, 5), 1: (5, 4)}
UNITS = {
    0: ((0, 0, 1), (1, 1, 1), (2, 2, 1), (0, 3, 1), (1, 4, 1)),
    1: ((0, 0, 1), (1, 1, 1), (2, 2, 1), (2, 3, 1)),
}
E = 5
FAR = [(a, b) for a in (2, 1, 3, 0) for b in (2, 1, 3, 0) if (a, b) != (0, 0)]
EUNIT = {0: (2, 0, 5), 1: (0, 0, 4)}
SLOTS = 5
PHASES = False


def adamw_update(gradient, clip, master, moment, second):
    scaled = clip * gradient
    first_new = beta_one * moment + (1.0 - beta_one) * scaled
    second_new = beta_two * second + (1.0 - beta_two) * scaled * scaled
    first_hat = first_new / (1.0 - beta_one**step_count)
    second_hat = second_new / (1.0 - beta_two**step_count)
    direction = first_hat / (jnp.sqrt(second_hat) + epsilon)
    freshened_values = master - learn_rate * (direction + shrink_factor * master)
    return (direction, freshened_values)


def body(core, hbm, outs, sc):
    (att_h, cot_h, nxt_h, mp_h, op_h, sp_h, me_h, oe_h, se_h, tn_h, tx_h, ec_h) = hbm
    (o_np, o_ne, o_dir, o_dire, o_mst, o_mste, o_norm) = outs
    s = sc
    pos = [lax.axis_index(a) for a in AXES]
    other = 1 - core
    first, count = MINE[core]
    ofirst, ocount = MINE[other]
    units = UNITS[core]
    eunit = EUNIT[core]

    def at(axis, d):
        spot = list(pos)
        spot[axis] = lax.rem(pos[axis] + d, 4)
        return spot

    def in_plane(q, a, b):
        i, j = [k for k in range(3) if k != q]
        spot = list(pos)
        spot[i] = lax.rem(pos[i] + a, 4)
        spot[j] = lax.rem(pos[j] + b, 4)
        return spot

    def plane_of(q, spot):
        return [spot[k] for k in range(3) if k != q]

    def cut(q, p):
        index = [slice(None)] * 3
        index[q] = p
        return tuple(index)

    partner = tuple(pos[:3]) + (other,)

    def remote(src, dst, send, recv, spot):
        copy = pltpu.make_async_remote_copy(
            src_ref=src, dst_ref=dst, send_sem=send, recv_sem=recv,
            device_id=tuple(spot), device_id_type=MESH,
        )
        copy.start()

    def got(ref, sem):
        pltpu.make_async_remote_copy(
            src_ref=ref, dst_ref=ref, send_sem=sem, recv_sem=sem,
            device_id=partner, device_id_type=MESH,
        ).wait_recv()

    phase = Phase()
    phase("start")
    loads = []
    for k, (src, dst) in enumerate((
        (att_h, s.att), (cot_h, s.cot), (tn_h, s.now), (tx_h, s.later), (ec_h, s.ecot),
        (mp_h, s.st.at[core, 0]), (op_h, s.st.at[core, 1]), (sp_h, s.st.at[core, 2]),
        (me_h, s.ste.at[core, 0]), (oe_h, s.ste.at[core, 1]), (se_h, s.ste.at[core, 2]),
        (nxt_h, s.nxt),
    )):
        loads.append(pltpu.make_async_copy(src, dst, s.load_sem.at[k]))
    for copy in loads[:5]:
        copy.start()

    phase("signal")
    barrier = pltpu.get_barrier_semaphore()
    peers = {}
    for q in range(3):
        for a in range(4):
            for b in range(4):
                if (a, b) != (0, 0):
                    key = [0, 0, 0]
                    i, j = [k for k in range(3) if k != q]
                    key[i], key[j] = a, b
                    peers[tuple(key)] = in_plane(q, a, b)
    everyone = [tuple(p) for _, p in sorted(peers.items())] + [partner]
    for spot in everyone:
        pl.semaphore_signal(barrier, inc=1, device_id=spot, device_id_type=MESH)

    def paired(tiles):
        return [tiles[k : k + 2] for k in range(0, len(tiles), 2)]

    def terms(tiles):
        t0, n = tiles[0], len(tiles)
        both = lax.dot_general(
            s.att[...], s.cot[:, t0 * 128 : (t0 + n) * 128], (((0,), (0,)), ((), ())),
            preferred_element_type=F32,
        )
        return [both[:, k * 128 : k * 128 + 128] for k in range(n)]

    phase("load")
    loads[0].wait()
    loads[1].wait()
    for copy in loads[5:]:
        copy.start()

    for k, tiles in enumerate(paired(list(range(ofirst, ofirst + ocount)))):
        phase(f"partner_terms{k}")
        parts = terms(tiles)
        for t, part in zip(tiles, parts):
            s.ps[t - ofirst] = part.astype(BF16)
        if k == 0:
            phase("barrier")
            pl.semaphore_wait(barrier, len(everyone))
        for t in tiles:
            remote(s.ps.at[t - ofirst], s.pr.at[t - ofirst], s.psend.at[t - ofirst], s.precv.at[t - ofirst], partner)

    x2 = s.x.reshape(SLOTS, 1152, 128)
    xe2 = s.xE.reshape(SLOTS, 256, 128)

    def stage_one(u, x, r1, q, j0, n):
        for d in (1, 3, 2):
            spot = at(q, d)
            remote(
                x.at[(pl.ds(j0, n),) + cut(q, spot[q])],
                r1.at[pl.ds(j0, n), d],
                s.send1.at[u], s.recv1.at[u], spot,
            )

    def keep_one(x, r1, q, j0, n):
        for j in range(j0, j0 + n):
            r1[j, 0] = x[(j,) + cut(q, pos[q])]

    for tiles in paired(list(range(first, first + count))):
        phase(f"own_terms{tiles[0] - first}")
        parts = terms(tiles)
        for t, part in zip(tiles, parts):
            j = t - first
            got(s.pr.at[j], s.precv.at[j])
            x2[j] = (part + s.pr[j].astype(F32)).astype(BF16)
            stage_one(j, s.x, s.r1, *units[j])

    phase("freqs")
    for k, src in enumerate((mp_h, op_h, sp_h)):
        remote(src, s.st.at[core, k], s.dsend.at[k], s.drecv.at[k], partner)
    for k, src in enumerate((me_h, oe_h, se_h)):
        remote(src, s.ste.at[core, k], s.dsend.at[3 + k], s.drecv.at[3 + k], partner)
    for k in (2, 3, 4):
        loads[k].wait()
    ladder = lax.broadcasted_iota(jnp.int32, (8, 128), 1).astype(F32)
    line = lax.broadcasted_iota(jnp.int32, (8, 128), 0)
    freqs = jnp.exp(-math.log(10000.0) * ladder / 128)
    moments = jnp.where(
        line == 0, s.now[0], jnp.where(line == 1, s.now[1], jnp.where(line == 2, s.later[0], s.later[1]))
    )
    phases = (moments * 1000.0) * freqs
    waves = jnp.concatenate([jnp.cos(phases), jnp.sin(phases)], axis=1).astype(BF16)
    columns = jnp.transpose(waves.astype(F32), (1, 0))
    cots = s.ecot[...].astype(F32)

    def eterm(t):
        c = cots[:, t * 128 : t * 128 + 128]
        return columns[:, 0:1] * c[0:1] + columns[:, 1:2] * c[1:2]

    phase("eterms")
    for j in range(ocount):
        s.psE[j] = eterm(ofirst + j).astype(BF16)
    remote(s.psE.at[pl.ds(0, ocount)], s.prE.at[pl.ds(0, ocount)], s.dsend.at[6], s.drecv.at[6], partner)
    for unit in units:
        keep_one(s.x, s.r1, *unit)
    phase("chip_e")
    got(s.prE.at[pl.ds(0, count)], s.drecv.at[6])
    for j in range(count):
        xe2[j] = (eterm(first + j) + s.prE[j].astype(F32)).astype(BF16)
    stage_one(E, s.xE, s.r1E, *eunit)
    keep_one(s.xE, s.r1E, *eunit)

    phase("state")
    for k in range(6):
        loads[5 + k].wait()
    for k in range(3):
        got(s.st.at[other, k], s.drecv.at[k])
        got(s.ste.at[other, k], s.drecv.at[3 + k])
    for k in range(3):
        for j in range(count):
            t = first + j
            for half in range(2):
                s.reg[k, j, 9 * half : 9 * half + 9] = s.st[half, k, pl.ds(t, 9, stride=9), :]
                s.regE[k, j, 2 * half : 2 * half + 2] = s.ste[half, k, pl.ds(t, 2, stride=9), :]

    r1v = s.r1.reshape(SLOTS, 4, 288, 128)
    y2 = s.y.reshape(SLOTS, 288, 128)
    r1ve = s.r1E.reshape(SLOTS, 4, 64, 128)
    y2e = s.yE.reshape(SLOTS, 64, 128)

    def stage_two(u, r1, r1v, y, y2, r2, words, q, j0, n):
        got(r1.at[pl.ds(j0, n), pl.ds(1, 3)], s.recv1.at[u])
        for j in range(j0, j0 + n):
            total = r1v[j, 0].astype(F32)
            for d in (1, 2, 3):
                total = total + r1v[j, d].astype(F32)
            y2[j] = total.astype(BF16)
        for a, b in FAR:
            spot = in_plane(q, a, b)
            p1, p2 = plane_of(q, spot)
            remote(
                y.at[pl.ds(j0, n), p1, p2],
                r2.at[pl.ds(j0, n), a * 4 + b, pl.ds(0, words)],
                s.send2.at[u], s.recv2.at[u], spot,
            )
        p1, p2 = plane_of(q, pos)
        for j in range(j0, j0 + n):
            r2[j, 0, 0:words] = y[j, p1, p2]

    for u, unit in enumerate(units):
        phase(f"two{u}")
        stage_two(u, s.r1, r1v, s.y, y2, s.r2, 9, *unit)
    phase("two_e")
    stage_two(E, s.r1E, r1ve, s.yE, y2e, s.r2E, 2, *eunit)

    r2v = s.r2.reshape(SLOTS, 16, 24, 128)
    r2ve = s.r2E.reshape(SLOTS, 16, 8, 128)
    squares = jnp.zeros((24, 128), F32)
    squares_e = jnp.zeros((8, 128), F32)
    for u, (q, j0, n) in enumerate(units):
        phase(f"sum{u}")
        got(s.r2.at[pl.ds(j0, n), pl.ds(1, 15), pl.ds(0, 9)], s.recv2.at[u])
        for j in range(j0, j0 + n):
            total = r2v[j, 0].astype(F32)
            for k in range(1, 16):
                total = total + r2v[j, k].astype(F32)
            s.g[j] = total
            squares = squares + total * total
    phase("sum_e")
    q, j0, n = eunit
    got(s.r2E.at[pl.ds(j0, n), pl.ds(1, 15), pl.ds(0, 2)], s.recv2.at[E])
    for j in range(j0, j0 + n):
        total = r2ve[j, 0].astype(F32)
        for k in range(1, 16):
            total = total + r2ve[j, k].astype(F32)
        s.gE[j] = total
        squares_e = squares_e + total * total

    phase("squares")
    rows = lax.broadcasted_iota(jnp.int32, (24, 128), 0)
    rows_e = lax.broadcasted_iota(jnp.int32, (8, 128), 0)
    squares = jnp.sum(jnp.where(rows < 18, squares, 0.0), axis=0, keepdims=True)
    squares = squares + jnp.sum(jnp.where(rows_e < 4, squares_e, 0.0), axis=0, keepdims=True)
    s.na[core] = squares
    remote(s.na.at[core], s.na.at[core], s.nsend.at[0], s.nrecv.at[0], partner)
    phase("norm_a")
    got(s.na.at[other], s.nrecv.at[0])
    pz, py, px = pos[:3]
    s.nb[pz, py] = s.na[0] + s.na[1]
    for a, b in FAR:
        remote(s.nb.at[pz, py], s.nb.at[pz, py], s.nsend.at[1], s.nrecv.at[1], in_plane(2, a, b))
    phase("norm_b")
    got(s.nw.at[pl.ds(0, 15)], s.nrecv.at[1])
    total = s.nb[0, 0]
    for k in range(1, 16):
        total = total + s.nb[k // 4, k % 4]
    s.nc[px] = total
    for d in (2, 1, 3):
        remote(s.nc.at[px], s.nc.at[px], s.nsend.at[2], s.nrecv.at[2], at(2, d))
    phase("norm_c")
    got(s.nw.at[pl.ds(0, 3)], s.nrecv.at[2])
    total = s.nc[0] + s.nc[1] + s.nc[2] + s.nc[3]
    grad_norm = jnp.sqrt(jnp.sum(total, axis=1, keepdims=True))
    clip = jnp.minimum(jnp.float32(1.0), max_norm / (grad_norm + 1e-06))
    o_norm[...] = jnp.broadcast_to(grad_norm, (1, 128))

    z2 = s.zz.reshape(SLOTS, 24, 128)
    z2e = s.zE.reshape(SLOTS, 8, 128)

    def update(u, g, reg, zz, z2, dirs, v, words, q, j0, n):
        for j in range(j0, j0 + n):
            direction, fresh = adamw_update(g[j], clip, reg[0, j], reg[1, j], reg[2, j])
            dirs[0, j] = direction
            dirs[1, j] = fresh
            z2[j] = fresh.astype(BF16)
        p1, p2 = plane_of(q, pos)
        for a, b in FAR:
            remote(
                zz.at[pl.ds(j0, n), pl.ds(0, words)],
                v.at[pl.ds(j0, n), p1, p2],
                s.send3.at[u], s.recv3.at[u], in_plane(q, a, b),
            )
        for j in range(j0, j0 + n):
            v[j, p1, p2] = zz[j, 0:words]

    order = [0, 1, 2, E] + list(range(3, count))
    phase("update")
    for u in order:
        if u == E:
            update(E, s.gE, s.regE, s.zE, z2e, s.dirsE, s.vE, 2, *eunit)
        else:
            update(u, s.g, s.reg, s.zz, z2, s.dirs, s.v, 9, *units[u])

    phase("outs")
    for k in range(2):
        for j in range(count):
            s.os[k, j, 0:9] = s.dirs[k, j, 9 * other : 9 * other + 9]
            s.osE[k, j, 0:2] = s.dirsE[k, j, 2 * other : 2 * other + 2]
    remote(s.os, s.orr, s.dsend.at[7], s.drecv.at[7], partner)
    remote(s.osE, s.orrE, s.dsend.at[8], s.drecv.at[8], partner)
    for k, (out, oute) in enumerate(((o_dir, o_dire), (o_mst, o_mste))):
        for j in range(count):
            out[pl.ds(first + j, 9, stride=9), :] = s.dirs[k, j, 9 * core : 9 * core + 9]
            oute[pl.ds(first + j, 2, stride=9), :] = s.dirsE[k, j, 2 * core : 2 * core + 2]

    def ring(u, r2, v, w, words, q, j0, n):
        got(r2.at[pl.ds(j0, n), pl.ds(1, 15), pl.ds(0, words)], s.recv3.at[u])
        place = w.at[(pl.ds(first + j0, n),) + cut(q, pos[q])]
        for d in (1, 3, 2):
            remote(v.at[pl.ds(j0, n)], place, s.send4.at[u], s.recv4.at[u, d - 1], at(q, d))
        remote(v.at[pl.ds(j0, n)], place, s.send5.at[u], s.recv5.at[u], partner)
        for j in range(j0, j0 + n):
            w[(first + j,) + cut(q, pos[q])] = v[j]

    for u in order:
        phase(f"ring{u}")
        if u == E:
            ring(E, s.r2E, s.vE, s.wE, 2, *eunit)
        else:
            ring(u, s.r2, s.v, s.w, 9, *units[u])

    phase("outs2")
    got(s.orr, s.drecv.at[7])
    got(s.orrE, s.drecv.at[8])
    for k, (out, oute) in enumerate(((o_dir, o_dire), (o_mst, o_mste))):
        for j in range(ocount):
            out[pl.ds(ofirst + j, 9, stride=9), :] = s.orr[k, j, 0:9]
            oute[pl.ds(ofirst + j, 2, stride=9), :] = s.orrE[k, j, 0:2]

    loads[11].wait()
    w2 = s.w.reshape(TILES, 1152, 128)
    we2 = s.wE.reshape(TILES, 256, 128)

    def own(u, v=s.v, w=s.w, unit=None):
        phase(f"own{u}")
        q, j0, n = unit or units[u]
        for d in (1, 3, 2):
            got(v.at[pl.ds(j0, n)], s.recv4.at[u, d - 1])
            quarter = w.at[(pl.ds(first + j0, n),) + cut(q, at(q, 4 - d)[q])]
            remote(quarter, quarter, s.send5.at[u], s.recv5.at[u], partner)

    def theirs(u):
        phase(f"theirs{u}")
        got(s.w.at[ofirst + u], s.recv5.at[u])

    def product(*tiles):
        phase(f"product{tiles[0]}")
        whole = jnp.concatenate([w2[t] for t in tiles], axis=1)
        mixed = jnp.dot(s.nxt[...], whole, preferred_element_type=F32).astype(BF16)
        for k, t in enumerate(tiles):
            o_np[:, t * 128 : t * 128 + 128] = mixed[:, k * 128 : k * 128 + 128]

    for u in (0, 1, 2):
        own(u)
    product(first, first + 1)
    theirs(0)
    product(first + 2, ofirst)
    own(E, s.vE, s.wE, eunit)
    for u in range(3, count):
        own(u)
    theirs(1)
    theirs(2)
    product(ofirst + 1, ofirst + 2)
    product(*range(first + 3, first + count))
    phase("last_e")
    got(s.wE.at[pl.ds(ofirst, ocount)], s.recv5.at[E])
    for t in range(0, TILES, 3):
        whole = jnp.concatenate([we2[t], we2[t + 1], we2[t + 2]], axis=1)
        mixed = jnp.dot(waves, whole, preferred_element_type=F32)
        o_ne[:, t * 128 : t * 128 + 384] = mixed[2:4].astype(BF16)
    for u in range(3, ocount):
        theirs(u)
    product(*range(ofirst + 3, ofirst + ocount))

    phase("drain")

    def sent(ref, sem):
        pltpu.make_async_remote_copy(
            src_ref=ref, dst_ref=ref, send_sem=sem, recv_sem=sem,
            device_id=partner, device_id_type=MESH,
        ).wait_send()

    for k in range(3):
        sent(s.st.at[core, k], s.dsend.at[k])
        sent(s.ste.at[core, k], s.dsend.at[3 + k])
    sent(s.psE.at[pl.ds(0, ocount)], s.dsend.at[6])
    sent(s.os, s.dsend.at[7])
    sent(s.osE, s.dsend.at[8])
    for j in range(ocount):
        sent(s.ps.at[j], s.psend.at[j])
    sent(s.na.at[core], s.nsend.at[0])
    sent(s.nw.at[pl.ds(0, 15)], s.nsend.at[1])
    sent(s.nw.at[pl.ds(0, 3)], s.nsend.at[2])
    for u, (q, j0, n) in enumerate(units):
        sent(s.r1.at[pl.ds(j0, n), pl.ds(1, 3)], s.send1.at[u])
        sent(s.r2.at[pl.ds(j0, n), pl.ds(1, 15), pl.ds(0, 9)], s.send2.at[u])
        sent(s.r2.at[pl.ds(j0, n), pl.ds(1, 15), pl.ds(0, 9)], s.send3.at[u])
        sent(s.r1.at[pl.ds(j0, n), pl.ds(1, 3)], s.send4.at[u])
        sent(s.w.at[pl.ds(first + j0, n)], s.send5.at[u])
    q, j0, n = eunit
    sent(s.r1E.at[pl.ds(j0, n), pl.ds(1, 3)], s.send1.at[E])
    sent(s.r2E.at[pl.ds(j0, n), pl.ds(1, 15), pl.ds(0, 2)], s.send2.at[E])
    sent(s.r2E.at[pl.ds(j0, n), pl.ds(1, 15), pl.ds(0, 2)], s.send3.at[E])
    sent(s.r1E.at[pl.ds(j0, n), pl.ds(1, 3)], s.send4.at[E])
    sent(s.wE.at[pl.ds(first, count)], s.send5.at[E])
    phase(None)


class Names:
    pass


class Phase:
    def __init__(self):
        self.open = None

    def __call__(self, name):
        if self.open is not None:
            self.open.__exit__(None, None, None)
            self.open = None
        if name is not None and PHASES:
            self.open = jax.named_scope(name)
            self.open.__enter__()


DMA = pltpu.SemaphoreType.DMA
SCRATCH = dict(
    att=pltpu.VMEM((512, 1152), BF16),
    cot=pltpu.VMEM((512, 1152), BF16),
    nxt=pltpu.VMEM((512, 1152), BF16),
    ecot=pltpu.VMEM((2, 1152), BF16),
    now=pltpu.SMEM((2,), F32),
    later=pltpu.SMEM((2,), F32),
    st=pltpu.VMEM((2, 3, 81, 128), F32),
    ste=pltpu.VMEM((2, 3, 18, 128), F32),
    ps=pltpu.VMEM((SLOTS, 1152, 128), BF16),
    pr=pltpu.VMEM((SLOTS, 1152, 128), BF16),
    psE=pltpu.VMEM((SLOTS, 256, 128), BF16),
    prE=pltpu.VMEM((SLOTS, 256, 128), BF16),
    x=pltpu.VMEM((SLOTS, 4, 4, 4, 9, 2, 128), BF16),
    xE=pltpu.VMEM((SLOTS, 4, 4, 4, 2, 2, 128), BF16),
    r1=pltpu.VMEM((SLOTS, 4, 4, 4, 9, 2, 128), BF16),
    r1E=pltpu.VMEM((SLOTS, 4, 4, 4, 2, 2, 128), BF16),
    y=pltpu.VMEM((SLOTS, 4, 4, 9, 2, 128), BF16),
    yE=pltpu.VMEM((SLOTS, 4, 4, 2, 2, 128), BF16),
    r2=pltpu.VMEM((SLOTS, 16, 12, 2, 128), BF16),
    r2E=pltpu.VMEM((SLOTS, 16, 4, 2, 128), BF16),
    reg=pltpu.VMEM((3, SLOTS, 24, 128), F32),
    regE=pltpu.VMEM((3, SLOTS, 8, 128), F32),
    g=pltpu.VMEM((SLOTS, 24, 128), F32),
    gE=pltpu.VMEM((SLOTS, 8, 128), F32),
    dirs=pltpu.VMEM((2, SLOTS, 24, 128), F32),
    dirsE=pltpu.VMEM((2, SLOTS, 8, 128), F32),
    zz=pltpu.VMEM((SLOTS, 12, 2, 128), BF16),
    zE=pltpu.VMEM((SLOTS, 4, 2, 128), BF16),
    v=pltpu.VMEM((SLOTS, 4, 4, 9, 2, 128), BF16),
    vE=pltpu.VMEM((SLOTS, 4, 4, 2, 2, 128), BF16),
    w=pltpu.VMEM((TILES, 4, 4, 4, 9, 2, 128), BF16),
    wE=pltpu.VMEM((TILES, 4, 4, 4, 2, 2, 128), BF16),
    os=pltpu.VMEM((2, SLOTS, 16, 128), F32),
    osE=pltpu.VMEM((2, SLOTS, 8, 128), F32),
    orr=pltpu.VMEM((2, SLOTS, 16, 128), F32),
    orrE=pltpu.VMEM((2, SLOTS, 8, 128), F32),
    na=pltpu.VMEM((2, 1, 128), F32),
    nb=pltpu.VMEM((4, 4, 1, 128), F32),
    nc=pltpu.VMEM((4, 1, 128), F32),
    nw=pltpu.VMEM((15, 1, 128), F32),
    load_sem=DMA((12,)),
    dsend=DMA((9,)),
    drecv=DMA((9,)),
    psend=DMA((SLOTS,)),
    precv=DMA((SLOTS,)),
    send1=DMA((6,)),
    recv1=DMA((6,)),
    send2=DMA((6,)),
    recv2=DMA((6,)),
    send3=DMA((6,)),
    recv3=DMA((6,)),
    send4=DMA((6,)),
    recv4=DMA((6, 3)),
    send5=DMA((6,)),
    recv5=DMA((6,)),
    nsend=DMA((3,)),
    nrecv=DMA((3,)),
)


def kernel(*refs):
    hbm, outs, scratch = refs[:12], refs[12:19], refs[19:]
    s = Names()
    for name, ref in zip(SCRATCH, scratch, strict=True):
        setattr(s, name, ref)
    core = lax.axis_index("c")
    for k in (0, 1):

        @pl.when(core == k)
        def _():
            body(k, hbm, outs, s)


def write_out(*refs):
    sems = refs[14]
    copies = [pltpu.make_async_copy(refs[k], refs[7 + k], sems.at[k]) for k in range(7)]
    for copy in copies:
        copy.start()
    for copy in copies:
        copy.wait()


def shards(
    attended, proj_cot, timesteps, embed_cot, master_proj, moment_proj, second_proj,
    master_embed, moment_embed, squared_moment_layer, attended_next, timesteps_next,
):
    flat = [a.reshape(-1, 128) for a in (master_proj, moment_proj, second_proj)]
    flat_e = [a.reshape(-1, 128) for a in (master_embed, moment_embed, squared_moment_layer)]
    anywhere = pl.BlockSpec(memory_space=pl.ANY)
    large = pl.BlockSpec(memory_space=pltpu.HBM)
    vmem = pl.BlockSpec(memory_space=pltpu.VMEM)
    shape = jax.ShapeDtypeStruct
    results = (
        shape((512, 1152), BF16), shape((2, 1152), BF16), shape((81, 128), F32),
        shape((18, 128), F32), shape((81, 128), F32), shape((18, 128), F32), shape((1, 128), F32),
    )
    inside = pl.pallas_call(
        kernel,
        out_shape=[pltpu.VMEM(r.shape, r.dtype) for r in results],
        in_specs=[large] * 12,
        out_specs=[vmem] * 7,
        scratch_shapes=list(SCRATCH.values()),
        compiler_params=pltpu.CompilerParams(
            collective_id=0, has_side_effects=True, vmem_limit_bytes=60 * 2**20
        ),
        name="step",
    )(attended, proj_cot, attended_next, *flat, *flat_e, timesteps, timesteps_next, embed_cot)
    nproj, nembed, d, de, m, mste, norm = pl.pallas_call(
        write_out,
        out_shape=results,
        in_specs=[vmem] * 7,
        out_specs=[large] * 7,
        scratch_shapes=[DMA((7,))],
        compiler_params=pltpu.CompilerParams(vmem_limit_bytes=8 * 2**20),
        name="write_out",
    )(*inside)
    return (
        nproj, nembed, d.reshape(-1), de.reshape(-1), m.reshape(-1), mste.reshape(-1), norm[0, 0],
    )


def solution(mesh):
    finer = Mesh(mesh.devices.reshape(4, 4, 4, 2), AXES)
    dp = P(AXES)
    wide = P(AXES, None)
    return jax.shard_map(
        shards,
        mesh=finer,
        in_specs=(wide, wide, dp, wide, dp, dp, dp, dp, dp, dp, wide, dp),
        out_specs=(wide, wide, dp, dp, dp, dp, P()),
        check_vma=False,
    )
```

```python
import functools
import math

import jax
import jax.numpy as jnp
from jax import lax
from jax.experimental import pallas as pl
from jax.experimental.pallas import tpu as pltpu
from jax.sharding import Mesh
from jax.sharding import PartitionSpec as P

AXES = ("z", "y", "x", "c")
MESH = pl.DeviceIdType.MESH
F32 = jnp.float32
BF16 = jnp.bfloat16

beta_one = 0.9
beta_two = 0.999
step_count = 1000.0
learn_rate = 0.0001
shrink_factor = 0.01
epsilon = 1e-08
max_norm = 1.0

TILES = 9
MINE = {0: (0, 5), 1: (5, 4)}
UNITS = {
    0: ((0, 0, 1), (1, 1, 1), (2, 2, 1), (0, 3, 1), (1, 4, 1)),
    1: ((0, 0, 1), (1, 1, 1), (2, 2, 1), (2, 3, 1)),
}
E = 5
AROUND = [
    (a, b, c) for a in (2, 1, 3, 0) for b in (2, 1, 3, 0) for c in (2, 1, 3, 0) if (a, b, c) != (0, 0, 0)
]
FAR = [(a, b) for a in (2, 1, 3, 0) for b in (2, 1, 3, 0) if (a, b) != (0, 0)]
EUNIT = {0: (1, 0, 5), 1: (0, 0, 4)}
SLOTS = 5
PHASES = False


def adamw_update(gradient, clip, master, moment, second):
    scaled = clip * gradient
    first_new = beta_one * moment + (1.0 - beta_one) * scaled
    second_new = beta_two * second + (1.0 - beta_two) * scaled * scaled
    first_hat = first_new / (1.0 - beta_one**step_count)
    second_hat = second_new / (1.0 - beta_two**step_count)
    direction = first_hat / (jnp.sqrt(second_hat) + epsilon)
    freshened_values = master - learn_rate * (direction + shrink_factor * master)
    return (direction, freshened_values)


def body(core, hbm, outs, sc):
    (att_h, cot_h, nxt_h, mp_h, op_h, sp_h, me_h, oe_h, se_h, tn_h, tx_h, ec_h) = hbm
    (o_np, o_ne, o_dir, o_dire, o_mst, o_mste, o_norm) = outs
    s = sc
    pos = [lax.axis_index(a) for a in AXES]
    other = 1 - core
    first, count = MINE[core]
    ofirst, ocount = MINE[other]
    units = UNITS[core]
    eunit = EUNIT[core]

    def at(axis, d):
        spot = list(pos)
        spot[axis] = lax.rem(pos[axis] + d, 4)
        return spot

    def in_plane(q, a, b):
        i, j = [k for k in range(3) if k != q]
        spot = list(pos)
        spot[i] = lax.rem(pos[i] + a, 4)
        spot[j] = lax.rem(pos[j] + b, 4)
        return spot

    def plane_of(q, spot):
        return [spot[k] for k in range(3) if k != q]

    def cut(q, p):
        index = [slice(None)] * 3
        index[q] = p
        return tuple(index)

    partner = tuple(pos[:3]) + (other,)

    def remote(src, dst, send, recv, spot):
        copy = pltpu.make_async_remote_copy(
            src_ref=src, dst_ref=dst, send_sem=send, recv_sem=recv,
            device_id=tuple(spot), device_id_type=MESH,
        )
        copy.start()

    def got(ref, sem):
        pltpu.make_async_remote_copy(
            src_ref=ref, dst_ref=ref, send_sem=sem, recv_sem=sem,
            device_id=partner, device_id_type=MESH,
        ).wait_recv()

    def sent(ref, sem):
        pltpu.make_async_remote_copy(
            src_ref=ref, dst_ref=ref, send_sem=sem, recv_sem=sem,
            device_id=partner, device_id_type=MESH,
        ).wait_send()

    phase = Phase()
    phase("start")
    def load(src, dst, k):
        pltpu.make_async_copy(src, dst, s.load_sem.at[k]).start()

    def loaded(ref, k):
        pltpu.make_async_copy(ref, ref, s.load_sem.at[k]).wait()

    load(tn_h, s.now, 0)
    load(tx_h, s.later, 1)
    load(ec_h, s.ecot, 2)
    load(att_h, s.att, 3)
    load(cot_h, s.cot, 4)

    phase("signal")
    barrier = pltpu.get_barrier_semaphore()
    around = [
        tuple(lax.rem(pos[k] + d[k], 4) for k in range(3)) + (pos[3],) for d in AROUND
    ]
    everyone = around + [partner]
    for spot in everyone:
        pl.semaphore_signal(barrier, inc=1, device_id=spot, device_id_type=MESH)

    def paired(tiles):
        return [tiles[k : k + 2] for k in range(0, len(tiles), 2)]

    def terms(tiles):
        cols = s.cot[:, tiles[0] * 128 : (tiles[-1] + 1) * 128]
        return [
            jnp.dot(s.attT[h * 576 : h * 576 + 576, :], cols, preferred_element_type=F32)
            for h in range(2)
        ]

    phase("freqs")
    loaded(s.now, 0)
    loaded(s.later, 1)
    loaded(s.ecot, 2)
    ladder = lax.broadcasted_iota(jnp.int32, (8, 128), 1).astype(F32)
    line = lax.broadcasted_iota(jnp.int32, (8, 128), 0)
    freqs = jnp.exp(-math.log(10000.0) * ladder / 128)
    moments = jnp.where(
        line == 0, s.now[0], jnp.where(line == 1, s.now[1], jnp.where(line == 2, s.later[0], s.later[1]))
    )
    phases = (moments * 1000.0) * freqs
    waves = jnp.concatenate([jnp.cos(phases), jnp.sin(phases)], axis=1).astype(BF16)
    columns = jnp.transpose(waves.astype(F32), (1, 0))
    cots = s.ecot[...].astype(F32)

    def eterm(t):
        c = cots[:, t * 128 : t * 128 + 128]
        return columns[:, 0:1] * c[0:1] + columns[:, 1:2] * c[1:2]

    for j in range(ocount):
        s.psE[j] = eterm(ofirst + j).astype(BF16)

    phase("load")
    loaded(s.att, 3)
    s.attT[...] = jnp.transpose(s.att[...], (1, 0))
    loaded(s.cot, 4)
    for k, src in enumerate((mp_h, op_h, sp_h)):
        load(src, s.st.at[core, k], 5)
    for k, src in enumerate((me_h, oe_h, se_h)):
        load(src, s.ste.at[core, k], 6)
    load(nxt_h, s.nxt, 7)

    for k, tiles in enumerate(paired(list(range(ofirst, ofirst + ocount)))):
        phase(f"partner_terms{k}")
        parts = terms(tiles)
        for i, t in enumerate(tiles):
            for h in range(2):
                s.ps[t - ofirst, h * 576 : h * 576 + 576] = parts[h][:, i * 128 : i * 128 + 128].astype(BF16)
        if k == 0:
            phase("barrier")
            pl.semaphore_wait(barrier, len(everyone))
            remote(s.psE.at[pl.ds(0, ocount)], s.prE.at[pl.ds(0, ocount)], s.dsend.at[2], s.drecv.at[2], partner)
        for t in tiles:
            remote(s.ps.at[t - ofirst], s.pr.at[t - ofirst], s.psend, s.recvc.at[t - ofirst], partner)
    for k, src in enumerate((mp_h, op_h, sp_h)):
        remote(src, s.st.at[core, k], s.dsend.at[0], s.drecv.at[0], partner)
    for k, src in enumerate((me_h, oe_h, se_h)):
        remote(src, s.ste.at[core, k], s.dsend.at[1], s.drecv.at[1], partner)

    x2 = s.x.reshape(SLOTS, 1152, 128)
    xe2 = s.xE.reshape(SLOTS, 256, 128)

    def stage_one(u, x, r1, q, j0, n):
        for d in (1, 3, 2):
            spot = at(q, d)
            remote(
                x.at[(pl.ds(j0, n),) + cut(q, spot[q])],
                r1.at[pl.ds(j0, n), d],
                s.senda.at[int(u == E)], s.recva.at[u], spot,
            )

    def keep_one(x, r1, q, j0, n):
        for j in range(j0, j0 + n):
            r1[j, 0] = x[(j,) + cut(q, pos[q])]

    phase("chip_e")
    got(s.prE.at[pl.ds(0, count)], s.drecv.at[2])
    for j in range(count):
        xe2[j] = (eterm(first + j) + s.prE[j].astype(F32)).astype(BF16)
    stage_one(E, s.xE, s.r1E, *eunit)

    for tiles in paired(list(range(first, first + count))):
        phase(f"own_terms{tiles[0] - first}")
        parts = terms(tiles)
        for i, t in enumerate(tiles):
            j = t - first
            got(s.pr.at[j], s.recvc.at[j])
            for h in range(2):
                part = parts[h][:, i * 128 : i * 128 + 128]
                x2[j, h * 576 : h * 576 + 576] = (part + s.pr[j, h * 576 : h * 576 + 576].astype(F32)).astype(BF16)
            stage_one(j, s.x, s.r1, *units[j])

    phase("keep")
    keep_one(s.xE, s.r1E, *eunit)
    for unit in units:
        keep_one(s.x, s.r1, *unit)

    phase("state")
    loaded(s.st.at[core], 5)
    loaded(s.ste.at[core], 6)
    got(s.st.at[other], s.drecv.at[0])
    got(s.ste.at[other], s.drecv.at[1])
    for k in range(3):
        for j in range(count):
            t = first + j
            for half in range(2):
                s.reg[k, j, 9 * half : 9 * half + 9] = s.st[half, k, pl.ds(t, 9, stride=9), :]
                s.regE[k, j, 2 * half : 2 * half + 2] = s.ste[half, k, pl.ds(t, 2, stride=9), :]

    r1v = s.r1.reshape(SLOTS, 4, 288, 128)
    y2 = s.y.reshape(SLOTS, 288, 128)
    r1ve = s.r1E.reshape(SLOTS, 4, 64, 128)
    y2e = s.yE.reshape(SLOTS, 64, 128)

    def stage_two(u, r1, r1v, y, y2, r2, words, q, j0, n):
        got(r1.at[pl.ds(j0, n), pl.ds(1, 3)], s.recva.at[u])
        for j in range(j0, j0 + n):
            total = r1v[j, 0].astype(F32)
            for d in (1, 2, 3):
                total = total + r1v[j, d].astype(F32)
            y2[j] = total.astype(BF16)
        for a, b in FAR:
            spot = in_plane(q, a, b)
            p1, p2 = plane_of(q, spot)
            remote(
                y.at[pl.ds(j0, n), p1, p2],
                r2.at[pl.ds(j0, n), a * 4 + b, pl.ds(0, words)],
                s.sendb.at[int(u == E)], s.recvb.at[u], spot,
            )
        p1, p2 = plane_of(q, pos)
        for j in range(j0, j0 + n):
            r2[j, 0, 0:words] = y[j, p1, p2]

    for u, unit in enumerate(units):
        phase(f"two{u}")
        stage_two(u, s.r1, r1v, s.y, y2, s.r2, 9, *unit)
    phase("two_e")
    stage_two(E, s.r1E, r1ve, s.yE, y2e, s.r2E, 2, *eunit)

    r2v = s.r2.reshape(SLOTS, 16, 24, 128)
    r2ve = s.r2E.reshape(SLOTS, 16, 8, 128)
    squares = jnp.zeros((24, 128), F32)
    squares_e = jnp.zeros((8, 128), F32)
    for u, (q, j0, n) in enumerate(units):
        phase(f"sum{u}")
        got(s.r2.at[pl.ds(j0, n), pl.ds(1, 15), pl.ds(0, 9)], s.recvb.at[u])
        for j in range(j0, j0 + n):
            total = r2v[j, 0].astype(F32)
            for k in range(1, 16):
                total = total + r2v[j, k].astype(F32)
            s.g[j] = total
            squares = squares + total * total
    phase("sum_e")
    q, j0, n = eunit
    got(s.r2E.at[pl.ds(j0, n), pl.ds(1, 15), pl.ds(0, 2)], s.recvb.at[E])
    for j in range(j0, j0 + n):
        total = r2ve[j, 0].astype(F32)
        for k in range(1, 16):
            total = total + r2ve[j, k].astype(F32)
        s.gE[j] = total
        squares_e = squares_e + total * total

    phase("squares")
    rows = lax.broadcasted_iota(jnp.int32, (24, 128), 0)
    rows_e = lax.broadcasted_iota(jnp.int32, (8, 128), 0)
    squares = jnp.sum(jnp.where(rows < 18, squares, 0.0), axis=0, keepdims=True)
    squares = squares + jnp.sum(jnp.where(rows_e < 4, squares_e, 0.0), axis=0, keepdims=True)
    s.na[core] = squares
    remote(s.na.at[core], s.na.at[core], s.nsend.at[0], s.nrecv.at[0], partner)
    phase("norm_a")
    got(s.na.at[other], s.nrecv.at[0])
    pz, py, px = pos[:3]
    mine = s.nb.at[pz, py, px]
    s.nb[pz, py, px] = s.na[0] + s.na[1]
    for spot in around:
        remote(mine, mine, s.nsend.at[1], s.nrecv.at[1], spot)
    sent(s.st.at[core], s.dsend.at[0])
    sent(s.ste.at[core], s.dsend.at[1])
    sent(s.r1.at[pl.ds(0, count), pl.ds(1, 3)], s.senda.at[0])
    sent(s.r1E.at[pl.ds(0, count), pl.ds(1, 3)], s.senda.at[1])
    sent(s.r2.at[pl.ds(0, count), pl.ds(1, 15), pl.ds(0, 9)], s.sendb.at[0])
    sent(s.r2E.at[pl.ds(0, count), pl.ds(1, 15), pl.ds(0, 2)], s.sendb.at[1])
    phase("norm_b")
    got(s.nw, s.nrecv.at[1])
    total = s.nb[0, 0, 0]
    for k in range(1, 64):
        total = total + s.nb[k // 16, k // 4 % 4, k % 4]
    grad_norm = jnp.sqrt(jnp.sum(total, axis=1, keepdims=True))
    clip = jnp.minimum(jnp.float32(1.0), max_norm / (grad_norm + 1e-06))
    o_norm[...] = jnp.broadcast_to(grad_norm, (1, 128))

    z2 = s.zz.reshape(SLOTS, 24, 128)
    z2e = s.zE.reshape(SLOTS, 8, 128)

    def update(u, g, reg, zz, z2, dirs, v, words, q, j0, n):
        for j in range(j0, j0 + n):
            direction, fresh = adamw_update(g[j], clip, reg[0, j], reg[1, j], reg[2, j])
            dirs[0, j] = direction
            dirs[1, j] = fresh
            z2[j] = fresh.astype(BF16)
        p1, p2 = plane_of(q, pos)
        for a, b in FAR:
            remote(
                zz.at[pl.ds(j0, n), pl.ds(0, words)],
                v.at[pl.ds(j0, n), p1, p2],
                s.senda.at[int(u == E)], s.recva.at[u], in_plane(q, a, b),
            )
        for j in range(j0, j0 + n):
            v[j, p1, p2] = zz[j, 0:words]

    order = list(range(count)) + [E]
    phase("update")
    for u in order:
        if u == E:
            update(E, s.gE, s.regE, s.zE, z2e, s.dirsE, s.vE, 2, *eunit)
        else:
            update(u, s.g, s.reg, s.zz, z2, s.dirs, s.v, 9, *units[u])

    phase("outs")
    for k in range(2):
        for j in range(count):
            s.os[k, j, 0:9] = s.dirs[k, j, 9 * other : 9 * other + 9]
            s.osE[k, j, 0:2] = s.dirsE[k, j, 2 * other : 2 * other + 2]
    remote(s.os, s.orr, s.dsend.at[0], s.drecv.at[0], partner)
    remote(s.osE, s.orrE, s.dsend.at[1], s.drecv.at[1], partner)
    for k, (out, oute) in enumerate(((o_dir, o_dire), (o_mst, o_mste))):
        for j in range(count):
            out[pl.ds(first + j, 9, stride=9), :] = s.dirs[k, j, 9 * core : 9 * core + 9]
            oute[pl.ds(first + j, 2, stride=9), :] = s.dirsE[k, j, 2 * core : 2 * core + 2]

    def ring(u, r2, v, w, words, q, j0, n):
        got(r2.at[pl.ds(j0, n), pl.ds(1, 15), pl.ds(0, words)], s.recva.at[u])
        place = w.at[(pl.ds(first + j0, n),) + cut(q, pos[q])]
        for d in (1, 3, 2):
            remote(v.at[pl.ds(j0, n)], place, s.sendb.at[int(u == E)], s.recvb.at[u], at(q, d))
        remote(v.at[pl.ds(j0, n)], place, s.sendc.at[int(u == E)], s.recvc.at[u], partner)
        for j in range(j0, j0 + n):
            w[(first + j,) + cut(q, pos[q])] = v[j]

    for u in order:
        phase(f"ring{u}")
        if u == E:
            ring(E, s.r2E, s.vE, s.wE, 2, *eunit)
        else:
            ring(u, s.r2, s.v, s.w, 9, *units[u])

    phase("outs2")
    got(s.orr, s.drecv.at[0])
    got(s.orrE, s.drecv.at[1])
    for k, (out, oute) in enumerate(((o_dir, o_dire), (o_mst, o_mste))):
        for j in range(ocount):
            out[pl.ds(ofirst + j, 9, stride=9), :] = s.orr[k, j, 0:9]
            oute[pl.ds(ofirst + j, 2, stride=9), :] = s.orrE[k, j, 0:2]

    loaded(s.nxt, 7)
    w2 = s.w.reshape(TILES, 1152, 128)
    we2 = s.wE.reshape(TILES, 256, 128)

    def own(u, r1, w, q, j0, n):
        phase(f"own{u}")
        got(r1.at[pl.ds(j0, n), pl.ds(1, 3)], s.recvb.at[u])
        for d in (1, 3, 2):
            quarter = w.at[(pl.ds(first + j0, n),) + cut(q, at(q, d)[q])]
            remote(quarter, quarter, s.sendc.at[int(u == E)], s.recvc.at[u], partner)

    def theirs(u):
        phase(f"theirs{u}")
        got(s.w.at[ofirst + u], s.recvc.at[u])

    def product(lo, hi):
        phase(f"product{lo}")
        whole = jnp.concatenate([w2[t] for t in range(lo, hi)], axis=1)
        for h in range(2):
            o_np[h * 256 : h * 256 + 256, lo * 128 : hi * 128] = jnp.dot(
                s.nxt[h * 256 : h * 256 + 256, :], whole, preferred_element_type=F32
            ).astype(BF16)

    def eproduct(lo, hi):
        phase(f"eproduct{lo}")
        whole = jnp.concatenate([we2[t] for t in range(lo, hi)], axis=1)
        mixed = jnp.dot(waves, whole, preferred_element_type=F32)
        o_ne[:, lo * 128 : hi * 128] = mixed[2:4].astype(BF16)

    for u in range(count):
        own(u, s.r1, s.w, *units[u])
    own(E, s.r1E, s.wE, *eunit)
    product(first, first + count)
    eproduct(first, first + count)
    for u in range(ocount):
        theirs(u)
    got(s.wE.at[pl.ds(ofirst, ocount)], s.recvc.at[E])
    product(ofirst, ofirst + ocount)
    eproduct(ofirst, ofirst + ocount)

    phase("drain")
    sent(s.psE.at[pl.ds(0, ocount)], s.dsend.at[2])
    sent(s.os, s.dsend.at[0])
    sent(s.osE, s.dsend.at[1])
    sent(s.ps.at[pl.ds(0, ocount)], s.psend)
    sent(s.na.at[core], s.nsend.at[0])
    sent(s.nw, s.nsend.at[1])
    sent(s.r2.at[pl.ds(0, count), pl.ds(1, 15), pl.ds(0, 9)], s.senda.at[0])
    sent(s.r2E.at[pl.ds(0, count), pl.ds(1, 15), pl.ds(0, 2)], s.senda.at[1])
    sent(s.r1.at[pl.ds(0, count), pl.ds(1, 3)], s.sendb.at[0])
    sent(s.r1E.at[pl.ds(0, count), pl.ds(1, 3)], s.sendb.at[1])
    sent(s.w.at[pl.ds(first, count)], s.sendc.at[0])
    sent(s.wE.at[pl.ds(first, count)], s.sendc.at[1])
    phase(None)


class Names:
    pass


class Phase:
    def __init__(self):
        self.open = None

    def __call__(self, name):
        if self.open is not None:
            self.open.__exit__(None, None, None)
            self.open = None
        if name is not None and PHASES:
            self.open = jax.named_scope(name)
            self.open.__enter__()


DMA = pltpu.SemaphoreType.DMA
SCRATCH = dict(
    att=pltpu.VMEM((512, 1152), BF16),
    attT=pltpu.VMEM((1152, 512), BF16),
    cot=pltpu.VMEM((512, 1152), BF16),
    nxt=pltpu.VMEM((512, 1152), BF16),
    ecot=pltpu.VMEM((2, 1152), BF16),
    now=pltpu.SMEM((2,), F32),
    later=pltpu.SMEM((2,), F32),
    st=pltpu.VMEM((2, 3, 81, 128), F32),
    ste=pltpu.VMEM((2, 3, 18, 128), F32),
    ps=pltpu.VMEM((SLOTS, 1152, 128), BF16),
    pr=pltpu.VMEM((SLOTS, 1152, 128), BF16),
    psE=pltpu.VMEM((SLOTS, 256, 128), BF16),
    prE=pltpu.VMEM((SLOTS, 256, 128), BF16),
    x=pltpu.VMEM((SLOTS, 4, 4, 4, 9, 2, 128), BF16),
    xE=pltpu.VMEM((SLOTS, 4, 4, 4, 2, 2, 128), BF16),
    r1=pltpu.VMEM((SLOTS, 4, 4, 4, 9, 2, 128), BF16),
    r1E=pltpu.VMEM((SLOTS, 4, 4, 4, 2, 2, 128), BF16),
    y=pltpu.VMEM((SLOTS, 4, 4, 9, 2, 128), BF16),
    yE=pltpu.VMEM((SLOTS, 4, 4, 2, 2, 128), BF16),
    r2=pltpu.VMEM((SLOTS, 16, 12, 2, 128), BF16),
    r2E=pltpu.VMEM((SLOTS, 16, 4, 2, 128), BF16),
    reg=pltpu.VMEM((3, SLOTS, 24, 128), F32),
    regE=pltpu.VMEM((3, SLOTS, 8, 128), F32),
    g=pltpu.VMEM((SLOTS, 24, 128), F32),
    gE=pltpu.VMEM((SLOTS, 8, 128), F32),
    dirs=pltpu.VMEM((2, SLOTS, 24, 128), F32),
    dirsE=pltpu.VMEM((2, SLOTS, 8, 128), F32),
    zz=pltpu.VMEM((SLOTS, 12, 2, 128), BF16),
    zE=pltpu.VMEM((SLOTS, 4, 2, 128), BF16),
    v=pltpu.VMEM((SLOTS, 4, 4, 9, 2, 128), BF16),
    vE=pltpu.VMEM((SLOTS, 4, 4, 2, 2, 128), BF16),
    w=pltpu.VMEM((TILES, 4, 4, 4, 9, 2, 128), BF16),
    wE=pltpu.VMEM((TILES, 4, 4, 4, 2, 2, 128), BF16),
    os=pltpu.VMEM((2, SLOTS, 16, 128), F32),
    osE=pltpu.VMEM((2, SLOTS, 8, 128), F32),
    orr=pltpu.VMEM((2, SLOTS, 16, 128), F32),
    orrE=pltpu.VMEM((2, SLOTS, 8, 128), F32),
    na=pltpu.VMEM((2, 1, 128), F32),
    nb=pltpu.VMEM((4, 4, 4, 1, 128), F32),
    nw=pltpu.VMEM((63, 1, 128), F32),
    load_sem=DMA((8,)),
    dsend=DMA((3,)),
    drecv=DMA((3,)),
    psend=DMA(()),
    senda=DMA((2,)),
    sendb=DMA((2,)),
    sendc=DMA((2,)),
    recva=DMA((6,)),
    recvb=DMA((6,)),
    recvc=DMA((6,)),
    nsend=DMA((2,)),
    nrecv=DMA((2,)),
)


def kernel(*refs):
    hbm, outs, scratch = refs[:12], refs[12:19], refs[19:]
    s = Names()
    for name, ref in zip(SCRATCH, scratch, strict=True):
        setattr(s, name, ref)
    core = lax.axis_index("c")
    for k in (0, 1):

        @pl.when(core == k)
        def _():
            body(k, hbm, outs, s)


def write_out(*refs):
    sems = refs[14]
    copies = [pltpu.make_async_copy(refs[k], refs[7 + k], sems.at[k]) for k in range(7)]
    for copy in copies:
        copy.start()
    for copy in copies:
        copy.wait()


def shards(
    attended, proj_cot, timesteps, embed_cot, master_proj, moment_proj, second_proj,
    master_embed, moment_embed, squared_moment_layer, attended_next, timesteps_next,
):
    flat = [a.reshape(-1, 128) for a in (master_proj, moment_proj, second_proj)]
    flat_e = [a.reshape(-1, 128) for a in (master_embed, moment_embed, squared_moment_layer)]
    anywhere = pl.BlockSpec(memory_space=pl.ANY)
    large = pl.BlockSpec(memory_space=pltpu.HBM)
    vmem = pl.BlockSpec(memory_space=pltpu.VMEM)
    shape = jax.ShapeDtypeStruct
    results = (
        shape((512, 1152), BF16), shape((2, 1152), BF16), shape((81, 128), F32),
        shape((18, 128), F32), shape((81, 128), F32), shape((18, 128), F32), shape((1, 128), F32),
    )
    inside = pl.pallas_call(
        kernel,
        out_shape=[pltpu.VMEM(r.shape, r.dtype) for r in results],
        in_specs=[large] * 12,
        out_specs=[vmem] * 7,
        scratch_shapes=list(SCRATCH.values()),
        compiler_params=pltpu.CompilerParams(
            collective_id=0, has_side_effects=True, vmem_limit_bytes=60 * 2**20
        ),
        name="step",
    )(attended, proj_cot, attended_next, *flat, *flat_e, timesteps, timesteps_next, embed_cot)
    nproj, nembed, d, de, m, mste, norm = pl.pallas_call(
        write_out,
        out_shape=results,
        in_specs=[vmem] * 7,
        out_specs=[large] * 7,
        scratch_shapes=[DMA((7,))],
        compiler_params=pltpu.CompilerParams(vmem_limit_bytes=8 * 2**20),
        name="write_out",
    )(*inside)
    return (
        nproj, nembed, d.reshape(-1), de.reshape(-1), m.reshape(-1), mste.reshape(-1), norm[0, 0],
    )


def solution(mesh):
    finer = Mesh(mesh.devices.reshape(4, 4, 4, 2), AXES)
    dp = P(AXES)
    wide = P(AXES, None)
    return jax.shard_map(
        shards,
        mesh=finer,
        in_specs=(wide, wide, dp, wide, dp, dp, dp, dp, dp, dp, wide, dp),
        out_specs=(wide, wide, dp, dp, dp, dp, P()),
        check_vma=False,
    )
```

```python
import functools
import math

import jax
import jax.numpy as jnp
from jax import lax
from jax.experimental import pallas as pl
from jax.experimental.pallas import tpu as pltpu
from jax.sharding import Mesh
from jax.sharding import PartitionSpec as P

AXES = ("z", "y", "x", "c")
MESH = pl.DeviceIdType.MESH
F32 = jnp.float32
BF16 = jnp.bfloat16

beta_one = 0.9
beta_two = 0.999
step_count = 1000.0
learn_rate = 0.0001
shrink_factor = 0.01
epsilon = 1e-08
max_norm = 1.0

TILES = 9
MINE = {0: (0, 5), 1: (5, 4)}
UNITS = {
    0: ((0, 0, 1), (1, 1, 1), (2, 2, 1), (0, 3, 1), (1, 4, 1)),
    1: ((0, 0, 1), (1, 1, 1), (2, 2, 1), (2, 3, 1)),
}
E = 5
AROUND = [
    (a, b, c) for a in (2, 1, 3, 0) for b in (2, 1, 3, 0) for c in (2, 1, 3, 0) if (a, b, c) != (0, 0, 0)
]
FAR = [(a, b) for a in (2, 1, 3, 0) for b in (2, 1, 3, 0) if (a, b) != (0, 0)]
EUNIT = {0: (0, 0, 5), 1: (0, 0, 4)}
SLOTS = 5
PHASES = False


def adamw_update(gradient, clip, master, moment, second):
    scaled = clip * gradient
    first_new = beta_one * moment + (1.0 - beta_one) * scaled
    second_new = beta_two * second + (1.0 - beta_two) * scaled * scaled
    first_hat = first_new / (1.0 - beta_one**step_count)
    second_hat = second_new / (1.0 - beta_two**step_count)
    direction = first_hat / (jnp.sqrt(second_hat) + epsilon)
    freshened_values = master - learn_rate * (direction + shrink_factor * master)
    return (direction, freshened_values)


def body(core, hbm, outs, sc):
    (att_h, cot_h, nxt_h, mp_h, op_h, sp_h, me_h, oe_h, se_h, tn_h, tx_h, ec_h) = hbm
    (o_np, o_ne, o_dir, o_dire, o_mst, o_mste, o_norm) = outs
    s = sc
    pos = [lax.axis_index(a) for a in AXES]
    other = 1 - core
    first, count = MINE[core]
    ofirst, ocount = MINE[other]
    units = UNITS[core]
    eunit = EUNIT[core]

    def at(axis, d):
        spot = list(pos)
        spot[axis] = lax.rem(pos[axis] + d, 4)
        return spot

    def in_plane(q, a, b):
        i, j = [k for k in range(3) if k != q]
        spot = list(pos)
        spot[i] = lax.rem(pos[i] + a, 4)
        spot[j] = lax.rem(pos[j] + b, 4)
        return spot

    def plane_of(q, spot):
        return [spot[k] for k in range(3) if k != q]

    def cut(q, p):
        index = [slice(None)] * 3
        index[q] = p
        return tuple(index)

    partner = tuple(pos[:3]) + (other,)

    def remote(src, dst, send, recv, spot):
        copy = pltpu.make_async_remote_copy(
            src_ref=src, dst_ref=dst, send_sem=send, recv_sem=recv,
            device_id=tuple(spot), device_id_type=MESH,
        )
        copy.start()

    def got(ref, sem):
        pltpu.make_async_remote_copy(
            src_ref=ref, dst_ref=ref, send_sem=sem, recv_sem=sem,
            device_id=partner, device_id_type=MESH,
        ).wait_recv()

    def sent(ref, sem):
        pltpu.make_async_remote_copy(
            src_ref=ref, dst_ref=ref, send_sem=sem, recv_sem=sem,
            device_id=partner, device_id_type=MESH,
        ).wait_send()

    phase = Phase()
    phase("start")
    def load(src, dst, k):
        pltpu.make_async_copy(src, dst, s.load_sem.at[k]).start()

    def loaded(ref, k):
        pltpu.make_async_copy(ref, ref, s.load_sem.at[k]).wait()

    load(tn_h, s.now, 0)
    load(tx_h, s.later, 1)
    load(ec_h, s.ecot, 2)
    load(att_h, s.att, 3)
    load(cot_h, s.cot, 4)

    phase("signal")
    barrier = pltpu.get_barrier_semaphore()
    around = [
        tuple(lax.rem(pos[k] + d[k], 4) for k in range(3)) + (pos[3],) for d in AROUND
    ]
    beside = [tuple(at(0, d)[:3]) + (c,) for d in range(4) for c in (core, other)][1:]
    everyone = around + [spot for spot in beside if spot[3] == other]
    for spot in everyone:
        pl.semaphore_signal(barrier, inc=1, device_id=spot, device_id_type=MESH)

    def paired(tiles):
        return [tiles[k : k + 2] for k in range(0, len(tiles), 2)]

    def terms(tiles):
        cols = s.cot[:, tiles[0] * 128 : (tiles[-1] + 1) * 128]
        return [
            jnp.dot(s.attT[h * 576 : h * 576 + 576, :], cols, preferred_element_type=F32)
            for h in range(2)
        ]

    phase("freqs")
    loaded(s.now, 0)
    loaded(s.later, 1)
    loaded(s.ecot, 2)
    ladder = lax.broadcasted_iota(jnp.int32, (8, 128), 1).astype(F32)
    line = lax.broadcasted_iota(jnp.int32, (8, 128), 0)
    freqs = jnp.exp(-math.log(10000.0) * ladder / 128)
    moments = jnp.where(
        line == 0, s.now[0], jnp.where(line == 1, s.now[1], jnp.where(line == 2, s.later[0], s.later[1]))
    )
    phases = (moments * 1000.0) * freqs
    waves = [jnp.cos(phases), jnp.sin(phases)]
    slot = pos[0] * 2 + core
    for k in range(TILES):
        s.eb[k, slot] = s.ecot[:, k * 128 : k * 128 + 128]
    for k in range(2):
        s.eb[TILES + k, slot] = waves[k][0:2].astype(BF16)
        s.eb[TILES + 2 + k, slot] = waves[k][2:4].astype(BF16)
    s.wz[...] = jnp.zeros(s.wz.shape, BF16)

    phase("load")
    loaded(s.att, 3)
    s.attT[...] = jnp.transpose(s.att[...], (1, 0))
    loaded(s.cot, 4)
    for k, src in enumerate((mp_h, op_h, sp_h)):
        load(src, s.st.at[core, k], 5)
    for k, src in enumerate((me_h, oe_h, se_h)):
        load(src, s.ste.at[core, k], 6)
    load(nxt_h, s.nxt, 7)

    for k, tiles in enumerate(paired(list(range(ofirst, ofirst + ocount)))):
        phase(f"partner_terms{k}")
        parts = terms(tiles)
        for i, t in enumerate(tiles):
            for h in range(2):
                s.ps[t - ofirst, h * 576 : h * 576 + 576] = parts[h][:, i * 128 : i * 128 + 128].astype(BF16)
        if k == 0:
            phase("barrier")
            pl.semaphore_wait(barrier, len(everyone))
            for spot in beside:
                remote(s.eb.at[:, slot], s.eb.at[:, slot], s.dsend.at[2], s.drecv.at[2], spot)
        for t in tiles:
            remote(s.ps.at[t - ofirst], s.pr.at[t - ofirst], s.psend, s.recvc.at[t - ofirst], partner)
    for k, src in enumerate((mp_h, op_h, sp_h)):
        remote(src, s.st.at[core, k], s.dsend.at[0], s.drecv.at[0], partner)
    for k, src in enumerate((me_h, oe_h, se_h)):
        remote(src, s.ste.at[core, k], s.dsend.at[1], s.drecv.at[1], partner)

    x2 = s.x.reshape(SLOTS, 1152, 128)

    def stage_one(u, x, r1, q, j0, n):
        for d in (1, 3, 2):
            spot = at(q, d)
            remote(
                x.at[(pl.ds(j0, n),) + cut(q, spot[q])],
                r1.at[pl.ds(j0, n), d],
                s.senda.at[int(u == E)], s.recva.at[u], spot,
            )

    def keep_one(x, r1, q, j0, n):
        for j in range(j0, j0 + n):
            r1[j, 0] = x[(j,) + cut(q, pos[q])]

    for tiles in paired(list(range(first, first + count))):
        phase(f"own_terms{tiles[0] - first}")
        parts = terms(tiles)
        for i, t in enumerate(tiles):
            j = t - first
            got(s.pr.at[j], s.recvc.at[j])
            for h in range(2):
                part = parts[h][:, i * 128 : i * 128 + 128]
                x2[j, h * 576 : h * 576 + 576] = (part + s.pr[j, h * 576 : h * 576 + 576].astype(F32)).astype(BF16)
            stage_one(j, s.x, s.r1, *units[j])

    phase("keep")
    for unit in units:
        keep_one(s.x, s.r1, *unit)

    phase("embed")
    ev = s.eb.reshape(TILES + 4, 16, 128)
    y2e = s.yE.reshape(SLOTS, 64, 128)
    got(s.eb.at[:, pl.ds(0, 7)], s.drecv.at[2])
    s.ef[:, 0 : count * 128] = lax.dot_general(
        jnp.concatenate([ev[TILES], ev[TILES + 1]], axis=1),
        jnp.concatenate([ev[first + j] for j in range(count)], axis=1),
        (((0,), (0,)), ((), ())), preferred_element_type=F32,
    )
    slab = pl.ds(pl.multiple_of(pos[0] * 64, 64), 64)
    for j in range(count):
        y2e[j] = s.ef[slab, j * 128 : j * 128 + 128].astype(BF16)

    phase("state")
    loaded(s.st.at[core], 5)
    loaded(s.ste.at[core], 6)
    got(s.st.at[other], s.drecv.at[0])
    got(s.ste.at[other], s.drecv.at[1])
    for k in range(3):
        for j in range(count):
            t = first + j
            for half in range(2):
                s.reg[k, j, 9 * half : 9 * half + 9] = s.st[half, k, pl.ds(t, 9, stride=9), :]
                s.regE[k, j, 2 * half : 2 * half + 2] = s.ste[half, k, pl.ds(t, 2, stride=9), :]

    r1v = s.r1.reshape(SLOTS, 4, 288, 128)
    y2 = s.y.reshape(SLOTS, 288, 128)

    def ring_sum(u, q, j0, n):
        got(s.r1.at[pl.ds(j0, n), pl.ds(1, 3)], s.recva.at[u])
        for j in range(j0, j0 + n):
            total = r1v[j, 0].astype(F32)
            for d in (1, 2, 3):
                total = total + r1v[j, d].astype(F32)
            y2[j] = total.astype(BF16)

    def stage_two(u, y, r2, words, q, j0, n):
        for a, b in FAR:
            spot = in_plane(q, a, b)
            p1, p2 = plane_of(q, spot)
            remote(
                y.at[pl.ds(j0, n), p1, p2],
                r2.at[pl.ds(j0, n), a * 4 + b, pl.ds(0, words)],
                s.sendb.at[int(u == E)], s.recvb.at[u], spot,
            )
        p1, p2 = plane_of(q, pos)
        for j in range(j0, j0 + n):
            r2[j, 0, 0:words] = y[j, p1, p2]

    phase("two_e")
    stage_two(E, s.yE, s.r2E, 2, *eunit)
    for u, unit in enumerate(units):
        phase(f"two{u}")
        ring_sum(u, *unit)
        stage_two(u, s.y, s.r2, 9, *unit)

    r2v = s.r2.reshape(SLOTS, 16, 24, 128)
    r2ve = s.r2E.reshape(SLOTS, 16, 8, 128)
    squares = jnp.zeros((24, 128), F32)
    squares_e = jnp.zeros((8, 128), F32)
    for u, (q, j0, n) in enumerate(units):
        phase(f"sum{u}")
        got(s.r2.at[pl.ds(j0, n), pl.ds(1, 15), pl.ds(0, 9)], s.recvb.at[u])
        for j in range(j0, j0 + n):
            total = r2v[j, 0].astype(F32)
            for k in range(1, 16):
                total = total + r2v[j, k].astype(F32)
            s.g[j] = total
            squares = squares + total * total
    phase("sum_e")
    q, j0, n = eunit
    got(s.r2E.at[pl.ds(j0, n), pl.ds(1, 15), pl.ds(0, 2)], s.recvb.at[E])
    for j in range(j0, j0 + n):
        total = r2ve[j, 0].astype(F32)
        for k in range(1, 16):
            total = total + r2ve[j, k].astype(F32)
        s.gE[j] = total
        squares_e = squares_e + total * total

    phase("squares")
    rows = lax.broadcasted_iota(jnp.int32, (24, 128), 0)
    rows_e = lax.broadcasted_iota(jnp.int32, (8, 128), 0)
    squares = jnp.sum(jnp.where(rows < 18, squares, 0.0), axis=0, keepdims=True)
    squares = squares + jnp.sum(jnp.where(rows_e < 4, squares_e, 0.0), axis=0, keepdims=True)
    s.na[core] = squares
    remote(s.na.at[core], s.na.at[core], s.nsend.at[0], s.nrecv.at[0], partner)
    phase("norm_a")
    got(s.na.at[other], s.nrecv.at[0])
    pz, py, px = pos[:3]
    mine = s.nb.at[pz, py, px]
    s.nb[pz, py, px] = s.na[0] + s.na[1]
    for spot in around:
        remote(mine, mine, s.nsend.at[1], s.nrecv.at[1], spot)
    sent(s.st.at[core], s.dsend.at[0])
    sent(s.ste.at[core], s.dsend.at[1])
    sent(s.r1.at[pl.ds(0, count), pl.ds(1, 3)], s.senda.at[0])
    sent(s.r2.at[pl.ds(0, count), pl.ds(1, 15), pl.ds(0, 9)], s.sendb.at[0])
    sent(s.r2E.at[pl.ds(0, count), pl.ds(1, 15), pl.ds(0, 2)], s.sendb.at[1])
    phase("norm_b")
    got(s.nw, s.nrecv.at[1])
    total = s.nb[0, 0, 0]
    for k in range(1, 64):
        total = total + s.nb[k // 16, k // 4 % 4, k % 4]
    grad_norm = jnp.sqrt(jnp.sum(total, axis=1, keepdims=True))
    clip = jnp.minimum(jnp.float32(1.0), max_norm / (grad_norm + 1e-06))
    o_norm[...] = jnp.broadcast_to(grad_norm, (1, 128))

    z2 = s.zz.reshape(SLOTS, 24, 128)
    z2e = s.zE.reshape(SLOTS, 8, 128)

    def update(u, g, reg, zz, z2, dirs, v, words, q, j0, n):
        for j in range(j0, j0 + n):
            direction, fresh = adamw_update(g[j], clip, reg[0, j], reg[1, j], reg[2, j])
            dirs[0, j] = direction
            dirs[1, j] = fresh
            z2[j] = fresh.astype(BF16)
        p1, p2 = plane_of(q, pos)
        for a, b in FAR:
            remote(
                zz.at[pl.ds(j0, n), pl.ds(0, words)],
                v.at[pl.ds(j0, n), p1, p2],
                s.senda.at[int(u == E)], s.recva.at[u], in_plane(q, a, b),
            )
        for j in range(j0, j0 + n):
            v[j, p1, p2] = zz[j, 0:words]

    order = list(range(count)) + [E]
    phase("update")
    for u in order:
        if u == E:
            update(E, s.gE, s.regE, s.zE, z2e, s.dirsE, s.vE, 2, *eunit)
        else:
            update(u, s.g, s.reg, s.zz, z2, s.dirs, s.v, 9, *units[u])

    phase("outs")
    for k in range(2):
        for j in range(count):
            s.os[k, j, 0:9] = s.dirs[k, j, 9 * other : 9 * other + 9]
            s.osE[k, j, 0:2] = s.dirsE[k, j, 2 * other : 2 * other + 2]
    remote(s.os, s.orr, s.dsend.at[0], s.drecv.at[0], partner)
    remote(s.osE, s.orrE, s.dsend.at[1], s.drecv.at[1], partner)
    for k, (out, oute) in enumerate(((o_dir, o_dire), (o_mst, o_mste))):
        for j in range(count):
            out[pl.ds(first + j, 9, stride=9), :] = s.dirs[k, j, 9 * core : 9 * core + 9]
            oute[pl.ds(first + j, 2, stride=9), :] = s.dirsE[k, j, 2 * core : 2 * core + 2]

    def ring(u, q, j0, n):
        got(s.r2.at[pl.ds(j0, n), pl.ds(1, 15), pl.ds(0, 9)], s.recva.at[u])
        place = s.w.at[(pl.ds(first + j0, n),) + cut(q, pos[q])]
        for d in (1, 3, 2):
            remote(s.v.at[pl.ds(j0, n)], place, s.sendb.at[0], s.recvq.at[u, d - 1], at(q, d))
        remote(s.v.at[pl.ds(j0, n)], place, s.sendc.at[0], s.recvc.at[u], partner)
        for j in range(j0, j0 + n):
            s.w[(first + j,) + cut(q, pos[q])] = s.v[j]

    for u in range(count):
        phase(f"ring{u}")
        ring(u, *units[u])

    phase("ring_e")
    got(s.r2E.at[pl.ds(0, count), pl.ds(1, 15), pl.ds(0, 2)], s.recva.at[E])
    v2e = s.vE.reshape(SLOTS, 64, 128)
    for j in range(count):
        s.wz[j, slab] = v2e[j]
    mixed = jnp.dot(
        jnp.concatenate([ev[TILES + 2], ev[TILES + 3]], axis=1),
        jnp.concatenate([s.wz[j] for j in range(count)], axis=1),
        preferred_element_type=F32,
    )
    for k in range(8):
        for j in range(count):
            s.ep[k, j] = mixed[2 * k : 2 * k + 2, j * 128 : j * 128 + 128]
    mine = pl.ds(first, count)
    for spot in beside:
        remote(
            s.ep.at[spot[0] * 2 + spot[3], pl.ds(0, count)], s.er.at[pos[0], mine],
            s.sendc.at[1], s.recvc.at[E], spot,
        )
    for j in range(count):
        s.er[pos[0], first + j] = s.ep[slot, j]

    phase("outs2")
    got(s.orr, s.drecv.at[0])
    got(s.orrE, s.drecv.at[1])
    for k, (out, oute) in enumerate(((o_dir, o_dire), (o_mst, o_mste))):
        for j in range(ocount):
            out[pl.ds(ofirst + j, 9, stride=9), :] = s.orr[k, j, 0:9]
            oute[pl.ds(ofirst + j, 2, stride=9), :] = s.orrE[k, j, 0:2]

    loaded(s.nxt, 7)
    w2 = s.w.reshape(TILES, 1152, 128)

    def own(u):
        phase(f"own{u}")
        q, j0, n = units[u]
        for d in (1, 3, 2):
            got(s.v.at[pl.ds(j0, n)], s.recvq.at[u, d - 1])
            quarter = s.w.at[(pl.ds(first + j0, n),) + cut(q, at(q, 4 - d)[q])]
            remote(quarter, quarter, s.sendc.at[0], s.recvc.at[u], partner)

    def theirs(u):
        phase(f"theirs{u}")
        got(s.w.at[ofirst + u], s.recvc.at[u])

    def product(tiles):
        phase(f"product{tiles[0]}")
        whole = jnp.concatenate([w2[k] for k in tiles], axis=1)
        for h in range(2):
            some = slice(h * 256, h * 256 + 256)
            mixed = jnp.dot(s.nxt[some, :], whole, preferred_element_type=F32).astype(BF16)
            for i, k in enumerate(tiles):
                o_np[some, k * 128 : k * 128 + 128] = mixed[:, i * 128 : i * 128 + 128]

    own(0)
    own(1)
    if core == 1:
        own(2)
    product([first, first + 1])
    for u in range(2 if core == 0 else 3, count):
        own(u)
    if core == 0:
        product([2, 3, 4])
        for u in range(ocount):
            theirs(u)
        product([5, 6, 7, 8])
    else:
        theirs(0)
        theirs(1)
        product([7, 8, 0, 1])
    phase("embed_out")
    got(s.ed.at[pl.ds(0, 3 * count + 4 * ocount)], s.recvc.at[E])
    for k in range(TILES):
        total = s.er[0, k] + s.er[1, k] + s.er[2, k] + s.er[3, k]
        o_ne[:, k * 128 : k * 128 + 128] = total.astype(BF16)
    if core == 1:
        for u in (2, 3, 4):
            theirs(u)
        product([2, 3, 4])

    phase("drain")
    sent(s.eb.at[:, pl.ds(0, 7)], s.dsend.at[2])
    sent(s.os, s.dsend.at[0])
    sent(s.osE, s.dsend.at[1])
    sent(s.ps.at[pl.ds(0, ocount)], s.psend)
    sent(s.na.at[core], s.nsend.at[0])
    sent(s.nw, s.nsend.at[1])
    sent(s.r2.at[pl.ds(0, count), pl.ds(1, 15), pl.ds(0, 9)], s.senda.at[0])
    sent(s.r2E.at[pl.ds(0, count), pl.ds(1, 15), pl.ds(0, 2)], s.senda.at[1])
    sent(s.r1.at[pl.ds(0, count), pl.ds(1, 3)], s.sendb.at[0])
    sent(s.w.at[pl.ds(first, count)], s.sendc.at[0])
    sent(s.ed.at[pl.ds(0, 7 * count)], s.sendc.at[1])
    phase(None)


class Names:
    pass


class Phase:
    def __init__(self):
        self.open = None

    def __call__(self, name):
        if self.open is not None:
            self.open.__exit__(None, None, None)
            self.open = None
        if name is not None and PHASES:
            self.open = jax.named_scope(name)
            self.open.__enter__()


DMA = pltpu.SemaphoreType.DMA
SCRATCH = dict(
    att=pltpu.VMEM((512, 1152), BF16),
    attT=pltpu.VMEM((1152, 512), BF16),
    cot=pltpu.VMEM((512, 1152), BF16),
    nxt=pltpu.VMEM((512, 1152), BF16),
    ecot=pltpu.VMEM((2, 1152), BF16),
    now=pltpu.SMEM((2,), F32),
    later=pltpu.SMEM((2,), F32),
    st=pltpu.VMEM((2, 3, 81, 128), F32),
    ste=pltpu.VMEM((2, 3, 18, 128), F32),
    ps=pltpu.VMEM((SLOTS, 1152, 128), BF16),
    pr=pltpu.VMEM((SLOTS, 1152, 128), BF16),
    x=pltpu.VMEM((SLOTS, 4, 4, 4, 9, 2, 128), BF16),
    r1=pltpu.VMEM((SLOTS, 4, 4, 4, 9, 2, 128), BF16),
    y=pltpu.VMEM((SLOTS, 4, 4, 9, 2, 128), BF16),
    yE=pltpu.VMEM((SLOTS, 4, 4, 2, 2, 128), BF16),
    r2=pltpu.VMEM((SLOTS, 16, 12, 2, 128), BF16),
    r2E=pltpu.VMEM((SLOTS, 16, 4, 2, 128), BF16),
    reg=pltpu.VMEM((3, SLOTS, 24, 128), F32),
    regE=pltpu.VMEM((3, SLOTS, 8, 128), F32),
    g=pltpu.VMEM((SLOTS, 24, 128), F32),
    gE=pltpu.VMEM((SLOTS, 8, 128), F32),
    dirs=pltpu.VMEM((2, SLOTS, 24, 128), F32),
    dirsE=pltpu.VMEM((2, SLOTS, 8, 128), F32),
    zz=pltpu.VMEM((SLOTS, 12, 2, 128), BF16),
    zE=pltpu.VMEM((SLOTS, 4, 2, 128), BF16),
    v=pltpu.VMEM((SLOTS, 4, 4, 9, 2, 128), BF16),
    vE=pltpu.VMEM((SLOTS, 4, 4, 2, 2, 128), BF16),
    w=pltpu.VMEM((TILES, 4, 4, 4, 9, 2, 128), BF16),
    os=pltpu.VMEM((2, SLOTS, 16, 128), F32),
    osE=pltpu.VMEM((2, SLOTS, 8, 128), F32),
    orr=pltpu.VMEM((2, SLOTS, 16, 128), F32),
    orrE=pltpu.VMEM((2, SLOTS, 8, 128), F32),
    eb=pltpu.VMEM((TILES + 4, 8, 2, 128), BF16),
    ef=pltpu.VMEM((256, 640), F32),
    wz=pltpu.VMEM((SLOTS, 256, 128), BF16),
    ep=pltpu.VMEM((8, SLOTS, 2, 128), F32),
    er=pltpu.VMEM((4, TILES, 2, 128), F32),
    ed=pltpu.VMEM((36, 2, 128), F32),
    na=pltpu.VMEM((2, 1, 128), F32),
    nb=pltpu.VMEM((4, 4, 4, 1, 128), F32),
    nw=pltpu.VMEM((63, 1, 128), F32),
    load_sem=DMA((8,)),
    dsend=DMA((3,)),
    drecv=DMA((3,)),
    psend=DMA(()),
    senda=DMA((2,)),
    sendb=DMA((2,)),
    sendc=DMA((2,)),
    recvq=DMA((5, 3)),
    recva=DMA((6,)),
    recvb=DMA((6,)),
    recvc=DMA((6,)),
    nsend=DMA((2,)),
    nrecv=DMA((2,)),
)


def kernel(*refs):
    hbm, outs, scratch = refs[:12], refs[12:19], refs[19:]
    s = Names()
    for name, ref in zip(SCRATCH, scratch, strict=True):
        setattr(s, name, ref)
    core = lax.axis_index("c")
    for k in (0, 1):

        @pl.when(core == k)
        def _():
            body(k, hbm, outs, s)


def write_out(*refs):
    sems = refs[14]
    copies = [pltpu.make_async_copy(refs[k], refs[7 + k], sems.at[k]) for k in range(7)]
    for copy in copies:
        copy.start()
    for copy in copies:
        copy.wait()


def shards(
    attended, proj_cot, timesteps, embed_cot, master_proj, moment_proj, second_proj,
    master_embed, moment_embed, squared_moment_layer, attended_next, timesteps_next,
):
    flat = [a.reshape(-1, 128) for a in (master_proj, moment_proj, second_proj)]
    flat_e = [a.reshape(-1, 128) for a in (master_embed, moment_embed, squared_moment_layer)]
    anywhere = pl.BlockSpec(memory_space=pl.ANY)
    large = pl.BlockSpec(memory_space=pltpu.HBM)
    vmem = pl.BlockSpec(memory_space=pltpu.VMEM)
    shape = jax.ShapeDtypeStruct
    results = (
        shape((512, 1152), BF16), shape((2, 1152), BF16), shape((81, 128), F32),
        shape((18, 128), F32), shape((81, 128), F32), shape((18, 128), F32), shape((1, 128), F32),
    )
    inside = pl.pallas_call(
        kernel,
        out_shape=[pltpu.VMEM(r.shape, r.dtype) for r in results],
        in_specs=[large] * 12,
        out_specs=[vmem] * 7,
        scratch_shapes=list(SCRATCH.values()),
        compiler_params=pltpu.CompilerParams(
            collective_id=0, has_side_effects=True, vmem_limit_bytes=60 * 2**20
        ),
        name="step",
    )(attended, proj_cot, attended_next, *flat, *flat_e, timesteps, timesteps_next, embed_cot)
    nproj, nembed, d, de, m, mste, norm = pl.pallas_call(
        write_out,
        out_shape=results,
        in_specs=[vmem] * 7,
        out_specs=[large] * 7,
        scratch_shapes=[DMA((7,))],
        compiler_params=pltpu.CompilerParams(vmem_limit_bytes=8 * 2**20),
        name="write_out",
    )(*inside)
    return (
        nproj, nembed, d.reshape(-1), de.reshape(-1), m.reshape(-1), mste.reshape(-1), norm[0, 0],
    )


def solution(mesh):
    finer = Mesh(mesh.devices.reshape(4, 4, 4, 2), AXES)
    dp = P(AXES)
    wide = P(AXES, None)
    return jax.shard_map(
        shards,
        mesh=finer,
        in_specs=(wide, wide, dp, wide, dp, dp, dp, dp, dp, dp, wide, dp),
        out_specs=(wide, wide, dp, dp, dp, dp, P()),
        check_vma=False,
    )
```

```python
import functools
import math

import jax
import jax.numpy as jnp
from jax import lax
from jax.experimental import pallas as pl
from jax.experimental.pallas import tpu as pltpu
from jax.sharding import Mesh
from jax.sharding import PartitionSpec as P

AXES = ("z", "y", "x", "c")
MESH = pl.DeviceIdType.MESH
F32 = jnp.float32
BF16 = jnp.bfloat16

beta_one = 0.9
beta_two = 0.999
step_count = 1000.0
learn_rate = 0.0001
shrink_factor = 0.01
epsilon = 1e-08
max_norm = 1.0

TILES = 9
MINE = {0: (0, 5), 1: (5, 4)}
UNITS = {
    0: ((0, 0, 1), (1, 1, 1), (2, 2, 1), (0, 3, 1), (1, 4, 1)),
    1: ((0, 0, 1), (1, 1, 1), (2, 2, 1), (2, 3, 1)),
}
E = 5
AROUND = [
    (a, b, c) for a in (2, 1, 3, 0) for b in (2, 1, 3, 0) for c in (2, 1, 3, 0) if (a, b, c) != (0, 0, 0)
]
FAR = [(a, b) for a in (2, 1, 3, 0) for b in (2, 1, 3, 0) if (a, b) != (0, 0)]
EUNIT = {0: (0, 0, 5), 1: (0, 0, 4)}
SLOTS = 5
PHASES = False


def adamw_update(gradient, clip, master, moment, second):
    scaled = clip * gradient
    first_new = beta_one * moment + (1.0 - beta_one) * scaled
    second_new = beta_two * second + (1.0 - beta_two) * scaled * scaled
    first_hat = first_new / (1.0 - beta_one**step_count)
    second_hat = second_new / (1.0 - beta_two**step_count)
    direction = first_hat / (jnp.sqrt(second_hat) + epsilon)
    freshened_values = master - learn_rate * (direction + shrink_factor * master)
    return (direction, freshened_values)


def body(core, hbm, outs, sc):
    (att_h, cot_h, nxt_h, mp_h, op_h, sp_h, me_h, oe_h, se_h, tn_h, tx_h, ec_h) = hbm
    (o_np, o_ne, o_dir, o_dire, o_mst, o_mste, o_norm) = outs
    s = sc
    pos = [lax.axis_index(a) for a in AXES]
    other = 1 - core
    first, count = MINE[core]
    ofirst, ocount = MINE[other]
    units = UNITS[core]
    eunit = EUNIT[core]

    def at(axis, d):
        spot = list(pos)
        spot[axis] = lax.rem(pos[axis] + d, 4)
        return spot

    def in_plane(q, a, b):
        i, j = [k for k in range(3) if k != q]
        spot = list(pos)
        spot[i] = lax.rem(pos[i] + a, 4)
        spot[j] = lax.rem(pos[j] + b, 4)
        return spot

    def plane_of(q, spot):
        return [spot[k] for k in range(3) if k != q]

    def cut(q, p):
        index = [slice(None)] * 3
        index[q] = p
        return tuple(index)

    partner = tuple(pos[:3]) + (other,)

    def remote(src, dst, send, recv, spot):
        copy = pltpu.make_async_remote_copy(
            src_ref=src, dst_ref=dst, send_sem=send, recv_sem=recv,
            device_id=tuple(spot), device_id_type=MESH,
        )
        copy.start()

    def got(ref, sem):
        pltpu.make_async_remote_copy(
            src_ref=ref, dst_ref=ref, send_sem=sem, recv_sem=sem,
            device_id=partner, device_id_type=MESH,
        ).wait_recv()

    def sent(ref, sem):
        pltpu.make_async_remote_copy(
            src_ref=ref, dst_ref=ref, send_sem=sem, recv_sem=sem,
            device_id=partner, device_id_type=MESH,
        ).wait_send()

    phase = Phase()
    phase("start")
    def load(src, dst, k):
        pltpu.make_async_copy(src, dst, s.load_sem.at[k]).start()

    def loaded(ref, k):
        pltpu.make_async_copy(ref, ref, s.load_sem.at[k]).wait()

    load(tn_h, s.now, 0)
    load(tx_h, s.later, 1)
    load(ec_h, s.ecot, 2)
    load(att_h, s.att, 3)
    load(cot_h, s.cot, 4)

    phase("signal")
    barrier = pltpu.get_barrier_semaphore()
    around = [
        tuple(lax.rem(pos[k] + d[k], 4) for k in range(3)) + (pos[3],) for d in AROUND
    ]
    beside = [tuple(at(0, d)[:3]) + (c,) for d in range(4) for c in (core, other)][1:]
    everyone = around + [spot for spot in beside if spot[3] == other]
    for spot in everyone:
        pl.semaphore_signal(barrier, inc=1, device_id=spot, device_id_type=MESH)

    def paired(tiles):
        return [tiles[k : k + 2] for k in range(0, len(tiles), 2)]

    def terms(tiles):
        cols = s.cot[:, tiles[0] * 128 : (tiles[-1] + 1) * 128]
        return [
            jnp.dot(s.attT[h * 576 : h * 576 + 576, :], cols, preferred_element_type=F32)
            for h in range(2)
        ]

    phase("freqs")
    loaded(s.now, 0)
    loaded(s.later, 1)
    loaded(s.ecot, 2)
    ladder = lax.broadcasted_iota(jnp.int32, (8, 128), 1).astype(F32)
    line = lax.broadcasted_iota(jnp.int32, (8, 128), 0)
    freqs = jnp.exp(-math.log(10000.0) * ladder / 128)
    moments = jnp.where(
        line == 0, s.now[0], jnp.where(line == 1, s.now[1], jnp.where(line == 2, s.later[0], s.later[1]))
    )
    phases = (moments * 1000.0) * freqs
    waves = [jnp.cos(phases), jnp.sin(phases)]
    slot = pos[0] * 2 + core
    for k in range(TILES):
        s.eb[k, slot] = s.ecot[:, k * 128 : k * 128 + 128]
    for k in range(2):
        s.eb[TILES + k, slot] = waves[k][0:2].astype(BF16)
        s.eb[TILES + 2 + k, slot] = waves[k][2:4].astype(BF16)
    s.wz[...] = jnp.zeros(s.wz.shape, BF16)

    phase("load")
    loaded(s.att, 3)
    s.attT[...] = jnp.transpose(s.att[...], (1, 0))
    loaded(s.cot, 4)
    for k, src in enumerate((mp_h, op_h, sp_h)):
        load(src, s.st.at[core, k], 5)
    for k, src in enumerate((me_h, oe_h, se_h)):
        load(src, s.ste.at[core, k], 6)
    load(nxt_h, s.nxt, 7)

    for k, tiles in enumerate(paired(list(range(ofirst, ofirst + ocount)))):
        phase(f"partner_terms{k}")
        parts = terms(tiles)
        for i, t in enumerate(tiles):
            for h in range(2):
                s.ps[t - ofirst, h * 576 : h * 576 + 576] = parts[h][:, i * 128 : i * 128 + 128].astype(BF16)
        if k == 0:
            phase("barrier")
            pl.semaphore_wait(barrier, len(everyone))
            for spot in beside:
                remote(s.eb.at[:, slot], s.eb.at[:, slot], s.dsend.at[2], s.drecv.at[2], spot)
        for t in tiles:
            remote(s.ps.at[t - ofirst], s.pr.at[t - ofirst], s.psend, s.recvc.at[t - ofirst], partner)
    for k, src in enumerate((mp_h, op_h, sp_h)):
        remote(src, s.st.at[core, k], s.dsend.at[0], s.drecv.at[0], partner)
    for k, src in enumerate((me_h, oe_h, se_h)):
        remote(src, s.ste.at[core, k], s.dsend.at[1], s.drecv.at[1], partner)

    x2 = s.x.reshape(SLOTS, 1152, 128)

    def stage_one(u, x, r1, q, j0, n):
        for d in (1, 3, 2):
            spot = at(q, d)
            remote(
                x.at[(pl.ds(j0, n),) + cut(q, spot[q])],
                r1.at[pl.ds(j0, n), d],
                s.senda.at[int(u == E)], s.recva.at[u], spot,
            )

    def keep_one(x, r1, q, j0, n):
        for j in range(j0, j0 + n):
            r1[j, 0] = x[(j,) + cut(q, pos[q])]

    groups = paired(list(range(first, first + count)))
    parts = {0: terms(groups[0])}
    for g, tiles in enumerate(groups):
        phase(f"own_terms{g}")
        if g + 1 < len(groups):
            parts[g + 1] = terms(groups[g + 1])
        for i, t in enumerate(tiles):
            j = t - first
            got(s.pr.at[j], s.recvc.at[j])
            for h in range(2):
                part = parts[g][h][:, i * 128 : i * 128 + 128]
                x2[j, h * 576 : h * 576 + 576] = (part + s.pr[j, h * 576 : h * 576 + 576].astype(F32)).astype(BF16)
            stage_one(j, s.x, s.r1, *units[j])

    phase("keep")
    for unit in units:
        keep_one(s.x, s.r1, *unit)

    phase("embed")
    ev = s.eb.reshape(TILES + 4, 16, 128)
    y2e = s.yE.reshape(SLOTS, 64, 128)
    got(s.eb.at[:, pl.ds(0, 7)], s.drecv.at[2])
    s.ef[:, 0 : count * 128] = lax.dot_general(
        jnp.concatenate([ev[TILES], ev[TILES + 1]], axis=1),
        jnp.concatenate([ev[first + j] for j in range(count)], axis=1),
        (((0,), (0,)), ((), ())), preferred_element_type=F32,
    )
    slab = pl.ds(pl.multiple_of(pos[0] * 64, 64), 64)
    for j in range(count):
        y2e[j] = s.ef[slab, j * 128 : j * 128 + 128].astype(BF16)

    phase("state")
    loaded(s.st.at[core], 5)
    loaded(s.ste.at[core], 6)
    got(s.st.at[other], s.drecv.at[0])
    got(s.ste.at[other], s.drecv.at[1])
    for k in range(3):
        for j in range(count):
            t = first + j
            for half in range(2):
                s.reg[k, j, 9 * half : 9 * half + 9] = s.st[half, k, pl.ds(t, 9, stride=9), :]
                s.regE[k, j, 2 * half : 2 * half + 2] = s.ste[half, k, pl.ds(t, 2, stride=9), :]

    r1v = s.r1.reshape(SLOTS, 4, 288, 128)
    y2 = s.y.reshape(SLOTS, 288, 128)

    def ring_sum(u, q, j0, n):
        got(s.r1.at[pl.ds(j0, n), pl.ds(1, 3)], s.recva.at[u])
        for j in range(j0, j0 + n):
            total = r1v[j, 0].astype(F32)
            for d in (1, 2, 3):
                total = total + r1v[j, d].astype(F32)
            y2[j] = total.astype(BF16)

    def stage_two(u, y, r2, words, q, j0, n):
        for a, b in FAR:
            spot = in_plane(q, a, b)
            p1, p2 = plane_of(q, spot)
            remote(
                y.at[pl.ds(j0, n), p1, p2],
                r2.at[pl.ds(j0, n), a * 4 + b, pl.ds(0, words)],
                s.sendb.at[int(u == E)], s.recvb.at[u], spot,
            )
        p1, p2 = plane_of(q, pos)
        for j in range(j0, j0 + n):
            r2[j, 0, 0:words] = y[j, p1, p2]

    phase("two_e")
    stage_two(E, s.yE, s.r2E, 2, *eunit)
    for u, unit in enumerate(units):
        phase(f"two{u}")
        ring_sum(u, *unit)
        stage_two(u, s.y, s.r2, 9, *unit)

    r2v = s.r2.reshape(SLOTS, 16, 24, 128)
    r2ve = s.r2E.reshape(SLOTS, 16, 8, 128)
    squares = jnp.zeros((24, 128), F32)
    squares_e = jnp.zeros((8, 128), F32)
    for u, (q, j0, n) in enumerate(units):
        phase(f"sum{u}")
        got(s.r2.at[pl.ds(j0, n), pl.ds(1, 15), pl.ds(0, 9)], s.recvb.at[u])
        for j in range(j0, j0 + n):
            total = r2v[j, 0].astype(F32)
            for k in range(1, 16):
                total = total + r2v[j, k].astype(F32)
            s.g[j] = total
            squares = squares + total * total
    phase("sum_e")
    q, j0, n = eunit
    got(s.r2E.at[pl.ds(j0, n), pl.ds(1, 15), pl.ds(0, 2)], s.recvb.at[E])
    for j in range(j0, j0 + n):
        total = r2ve[j, 0].astype(F32)
        for k in range(1, 16):
            total = total + r2ve[j, k].astype(F32)
        s.gE[j] = total
        squares_e = squares_e + total * total

    phase("squares")
    rows = lax.broadcasted_iota(jnp.int32, (24, 128), 0)
    rows_e = lax.broadcasted_iota(jnp.int32, (8, 128), 0)
    squares = jnp.sum(jnp.where(rows < 18, squares, 0.0), axis=0, keepdims=True)
    squares = squares + jnp.sum(jnp.where(rows_e < 4, squares_e, 0.0), axis=0, keepdims=True)
    s.na[core] = squares
    remote(s.na.at[core], s.na.at[core], s.nsend.at[0], s.nrecv.at[0], partner)
    phase("norm_a")
    got(s.na.at[other], s.nrecv.at[0])
    pz, py, px = pos[:3]
    mine = s.nb.at[pz, py, px]
    s.nb[pz, py, px] = s.na[0] + s.na[1]
    for spot in around:
        remote(mine, mine, s.nsend.at[1], s.nrecv.at[1], spot)
    sent(s.st.at[core], s.dsend.at[0])
    sent(s.ste.at[core], s.dsend.at[1])
    sent(s.r1.at[pl.ds(0, count), pl.ds(1, 3)], s.senda.at[0])
    sent(s.r2.at[pl.ds(0, count), pl.ds(1, 15), pl.ds(0, 9)], s.sendb.at[0])
    sent(s.r2E.at[pl.ds(0, count), pl.ds(1, 15), pl.ds(0, 2)], s.sendb.at[1])
    phase("norm_b")
    got(s.nw, s.nrecv.at[1])
    total = s.nb[0, 0, 0]
    for k in range(1, 64):
        total = total + s.nb[k // 16, k // 4 % 4, k % 4]
    grad_norm = jnp.sqrt(jnp.sum(total, axis=1, keepdims=True))
    clip = jnp.minimum(jnp.float32(1.0), max_norm / (grad_norm + 1e-06))
    o_norm[...] = jnp.broadcast_to(grad_norm, (1, 128))

    z2 = s.zz.reshape(SLOTS, 24, 128)
    z2e = s.zE.reshape(SLOTS, 8, 128)

    def update(u, g, reg, zz, z2, dirs, v, words, q, j0, n):
        for j in range(j0, j0 + n):
            direction, fresh = adamw_update(g[j], clip, reg[0, j], reg[1, j], reg[2, j])
            dirs[0, j] = direction
            dirs[1, j] = fresh
            z2[j] = fresh.astype(BF16)
        p1, p2 = plane_of(q, pos)
        for a, b in FAR:
            remote(
                zz.at[pl.ds(j0, n), pl.ds(0, words)],
                v.at[pl.ds(j0, n), p1, p2],
                s.senda.at[int(u == E)], s.recva.at[u], in_plane(q, a, b),
            )
        for j in range(j0, j0 + n):
            v[j, p1, p2] = zz[j, 0:words]

    order = list(range(count)) + [E]
    phase("update")
    for u in order:
        if u == E:
            update(E, s.gE, s.regE, s.zE, z2e, s.dirsE, s.vE, 2, *eunit)
        else:
            update(u, s.g, s.reg, s.zz, z2, s.dirs, s.v, 9, *units[u])

    phase("outs")
    for k in range(2):
        for j in range(count):
            s.os[k, j, 0:9] = s.dirs[k, j, 9 * other : 9 * other + 9]
            s.osE[k, j, 0:2] = s.dirsE[k, j, 2 * other : 2 * other + 2]
    remote(s.os, s.orr, s.dsend.at[0], s.drecv.at[0], partner)
    remote(s.osE, s.orrE, s.dsend.at[1], s.drecv.at[1], partner)
    for k, (out, oute) in enumerate(((o_dir, o_dire), (o_mst, o_mste))):
        for j in range(count):
            out[pl.ds(first + j, 9, stride=9), :] = s.dirs[k, j, 9 * core : 9 * core + 9]
            oute[pl.ds(first + j, 2, stride=9), :] = s.dirsE[k, j, 2 * core : 2 * core + 2]

    def ring(u, q, j0, n):
        got(s.r2.at[pl.ds(j0, n), pl.ds(1, 15), pl.ds(0, 9)], s.recva.at[u])
        place = s.w.at[(pl.ds(first + j0, n),) + cut(q, pos[q])]
        for d in (1, 3, 2):
            remote(s.v.at[pl.ds(j0, n)], place, s.sendb.at[0], s.recvq.at[u, d - 1], at(q, d))
        remote(s.v.at[pl.ds(j0, n)], place, s.sendc.at[0], s.recvc.at[u], partner)
        for j in range(j0, j0 + n):
            s.w[(first + j,) + cut(q, pos[q])] = s.v[j]

    for u in range(count):
        phase(f"ring{u}")
        ring(u, *units[u])

    phase("ring_e")
    got(s.r2E.at[pl.ds(0, count), pl.ds(1, 15), pl.ds(0, 2)], s.recva.at[E])
    v2e = s.vE.reshape(SLOTS, 64, 128)
    for j in range(count):
        s.wz[j, slab] = v2e[j]
    mixed = jnp.dot(
        jnp.concatenate([ev[TILES + 2], ev[TILES + 3]], axis=1),
        jnp.concatenate([s.wz[j] for j in range(count)], axis=1),
        preferred_element_type=F32,
    )
    for k in range(8):
        for j in range(count):
            s.ep[k, j] = mixed[2 * k : 2 * k + 2, j * 128 : j * 128 + 128]
    mine = pl.ds(first, count)
    for spot in beside:
        remote(
            s.ep.at[spot[0] * 2 + spot[3], pl.ds(0, count)], s.er.at[pos[0], mine],
            s.sendc.at[1], s.recvc.at[E], spot,
        )
    for j in range(count):
        s.er[pos[0], first + j] = s.ep[slot, j]

    phase("outs2")
    got(s.orr, s.drecv.at[0])
    got(s.orrE, s.drecv.at[1])
    for k, (out, oute) in enumerate(((o_dir, o_dire), (o_mst, o_mste))):
        for j in range(ocount):
            out[pl.ds(ofirst + j, 9, stride=9), :] = s.orr[k, j, 0:9]
            oute[pl.ds(ofirst + j, 2, stride=9), :] = s.orrE[k, j, 0:2]

    loaded(s.nxt, 7)
    w2 = s.w.reshape(TILES, 1152, 128)

    def own(u):
        phase(f"own{u}")
        q, j0, n = units[u]
        for d in (1, 3, 2):
            got(s.v.at[pl.ds(j0, n)], s.recvq.at[u, d - 1])
            quarter = s.w.at[(pl.ds(first + j0, n),) + cut(q, at(q, 4 - d)[q])]
            remote(quarter, quarter, s.sendc.at[0], s.recvc.at[u], partner)

    def theirs(u):
        phase(f"theirs{u}")
        got(s.w.at[ofirst + u], s.recvc.at[u])

    def product(tiles):
        phase(f"product{tiles[0]}")
        whole = jnp.concatenate([w2[k] for k in tiles], axis=1)
        for h in range(2):
            some = slice(h * 256, h * 256 + 256)
            mixed = jnp.dot(s.nxt[some, :], whole, preferred_element_type=F32).astype(BF16)
            for i, k in enumerate(tiles):
                o_np[some, k * 128 : k * 128 + 128] = mixed[:, i * 128 : i * 128 + 128]

    def embed_out():
        phase("embed_out")
        got(s.ed.at[pl.ds(0, 3 * count + 4 * ocount)], s.recvc.at[E])
        for k in range(TILES):
            total = s.er[0, k] + s.er[1, k] + s.er[2, k] + s.er[3, k]
            o_ne[:, k * 128 : k * 128 + 128] = total.astype(BF16)

    own(0)
    own(1)
    if core == 0:
        product([0, 1])
        own(3)
        own(4)
        own(2)
        product([2, 3, 4])
        embed_out()
        for u in range(ocount):
            theirs(u)
        product([5, 6, 7, 8])
    else:
        own(2)
        product([5, 6])
        own(3)
        theirs(0)
        theirs(1)
        product([7, 8, 0, 1])
        embed_out()
        theirs(3)
        theirs(4)
        product([3, 4])
        theirs(2)
        product([2])

    phase("drain")
    sent(s.eb.at[:, pl.ds(0, 7)], s.dsend.at[2])
    sent(s.os, s.dsend.at[0])
    sent(s.osE, s.dsend.at[1])
    sent(s.ps.at[pl.ds(0, ocount)], s.psend)
    sent(s.na.at[core], s.nsend.at[0])
    sent(s.nw, s.nsend.at[1])
    sent(s.r2.at[pl.ds(0, count), pl.ds(1, 15), pl.ds(0, 9)], s.senda.at[0])
    sent(s.r2E.at[pl.ds(0, count), pl.ds(1, 15), pl.ds(0, 2)], s.senda.at[1])
    sent(s.r1.at[pl.ds(0, count), pl.ds(1, 3)], s.sendb.at[0])
    sent(s.w.at[pl.ds(first, count)], s.sendc.at[0])
    sent(s.ed.at[pl.ds(0, 7 * count)], s.sendc.at[1])
    phase(None)


class Names:
    pass


class Phase:
    def __init__(self):
        self.open = None

    def __call__(self, name):
        if self.open is not None:
            self.open.__exit__(None, None, None)
            self.open = None
        if name is not None and PHASES:
            self.open = jax.named_scope(name)
            self.open.__enter__()


DMA = pltpu.SemaphoreType.DMA
SCRATCH = dict(
    att=pltpu.VMEM((512, 1152), BF16),
    attT=pltpu.VMEM((1152, 512), BF16),
    cot=pltpu.VMEM((512, 1152), BF16),
    nxt=pltpu.VMEM((512, 1152), BF16),
    ecot=pltpu.VMEM((2, 1152), BF16),
    now=pltpu.SMEM((2,), F32),
    later=pltpu.SMEM((2,), F32),
    st=pltpu.VMEM((2, 3, 81, 128), F32),
    ste=pltpu.VMEM((2, 3, 18, 128), F32),
    ps=pltpu.VMEM((SLOTS, 1152, 128), BF16),
    pr=pltpu.VMEM((SLOTS, 1152, 128), BF16),
    x=pltpu.VMEM((SLOTS, 4, 4, 4, 9, 2, 128), BF16),
    r1=pltpu.VMEM((SLOTS, 4, 4, 4, 9, 2, 128), BF16),
    y=pltpu.VMEM((SLOTS, 4, 4, 9, 2, 128), BF16),
    yE=pltpu.VMEM((SLOTS, 4, 4, 2, 2, 128), BF16),
    r2=pltpu.VMEM((SLOTS, 16, 12, 2, 128), BF16),
    r2E=pltpu.VMEM((SLOTS, 16, 4, 2, 128), BF16),
    reg=pltpu.VMEM((3, SLOTS, 24, 128), F32),
    regE=pltpu.VMEM((3, SLOTS, 8, 128), F32),
    g=pltpu.VMEM((SLOTS, 24, 128), F32),
    gE=pltpu.VMEM((SLOTS, 8, 128), F32),
    dirs=pltpu.VMEM((2, SLOTS, 24, 128), F32),
    dirsE=pltpu.VMEM((2, SLOTS, 8, 128), F32),
    zz=pltpu.VMEM((SLOTS, 12, 2, 128), BF16),
    zE=pltpu.VMEM((SLOTS, 4, 2, 128), BF16),
    v=pltpu.VMEM((SLOTS, 4, 4, 9, 2, 128), BF16),
    vE=pltpu.VMEM((SLOTS, 4, 4, 2, 2, 128), BF16),
    w=pltpu.VMEM((TILES, 4, 4, 4, 9, 2, 128), BF16),
    os=pltpu.VMEM((2, SLOTS, 16, 128), F32),
    osE=pltpu.VMEM((2, SLOTS, 8, 128), F32),
    orr=pltpu.VMEM((2, SLOTS, 16, 128), F32),
    orrE=pltpu.VMEM((2, SLOTS, 8, 128), F32),
    eb=pltpu.VMEM((TILES + 4, 8, 2, 128), BF16),
    ef=pltpu.VMEM((256, 640), F32),
    wz=pltpu.VMEM((SLOTS, 256, 128), BF16),
    ep=pltpu.VMEM((8, SLOTS, 2, 128), F32),
    er=pltpu.VMEM((4, TILES, 2, 128), F32),
    ed=pltpu.VMEM((36, 2, 128), F32),
    na=pltpu.VMEM((2, 1, 128), F32),
    nb=pltpu.VMEM((4, 4, 4, 1, 128), F32),
    nw=pltpu.VMEM((63, 1, 128), F32),
    load_sem=DMA((8,)),
    dsend=DMA((3,)),
    drecv=DMA((3,)),
    psend=DMA(()),
    senda=DMA((2,)),
    sendb=DMA((2,)),
    sendc=DMA((2,)),
    recvq=DMA((5, 3)),
    recva=DMA((6,)),
    recvb=DMA((6,)),
    recvc=DMA((6,)),
    nsend=DMA((2,)),
    nrecv=DMA((2,)),
)


def kernel(*refs):
    hbm, outs, scratch = refs[:12], refs[12:19], refs[19:]
    s = Names()
    for name, ref in zip(SCRATCH, scratch, strict=True):
        setattr(s, name, ref)
    core = lax.axis_index("c")
    for k in (0, 1):

        @pl.when(core == k)
        def _():
            body(k, hbm, outs, s)


def write_out(*refs):
    sems = refs[14]
    copies = [pltpu.make_async_copy(refs[k], refs[7 + k], sems.at[k]) for k in range(7)]
    for copy in copies:
        copy.start()
    for copy in copies:
        copy.wait()


def shards(
    attended, proj_cot, timesteps, embed_cot, master_proj, moment_proj, second_proj,
    master_embed, moment_embed, squared_moment_layer, attended_next, timesteps_next,
):
    flat = [a.reshape(-1, 128) for a in (master_proj, moment_proj, second_proj)]
    flat_e = [a.reshape(-1, 128) for a in (master_embed, moment_embed, squared_moment_layer)]
    anywhere = pl.BlockSpec(memory_space=pl.ANY)
    large = pl.BlockSpec(memory_space=pltpu.HBM)
    vmem = pl.BlockSpec(memory_space=pltpu.VMEM)
    shape = jax.ShapeDtypeStruct
    results = (
        shape((512, 1152), BF16), shape((2, 1152), BF16), shape((81, 128), F32),
        shape((18, 128), F32), shape((81, 128), F32), shape((18, 128), F32), shape((1, 128), F32),
    )
    inside = pl.pallas_call(
        kernel,
        out_shape=[pltpu.VMEM(r.shape, r.dtype) for r in results],
        in_specs=[large] * 12,
        out_specs=[vmem] * 7,
        scratch_shapes=list(SCRATCH.values()),
        compiler_params=pltpu.CompilerParams(
            collective_id=0, has_side_effects=True, vmem_limit_bytes=60 * 2**20
        ),
        name="step",
    )(attended, proj_cot, attended_next, *flat, *flat_e, timesteps, timesteps_next, embed_cot)
    nproj, nembed, d, de, m, mste, norm = pl.pallas_call(
        write_out,
        out_shape=results,
        in_specs=[vmem] * 7,
        out_specs=[large] * 7,
        scratch_shapes=[DMA((7,))],
        compiler_params=pltpu.CompilerParams(vmem_limit_bytes=8 * 2**20),
        name="write_out",
    )(*inside)
    return (
        nproj, nembed, d.reshape(-1), de.reshape(-1), m.reshape(-1), mste.reshape(-1), norm[0, 0],
    )


def solution(mesh):
    finer = Mesh(mesh.devices.reshape(4, 4, 4, 2), AXES)
    dp = P(AXES)
    wide = P(AXES, None)
    return jax.shard_map(
        shards,
        mesh=finer,
        in_specs=(wide, wide, dp, wide, dp, dp, dp, dp, dp, dp, wide, dp),
        out_specs=(wide, wide, dp, dp, dp, dp, P()),
        check_vma=False,
    )
```

```python
import functools
import math

import jax
import jax.numpy as jnp
from jax import lax
from jax.experimental import pallas as pl
from jax.experimental.pallas import tpu as pltpu
from jax.sharding import Mesh
from jax.sharding import PartitionSpec as P

AXES = ("z", "y", "x", "c")
MESH = pl.DeviceIdType.MESH
F32 = jnp.float32
BF16 = jnp.bfloat16

beta_one = 0.9
beta_two = 0.999
step_count = 1000.0
learn_rate = 0.0001
shrink_factor = 0.01
epsilon = 1e-08
max_norm = 1.0

TILES = 9
MINE = {0: (0, 5), 1: (5, 4)}
UNITS = {
    0: ((0, 0, 1), (1, 1, 1), (2, 2, 1), (0, 3, 1), (1, 4, 1)),
    1: ((0, 0, 1), (1, 1, 1), (2, 2, 1), (2, 3, 1)),
}
E = 5
AROUND = [
    (a, b, c) for a in (2, 1, 3, 0) for b in (2, 1, 3, 0) for c in (2, 1, 3, 0) if (a, b, c) != (0, 0, 0)
]
FAR = [(a, b) for a in (2, 1, 3, 0) for b in (2, 1, 3, 0) if (a, b) != (0, 0)]
EUNIT = {0: (0, 0, 5), 1: (0, 0, 4)}
SLOTS = 5
PHASES = False


def adamw_update(gradient, clip, master, moment, second):
    scaled = clip * gradient
    first_new = beta_one * moment + (1.0 - beta_one) * scaled
    second_new = beta_two * second + (1.0 - beta_two) * scaled * scaled
    first_hat = first_new / (1.0 - beta_one**step_count)
    second_hat = second_new / (1.0 - beta_two**step_count)
    direction = first_hat / (jnp.sqrt(second_hat) + epsilon)
    freshened_values = master - learn_rate * (direction + shrink_factor * master)
    return (direction, freshened_values)


def body(core, hbm, outs, sc):
    (att_h, cot_h, nxt_h, mp_h, op_h, sp_h, me_h, oe_h, se_h, tn_h, tx_h, ec_h) = hbm
    (o_np, o_ne, o_dir, o_dire, o_mst, o_mste, o_norm) = outs
    s = sc
    pos = [lax.axis_index(a) for a in AXES]
    other = 1 - core
    first, count = MINE[core]
    ofirst, ocount = MINE[other]
    units = UNITS[core]
    eunit = EUNIT[core]

    def at(axis, d):
        spot = list(pos)
        spot[axis] = lax.rem(pos[axis] + d, 4)
        return spot

    def in_plane(q, a, b):
        i, j = [k for k in range(3) if k != q]
        spot = list(pos)
        spot[i] = lax.rem(pos[i] + a, 4)
        spot[j] = lax.rem(pos[j] + b, 4)
        return spot

    def plane_of(q, spot):
        return [spot[k] for k in range(3) if k != q]

    def cut(q, p):
        index = [slice(None)] * 3
        index[q] = p
        return tuple(index)

    partner = tuple(pos[:3]) + (other,)

    def remote(src, dst, send, recv, spot):
        copy = pltpu.make_async_remote_copy(
            src_ref=src, dst_ref=dst, send_sem=send, recv_sem=recv,
            device_id=tuple(spot), device_id_type=MESH,
        )
        copy.start()

    def got(ref, sem):
        pltpu.make_async_remote_copy(
            src_ref=ref, dst_ref=ref, send_sem=sem, recv_sem=sem,
            device_id=partner, device_id_type=MESH,
        ).wait_recv()

    def sent(ref, sem):
        pltpu.make_async_remote_copy(
            src_ref=ref, dst_ref=ref, send_sem=sem, recv_sem=sem,
            device_id=partner, device_id_type=MESH,
        ).wait_send()

    phase = Phase()
    phase("start")
    def load(src, dst, k):
        pltpu.make_async_copy(src, dst, s.load_sem.at[k]).start()

    def loaded(ref, k):
        pltpu.make_async_copy(ref, ref, s.load_sem.at[k]).wait()

    load(tn_h, s.now, 0)
    load(tx_h, s.later, 1)
    load(ec_h, s.ecot, 2)
    load(att_h, s.att, 3)
    load(cot_h, s.cot, 4)

    phase("signal")
    barrier = pltpu.get_barrier_semaphore()
    around = [
        tuple(lax.rem(pos[k] + d[k], 4) for k in range(3)) + (pos[3],) for d in AROUND
    ]
    beside = [tuple(at(0, d)[:3]) + (c,) for d in range(4) for c in (core, other)][1:]
    everyone = around + [spot for spot in beside if spot[3] == other]
    for spot in everyone:
        pl.semaphore_signal(barrier, inc=1, device_id=spot, device_id_type=MESH)

    def paired(tiles):
        return [tiles[k : k + 2] for k in range(0, len(tiles), 2)]

    def terms(tiles):
        cols = s.cot[:, tiles[0] * 128 : (tiles[-1] + 1) * 128]
        return [
            jnp.dot(s.attT[h * 576 : h * 576 + 576, :], cols, preferred_element_type=F32)
            for h in range(2)
        ]

    phase("freqs")
    loaded(s.now, 0)
    loaded(s.later, 1)
    loaded(s.ecot, 2)
    ladder = lax.broadcasted_iota(jnp.int32, (8, 128), 1).astype(F32)
    line = lax.broadcasted_iota(jnp.int32, (8, 128), 0)
    freqs = jnp.exp(-math.log(10000.0) * ladder / 128)
    moments = jnp.where(
        line == 0, s.now[0], jnp.where(line == 1, s.now[1], jnp.where(line == 2, s.later[0], s.later[1]))
    )
    phases = (moments * 1000.0) * freqs
    waves = [jnp.cos(phases), jnp.sin(phases)]
    slot = pos[0] * 2 + core
    for k in range(TILES):
        s.eb[k, slot] = s.ecot[:, k * 128 : k * 128 + 128]
    for k in range(2):
        s.eb[TILES + k, slot] = waves[k][0:2].astype(BF16)
        s.eb[TILES + 2 + k, slot] = waves[k][2:4].astype(BF16)
    s.wz[...] = jnp.zeros(s.wz.shape, BF16)

    phase("load")
    loaded(s.att, 3)
    s.attT[...] = jnp.transpose(s.att[...], (1, 0))
    loaded(s.cot, 4)
    for k, src in enumerate((mp_h, op_h, sp_h)):
        load(src, s.st.at[core, k], 5)
    for k, src in enumerate((me_h, oe_h, se_h)):
        load(src, s.ste.at[core, k], 6)
    load(nxt_h, s.nxt, 7)

    for k, tiles in enumerate(paired(list(range(ofirst, ofirst + ocount)))):
        phase(f"partner_terms{k}")
        parts = terms(tiles)
        for i, t in enumerate(tiles):
            for h in range(2):
                s.ps[t - ofirst, h * 576 : h * 576 + 576] = parts[h][:, i * 128 : i * 128 + 128].astype(BF16)
        if k == 0:
            phase("barrier")
            pl.semaphore_wait(barrier, len(everyone))
            for spot in beside:
                remote(s.eb.at[:, slot], s.eb.at[:, slot], s.dsend.at[2], s.drecv.at[2], spot)
        for t in tiles:
            remote(s.ps.at[t - ofirst], s.pr.at[t - ofirst], s.psend, s.recvc.at[t - ofirst], partner)
    for k, src in enumerate((mp_h, op_h, sp_h)):
        remote(src, s.st.at[core, k], s.dsend.at[0], s.drecv.at[0], partner)
    for k, src in enumerate((me_h, oe_h, se_h)):
        remote(src, s.ste.at[core, k], s.dsend.at[1], s.drecv.at[1], partner)

    x2 = s.x.reshape(SLOTS, 1152, 128)

    def stage_one(u, x, r1, q, j0, n):
        for d in (1, 3, 2):
            spot = at(q, d)
            remote(
                x.at[(pl.ds(j0, n),) + cut(q, spot[q])],
                r1.at[pl.ds(j0, n), d],
                s.senda.at[int(u == E)], s.recva.at[u], spot,
            )

    def keep_one(x, r1, q, j0, n):
        for j in range(j0, j0 + n):
            r1[j, 0] = x[(j,) + cut(q, pos[q])]

    groups = paired(list(range(first, first + count)))
    parts = {0: terms(groups[0])}
    for g, tiles in enumerate(groups):
        phase(f"own_terms{g}")
        for t in tiles:
            got(s.pr.at[t - first], s.recvc.at[t - first])
        if g + 1 < len(groups):
            parts[g + 1] = terms(groups[g + 1])
        for i, t in enumerate(tiles):
            j = t - first
            for h in range(2):
                part = parts[g][h][:, i * 128 : i * 128 + 128]
                x2[j, h * 576 : h * 576 + 576] = (part + s.pr[j, h * 576 : h * 576 + 576].astype(F32)).astype(BF16)
        for t in tiles:
            stage_one(t - first, s.x, s.r1, *units[t - first])

    phase("keep")
    for unit in units:
        keep_one(s.x, s.r1, *unit)

    phase("embed")
    ev = s.eb.reshape(TILES + 4, 16, 128)
    y2e = s.yE.reshape(SLOTS, 64, 128)
    got(s.eb.at[:, pl.ds(0, 7)], s.drecv.at[2])
    s.ef[:, 0 : count * 128] = lax.dot_general(
        jnp.concatenate([ev[TILES], ev[TILES + 1]], axis=1),
        jnp.concatenate([ev[first + j] for j in range(count)], axis=1),
        (((0,), (0,)), ((), ())), preferred_element_type=F32,
    )
    slab = pl.ds(pl.multiple_of(pos[0] * 64, 64), 64)
    for j in range(count):
        y2e[j] = s.ef[slab, j * 128 : j * 128 + 128].astype(BF16)

    phase("state")
    loaded(s.st.at[core], 5)
    loaded(s.ste.at[core], 6)
    got(s.st.at[other], s.drecv.at[0])
    got(s.ste.at[other], s.drecv.at[1])
    for k in range(3):
        for j in range(count):
            t = first + j
            for half in range(2):
                s.reg[k, j, 9 * half : 9 * half + 9] = s.st[half, k, pl.ds(t, 9, stride=9), :]
                s.regE[k, j, 2 * half : 2 * half + 2] = s.ste[half, k, pl.ds(t, 2, stride=9), :]

    r1v = s.r1.reshape(SLOTS, 4, 288, 128)
    y2 = s.y.reshape(SLOTS, 288, 128)

    def ring_sum(u, q, j0, n):
        got(s.r1.at[pl.ds(j0, n), pl.ds(1, 3)], s.recva.at[u])
        for j in range(j0, j0 + n):
            total = r1v[j, 0].astype(F32)
            for d in (1, 2, 3):
                total = total + r1v[j, d].astype(F32)
            y2[j] = total.astype(BF16)

    def stage_two(u, y, r2, words, q, j0, n):
        for a, b in FAR:
            spot = in_plane(q, a, b)
            p1, p2 = plane_of(q, spot)
            remote(
                y.at[pl.ds(j0, n), p1, p2],
                r2.at[pl.ds(j0, n), a * 4 + b, pl.ds(0, words)],
                s.sendb.at[int(u == E)], s.recvb.at[u], spot,
            )
        p1, p2 = plane_of(q, pos)
        for j in range(j0, j0 + n):
            r2[j, 0, 0:words] = y[j, p1, p2]

    phase("two_e")
    stage_two(E, s.yE, s.r2E, 2, *eunit)
    for u, unit in enumerate(units):
        phase(f"two{u}")
        ring_sum(u, *unit)
        stage_two(u, s.y, s.r2, 9, *unit)

    r2v = s.r2.reshape(SLOTS, 16, 24, 128)
    r2ve = s.r2E.reshape(SLOTS, 16, 8, 128)
    squares = jnp.zeros((24, 128), F32)
    squares_e = jnp.zeros((8, 128), F32)
    phase("sum_e")
    q, j0, n = eunit
    got(s.r2E.at[pl.ds(j0, n), pl.ds(1, 15), pl.ds(0, 2)], s.recvb.at[E])
    for j in range(j0, j0 + n):
        total = r2ve[j, 0].astype(F32)
        for k in range(1, 16):
            total = total + r2ve[j, k].astype(F32)
        s.gE[j] = total
        squares_e = squares_e + total * total

    for u, (q, j0, n) in enumerate(units):
        phase(f"sum{u}")
        got(s.r2.at[pl.ds(j0, n), pl.ds(1, 15), pl.ds(0, 9)], s.recvb.at[u])
        for j in range(j0, j0 + n):
            total = r2v[j, 0].astype(F32)
            for k in range(1, 16):
                total = total + r2v[j, k].astype(F32)
            s.g[j] = total
            squares = squares + total * total
    phase("squares")
    rows = lax.broadcasted_iota(jnp.int32, (24, 128), 0)
    rows_e = lax.broadcasted_iota(jnp.int32, (8, 128), 0)
    squares = jnp.sum(jnp.where(rows < 18, squares, 0.0), axis=0, keepdims=True)
    squares = squares + jnp.sum(jnp.where(rows_e < 4, squares_e, 0.0), axis=0, keepdims=True)
    s.na[core] = squares
    remote(s.na.at[core], s.na.at[core], s.nsend.at[0], s.nrecv.at[0], partner)
    phase("norm_a")
    got(s.na.at[other], s.nrecv.at[0])
    pz, py, px = pos[:3]
    mine = s.nb.at[pz, py, px]
    s.nb[pz, py, px] = s.na[0] + s.na[1]
    for spot in around:
        remote(mine, mine, s.nsend.at[1], s.nrecv.at[1], spot)
    sent(s.st.at[core], s.dsend.at[0])
    sent(s.ste.at[core], s.dsend.at[1])
    sent(s.r1.at[pl.ds(0, count), pl.ds(1, 3)], s.senda.at[0])
    sent(s.r2.at[pl.ds(0, count), pl.ds(1, 15), pl.ds(0, 9)], s.sendb.at[0])
    sent(s.r2E.at[pl.ds(0, count), pl.ds(1, 15), pl.ds(0, 2)], s.sendb.at[1])
    phase("norm_b")
    got(s.nw, s.nrecv.at[1])
    level = [s.nb[k // 16, k // 4 % 4, k % 4] for k in range(64)]
    while len(level) > 1:
        level = [a + b for a, b in zip(level[::2], level[1::2])]
    total = level[0]
    grad_norm = jnp.sqrt(jnp.sum(total, axis=1, keepdims=True))
    clip = jnp.minimum(jnp.float32(1.0), max_norm / (grad_norm + 1e-06))
    o_norm[...] = jnp.broadcast_to(grad_norm, (1, 128))

    z2 = s.zz.reshape(SLOTS, 24, 128)
    z2e = s.zE.reshape(SLOTS, 8, 128)

    def update(u, g, reg, zz, z2, dirs, v, words, q, j0, n):
        for j in range(j0, j0 + n):
            direction, fresh = adamw_update(g[j], clip, reg[0, j], reg[1, j], reg[2, j])
            dirs[0, j] = direction
            dirs[1, j] = fresh
            z2[j] = fresh.astype(BF16)
        p1, p2 = plane_of(q, pos)
        for a, b in FAR:
            remote(
                zz.at[pl.ds(j0, n), pl.ds(0, words)],
                v.at[pl.ds(j0, n), p1, p2],
                s.senda.at[int(u == E)], s.recva.at[u], in_plane(q, a, b),
            )
        for j in range(j0, j0 + n):
            v[j, p1, p2] = zz[j, 0:words]

    order = list(range(count)) + [E]
    phase("update")
    for u in order:
        if u == E:
            update(E, s.gE, s.regE, s.zE, z2e, s.dirsE, s.vE, 2, *eunit)
        else:
            update(u, s.g, s.reg, s.zz, z2, s.dirs, s.v, 9, *units[u])

    phase("outs")
    for k in range(2):
        for j in range(count):
            s.os[k, j, 0:9] = s.dirs[k, j, 9 * other : 9 * other + 9]
            s.osE[k, j, 0:2] = s.dirsE[k, j, 2 * other : 2 * other + 2]
    remote(s.os, s.orr, s.dsend.at[0], s.drecv.at[0], partner)
    remote(s.osE, s.orrE, s.dsend.at[1], s.drecv.at[1], partner)
    for k, (out, oute) in enumerate(((o_dir, o_dire), (o_mst, o_mste))):
        for j in range(count):
            out[pl.ds(first + j, 9, stride=9), :] = s.dirs[k, j, 9 * core : 9 * core + 9]
            oute[pl.ds(first + j, 2, stride=9), :] = s.dirsE[k, j, 2 * core : 2 * core + 2]

    def ring(u, q, j0, n):
        got(s.r2.at[pl.ds(j0, n), pl.ds(1, 15), pl.ds(0, 9)], s.recva.at[u])
        place = s.w.at[(pl.ds(first + j0, n),) + cut(q, pos[q])]
        for d in (1, 3, 2):
            remote(s.v.at[pl.ds(j0, n)], place, s.sendb.at[0], s.recvq.at[u, d - 1], at(q, d))
        remote(s.v.at[pl.ds(j0, n)], place, s.sendc.at[0], s.recvc.at[u], partner)
        for j in range(j0, j0 + n):
            s.w[(first + j,) + cut(q, pos[q])] = s.v[j]

    for u in range(count):
        phase(f"ring{u}")
        ring(u, *units[u])

    phase("ring_e")
    got(s.r2E.at[pl.ds(0, count), pl.ds(1, 15), pl.ds(0, 2)], s.recva.at[E])
    v2e = s.vE.reshape(SLOTS, 64, 128)
    for j in range(count):
        s.wz[j, slab] = v2e[j]
    mixed = jnp.dot(
        jnp.concatenate([ev[TILES + 2], ev[TILES + 3]], axis=1),
        jnp.concatenate([s.wz[j] for j in range(count)], axis=1),
        preferred_element_type=F32,
    )
    for k in range(8):
        for j in range(count):
            s.ep[k, j] = mixed[2 * k : 2 * k + 2, j * 128 : j * 128 + 128]
    mine = pl.ds(first, count)
    for spot in beside:
        remote(
            s.ep.at[spot[0] * 2 + spot[3], pl.ds(0, count)], s.er.at[pos[0], mine],
            s.sendc.at[1], s.recvc.at[E], spot,
        )
    for j in range(count):
        s.er[pos[0], first + j] = s.ep[slot, j]

    phase("outs2")
    got(s.orr, s.drecv.at[0])
    got(s.orrE, s.drecv.at[1])
    for k, (out, oute) in enumerate(((o_dir, o_dire), (o_mst, o_mste))):
        for j in range(ocount):
            out[pl.ds(ofirst + j, 9, stride=9), :] = s.orr[k, j, 0:9]
            oute[pl.ds(ofirst + j, 2, stride=9), :] = s.orrE[k, j, 0:2]

    loaded(s.nxt, 7)
    w2 = s.w.reshape(TILES, 1152, 128)

    def own(u):
        phase(f"own{u}")
        q, j0, n = units[u]
        for d in (1, 3, 2):
            got(s.v.at[pl.ds(j0, n)], s.recvq.at[u, d - 1])
            quarter = s.w.at[(pl.ds(first + j0, n),) + cut(q, at(q, 4 - d)[q])]
            remote(quarter, quarter, s.sendc.at[0], s.recvc.at[u], partner)

    def theirs(u):
        phase(f"theirs{u}")
        got(s.w.at[ofirst + u], s.recvc.at[u])

    def product(tiles):
        phase(f"product{tiles[0]}")
        whole = jnp.concatenate([w2[k] for k in tiles], axis=1)
        halves = 2 if len(tiles) < 3 else 1
        for h in range(halves):
            some = slice(h * 256, h * 256 + 512 // halves)
            mixed = jnp.dot(s.nxt[some, :], whole, preferred_element_type=F32).astype(BF16)
            for i, k in enumerate(tiles):
                o_np[some, k * 128 : k * 128 + 128] = mixed[:, i * 128 : i * 128 + 128]

    def embed_out():
        phase("embed_out")
        got(s.ed.at[pl.ds(0, 3 * count + 4 * ocount)], s.recvc.at[E])
        for k in range(TILES):
            total = s.er[0, k] + s.er[1, k] + s.er[2, k] + s.er[3, k]
            o_ne[:, k * 128 : k * 128 + 128] = total.astype(BF16)

    def many(base, *tiles):
        product([base + k for k in tiles])

    own(0)
    own(1)
    if count == 5:
        many(first, 0, 1)
        theirs(0)
        theirs(1)
        many(ofirst, 0, 1)
        own(3)
        own(4)
        own(2)
        many(first, 2, 3, 4)
        embed_out()
        theirs(2)
        theirs(3)
        many(ofirst, 2, 3)
    else:
        own(2)
        many(first, 0, 1, 2)
        theirs(0)
        theirs(1)
        many(ofirst, 0, 1)
        own(3)
        many(first, 3)
        embed_out()
        theirs(3)
        theirs(4)
        many(ofirst, 3, 4)
        theirs(2)
        many(ofirst, 2)

    phase("drain")
    sent(s.eb.at[:, pl.ds(0, 7)], s.dsend.at[2])
    sent(s.os, s.dsend.at[0])
    sent(s.osE, s.dsend.at[1])
    sent(s.ps.at[pl.ds(0, ocount)], s.psend)
    sent(s.na.at[core], s.nsend.at[0])
    sent(s.nw, s.nsend.at[1])
    sent(s.r2.at[pl.ds(0, count), pl.ds(1, 15), pl.ds(0, 9)], s.senda.at[0])
    sent(s.r2E.at[pl.ds(0, count), pl.ds(1, 15), pl.ds(0, 2)], s.senda.at[1])
    sent(s.r1.at[pl.ds(0, count), pl.ds(1, 3)], s.sendb.at[0])
    sent(s.w.at[pl.ds(first, count)], s.sendc.at[0])
    sent(s.ed.at[pl.ds(0, 7 * count)], s.sendc.at[1])
    phase(None)


class Names:
    pass


class Phase:
    def __init__(self):
        self.open = None

    def __call__(self, name):
        if self.open is not None:
            self.open.__exit__(None, None, None)
            self.open = None
        if name is not None and PHASES:
            self.open = jax.named_scope(name)
            self.open.__enter__()


DMA = pltpu.SemaphoreType.DMA
SCRATCH = dict(
    att=pltpu.VMEM((512, 1152), BF16),
    attT=pltpu.VMEM((1152, 512), BF16),
    cot=pltpu.VMEM((512, 1152), BF16),
    nxt=pltpu.VMEM((512, 1152), BF16),
    ecot=pltpu.VMEM((2, 1152), BF16),
    now=pltpu.SMEM((2,), F32),
    later=pltpu.SMEM((2,), F32),
    st=pltpu.VMEM((2, 3, 81, 128), F32),
    ste=pltpu.VMEM((2, 3, 18, 128), F32),
    ps=pltpu.VMEM((SLOTS, 1152, 128), BF16),
    pr=pltpu.VMEM((SLOTS, 1152, 128), BF16),
    x=pltpu.VMEM((SLOTS, 4, 4, 4, 9, 2, 128), BF16),
    r1=pltpu.VMEM((SLOTS, 4, 4, 4, 9, 2, 128), BF16),
    y=pltpu.VMEM((SLOTS, 4, 4, 9, 2, 128), BF16),
    yE=pltpu.VMEM((SLOTS, 4, 4, 2, 2, 128), BF16),
    r2=pltpu.VMEM((SLOTS, 16, 12, 2, 128), BF16),
    r2E=pltpu.VMEM((SLOTS, 16, 4, 2, 128), BF16),
    reg=pltpu.VMEM((3, SLOTS, 24, 128), F32),
    regE=pltpu.VMEM((3, SLOTS, 8, 128), F32),
    g=pltpu.VMEM((SLOTS, 24, 128), F32),
    gE=pltpu.VMEM((SLOTS, 8, 128), F32),
    dirs=pltpu.VMEM((2, SLOTS, 24, 128), F32),
    dirsE=pltpu.VMEM((2, SLOTS, 8, 128), F32),
    zz=pltpu.VMEM((SLOTS, 12, 2, 128), BF16),
    zE=pltpu.VMEM((SLOTS, 4, 2, 128), BF16),
    v=pltpu.VMEM((SLOTS, 4, 4, 9, 2, 128), BF16),
    vE=pltpu.VMEM((SLOTS, 4, 4, 2, 2, 128), BF16),
    w=pltpu.VMEM((TILES, 4, 4, 4, 9, 2, 128), BF16),
    os=pltpu.VMEM((2, SLOTS, 16, 128), F32),
    osE=pltpu.VMEM((2, SLOTS, 8, 128), F32),
    orr=pltpu.VMEM((2, SLOTS, 16, 128), F32),
    orrE=pltpu.VMEM((2, SLOTS, 8, 128), F32),
    eb=pltpu.VMEM((TILES + 4, 8, 2, 128), BF16),
    ef=pltpu.VMEM((256, 640), F32),
    wz=pltpu.VMEM((SLOTS, 256, 128), BF16),
    ep=pltpu.VMEM((8, SLOTS, 2, 128), F32),
    er=pltpu.VMEM((4, TILES, 2, 128), F32),
    ed=pltpu.VMEM((36, 2, 128), F32),
    na=pltpu.VMEM((2, 1, 128), F32),
    nb=pltpu.VMEM((4, 4, 4, 1, 128), F32),
    nw=pltpu.VMEM((63, 1, 128), F32),
    load_sem=DMA((8,)),
    dsend=DMA((3,)),
    drecv=DMA((3,)),
    psend=DMA(()),
    senda=DMA((2,)),
    sendb=DMA((2,)),
    sendc=DMA((2,)),
    recvq=DMA((5, 3)),
    recva=DMA((6,)),
    recvb=DMA((6,)),
    recvc=DMA((6,)),
    nsend=DMA((2,)),
    nrecv=DMA((2,)),
)


def kernel(*refs):
    hbm, outs, scratch = refs[:12], refs[12:19], refs[19:]
    s = Names()
    for name, ref in zip(SCRATCH, scratch, strict=True):
        setattr(s, name, ref)
    core = lax.axis_index("c")
    for k in (0, 1):

        @pl.when(core == k)
        def _():
            body(k, hbm, outs, s)


def write_out(*refs):
    sems = refs[14]
    copies = [pltpu.make_async_copy(refs[k], refs[7 + k], sems.at[k]) for k in range(7)]
    for copy in copies:
        copy.start()
    for copy in copies:
        copy.wait()


def shards(
    attended, proj_cot, timesteps, embed_cot, master_proj, moment_proj, second_proj,
    master_embed, moment_embed, squared_moment_layer, attended_next, timesteps_next,
):
    flat = [a.reshape(-1, 128) for a in (master_proj, moment_proj, second_proj)]
    flat_e = [a.reshape(-1, 128) for a in (master_embed, moment_embed, squared_moment_layer)]
    anywhere = pl.BlockSpec(memory_space=pl.ANY)
    large = pl.BlockSpec(memory_space=pltpu.HBM)
    vmem = pl.BlockSpec(memory_space=pltpu.VMEM)
    shape = jax.ShapeDtypeStruct
    results = (
        shape((512, 1152), BF16), shape((2, 1152), BF16), shape((81, 128), F32),
        shape((18, 128), F32), shape((81, 128), F32), shape((18, 128), F32), shape((1, 128), F32),
    )
    inside = pl.pallas_call(
        kernel,
        out_shape=[pltpu.VMEM(r.shape, r.dtype) for r in results],
        in_specs=[large] * 12,
        out_specs=[vmem] * 7,
        scratch_shapes=list(SCRATCH.values()),
        compiler_params=pltpu.CompilerParams(
            collective_id=0, has_side_effects=True, vmem_limit_bytes=60 * 2**20
        ),
        name="step",
    )(attended, proj_cot, attended_next, *flat, *flat_e, timesteps, timesteps_next, embed_cot)
    nproj, nembed, d, de, m, mste, norm = pl.pallas_call(
        write_out,
        out_shape=results,
        in_specs=[vmem] * 7,
        out_specs=[large] * 7,
        scratch_shapes=[DMA((7,))],
        compiler_params=pltpu.CompilerParams(vmem_limit_bytes=8 * 2**20),
        name="write_out",
    )(*inside)
    return (
        nproj, nembed, d.reshape(-1), de.reshape(-1), m.reshape(-1), mste.reshape(-1), norm[0, 0],
    )


def solution(mesh):
    finer = Mesh(mesh.devices.reshape(4, 4, 4, 2), AXES)
    dp = P(AXES)
    wide = P(AXES, None)
    return jax.shard_map(
        shards,
        mesh=finer,
        in_specs=(wide, wide, dp, wide, dp, dp, dp, dp, dp, dp, wide, dp),
        out_specs=(wide, wide, dp, dp, dp, dp, P()),
        check_vma=False,
    )
```

```python
import functools
import math

import jax
import jax.numpy as jnp
from jax import lax
from jax.experimental import pallas as pl
from jax.experimental.pallas import tpu as pltpu
from jax.sharding import Mesh
from jax.sharding import PartitionSpec as P

AXES = ("z", "y", "x", "c")
MESH = pl.DeviceIdType.MESH
F32 = jnp.float32
BF16 = jnp.bfloat16

beta_one = 0.9
beta_two = 0.999
step_count = 1000.0
learn_rate = 0.0001
shrink_factor = 0.01
epsilon = 1e-08
max_norm = 1.0

TILES = 9
MINE = {0: (0, 5), 1: (5, 4)}
UNITS = {
    0: ((0, 0, 1), (1, 1, 1), (2, 2, 1), (0, 3, 1), (1, 4, 1)),
    1: ((0, 0, 1), (1, 1, 1), (2, 2, 1), (2, 3, 1)),
}
E = 5
AROUND = [
    (a, b, c) for a in (2, 1, 3, 0) for b in (2, 1, 3, 0) for c in (2, 1, 3, 0) if (a, b, c) != (0, 0, 0)
]
FAR = [(a, b) for a in (2, 1, 3, 0) for b in (2, 1, 3, 0) if (a, b) != (0, 0)]
EUNIT = {0: (0, 0, 5), 1: (0, 0, 4)}
SLOTS = 5
PHASES = False


def adamw_update(gradient, clip, master, moment, second):
    scaled = clip * gradient
    first_new = beta_one * moment + (1.0 - beta_one) * scaled
    second_new = beta_two * second + (1.0 - beta_two) * scaled * scaled
    first_hat = first_new / (1.0 - beta_one**step_count)
    second_hat = second_new / (1.0 - beta_two**step_count)
    direction = first_hat / (jnp.sqrt(second_hat) + epsilon)
    freshened_values = master - learn_rate * (direction + shrink_factor * master)
    return (direction, freshened_values)


def body(core, hbm, outs, sc):
    (att_h, cot_h, nxt_h, mp_h, op_h, sp_h, me_h, oe_h, se_h, tn_h, tx_h, ec_h) = hbm
    (o_np, o_ne, o_dir, o_dire, o_mst, o_mste, o_norm) = outs
    s = sc
    pos = [lax.axis_index(a) for a in AXES]
    other = 1 - core
    first, count = MINE[core]
    ofirst, ocount = MINE[other]
    units = UNITS[core]
    eunit = EUNIT[core]

    def at(axis, d):
        spot = list(pos)
        spot[axis] = lax.rem(pos[axis] + d, 4)
        return spot

    def in_plane(q, a, b):
        i, j = [k for k in range(3) if k != q]
        spot = list(pos)
        spot[i] = lax.rem(pos[i] + a, 4)
        spot[j] = lax.rem(pos[j] + b, 4)
        return spot

    def plane_of(q, spot):
        return [spot[k] for k in range(3) if k != q]

    def cut(q, p):
        index = [slice(None)] * 3
        index[q] = p
        return tuple(index)

    partner = tuple(pos[:3]) + (other,)

    def remote(src, dst, send, recv, spot):
        copy = pltpu.make_async_remote_copy(
            src_ref=src, dst_ref=dst, send_sem=send, recv_sem=recv,
            device_id=tuple(spot), device_id_type=MESH,
        )
        copy.start()

    def got(ref, sem):
        pltpu.make_async_remote_copy(
            src_ref=ref, dst_ref=ref, send_sem=sem, recv_sem=sem,
            device_id=partner, device_id_type=MESH,
        ).wait_recv()

    def sent(ref, sem):
        pltpu.make_async_remote_copy(
            src_ref=ref, dst_ref=ref, send_sem=sem, recv_sem=sem,
            device_id=partner, device_id_type=MESH,
        ).wait_send()

    phase = Phase()
    phase("start")
    def load(src, dst, k):
        pltpu.make_async_copy(src, dst, s.load_sem.at[k]).start()

    def loaded(ref, k):
        pltpu.make_async_copy(ref, ref, s.load_sem.at[k]).wait()

    load(tn_h, s.now, 0)
    load(tx_h, s.later, 1)
    load(ec_h, s.ecot, 2)
    load(att_h, s.att, 3)
    load(cot_h, s.cot, 4)

    phase("signal")
    barrier = pltpu.get_barrier_semaphore()
    around = [
        tuple(lax.rem(pos[k] + d[k], 4) for k in range(3)) + (pos[3],) for d in AROUND
    ]
    beside = [tuple(at(0, d)[:3]) + (c,) for d in range(4) for c in (core, other)][1:]
    rings = [tuple(at(q, d)) for q in range(3) for d in (2, 1, 3)]
    everyone = rings + [spot for spot in beside if spot[3] == other]
    for spot in everyone:
        pl.semaphore_signal(barrier, inc=1, device_id=spot, device_id_type=MESH)

    def paired(tiles):
        return [tiles[k : k + 2] for k in range(0, len(tiles), 2)]

    def terms(tiles):
        cols = s.cot[:, tiles[0] * 128 : (tiles[-1] + 1) * 128]
        return [
            jnp.dot(s.attT[h * 576 : h * 576 + 576, :], cols, preferred_element_type=F32)
            for h in range(2)
        ]

    phase("freqs")
    loaded(s.now, 0)
    loaded(s.later, 1)
    loaded(s.ecot, 2)
    ladder = lax.broadcasted_iota(jnp.int32, (8, 128), 1).astype(F32)
    line = lax.broadcasted_iota(jnp.int32, (8, 128), 0)
    freqs = jnp.exp(-math.log(10000.0) * ladder / 128)
    moments = jnp.where(
        line == 0, s.now[0], jnp.where(line == 1, s.now[1], jnp.where(line == 2, s.later[0], s.later[1]))
    )
    phases = (moments * 1000.0) * freqs
    waves = [jnp.cos(phases), jnp.sin(phases)]
    slot = pos[0] * 2 + core
    for k in range(TILES):
        s.eb[k, slot] = s.ecot[:, k * 128 : k * 128 + 128]
    for k in range(2):
        s.eb[TILES + k, slot] = waves[k][0:2].astype(BF16)
        s.eb[TILES + 2 + k, slot] = waves[k][2:4].astype(BF16)
    s.wz[...] = jnp.zeros(s.wz.shape, BF16)

    phase("load")
    loaded(s.att, 3)
    s.attT[...] = jnp.transpose(s.att[...], (1, 0))
    loaded(s.cot, 4)
    for k, src in enumerate((mp_h, op_h, sp_h)):
        load(src, s.st.at[core, k], 5)
    for k, src in enumerate((me_h, oe_h, se_h)):
        load(src, s.ste.at[core, k], 6)
    load(nxt_h, s.nxt, 7)

    for k, tiles in enumerate(paired(list(range(ofirst, ofirst + ocount)))):
        phase(f"partner_terms{k}")
        parts = terms(tiles)
        for i, t in enumerate(tiles):
            for h in range(2):
                s.ps[t - ofirst, h * 576 : h * 576 + 576] = parts[h][:, i * 128 : i * 128 + 128].astype(BF16)
        if k == 0:
            phase("barrier")
            pl.semaphore_wait(barrier, len(everyone))
            for spot in beside:
                remote(s.eb.at[:, slot], s.eb.at[:, slot], s.dsend.at[2], s.drecv.at[2], spot)
        for t in tiles:
            remote(s.ps.at[t - ofirst], s.pr.at[t - ofirst], s.psend, s.recvc.at[t - ofirst], partner)
    for k, src in enumerate((mp_h, op_h, sp_h)):
        remote(src, s.st.at[core, k], s.dsend.at[0], s.drecv.at[0], partner)
    for k, src in enumerate((me_h, oe_h, se_h)):
        remote(src, s.ste.at[core, k], s.dsend.at[1], s.drecv.at[1], partner)

    x2 = s.x.reshape(SLOTS, 1152, 128)

    def stage_one(u, x, r1, q, j0, n):
        for d in (1, 3, 2):
            spot = at(q, d)
            remote(
                x.at[(pl.ds(j0, n),) + cut(q, spot[q])],
                r1.at[pl.ds(j0, n), d],
                s.senda.at[int(u == E)], s.recva.at[u], spot,
            )

    def keep_one(x, r1, q, j0, n):
        for j in range(j0, j0 + n):
            r1[j, 0] = x[(j,) + cut(q, pos[q])]

    groups = paired(list(range(first, first + count)))
    parts = {0: terms(groups[0])}
    for g, tiles in enumerate(groups):
        phase(f"own_terms{g}")
        for t in tiles:
            got(s.pr.at[t - first], s.recvc.at[t - first])
        if g + 1 < len(groups):
            parts[g + 1] = terms(groups[g + 1])
        for i, t in enumerate(tiles):
            j = t - first
            for h in range(2):
                part = parts[g][h][:, i * 128 : i * 128 + 128]
                x2[j, h * 576 : h * 576 + 576] = (part + s.pr[j, h * 576 : h * 576 + 576].astype(F32)).astype(BF16)
        for t in tiles:
            stage_one(t - first, s.x, s.r1, *units[t - first])

    phase("keep")
    for unit in units:
        keep_one(s.x, s.r1, *unit)

    phase("embed")
    ev = s.eb.reshape(TILES + 4, 16, 128)
    y2e = s.yE.reshape(SLOTS, 64, 128)
    got(s.eb.at[:, pl.ds(0, 7)], s.drecv.at[2])
    s.ef[:, 0 : count * 128] = lax.dot_general(
        jnp.concatenate([ev[TILES], ev[TILES + 1]], axis=1),
        jnp.concatenate([ev[first + j] for j in range(count)], axis=1),
        (((0,), (0,)), ((), ())), preferred_element_type=F32,
    )
    slab = pl.ds(pl.multiple_of(pos[0] * 64, 64), 64)
    for j in range(count):
        y2e[j] = s.ef[slab, j * 128 : j * 128 + 128].astype(BF16)

    phase("state")
    loaded(s.st.at[core], 5)
    loaded(s.ste.at[core], 6)
    got(s.st.at[other], s.drecv.at[0])
    got(s.ste.at[other], s.drecv.at[1])
    for k in range(3):
        for j in range(count):
            t = first + j
            for half in range(2):
                s.reg[k, j, 9 * half : 9 * half + 9] = s.st[half, k, pl.ds(t, 9, stride=9), :]
                s.regE[k, j, 2 * half : 2 * half + 2] = s.ste[half, k, pl.ds(t, 2, stride=9), :]

    r1v = s.r1.reshape(SLOTS, 4, 288, 128)
    y2 = s.y.reshape(SLOTS, 288, 128)

    def ring_sum(u, q, j0, n):
        got(s.r1.at[pl.ds(j0, n), pl.ds(1, 3)], s.recva.at[u])
        for j in range(j0, j0 + n):
            total = r1v[j, 0].astype(F32)
            for d in (1, 2, 3):
                total = total + r1v[j, d].astype(F32)
            y2[j] = total.astype(BF16)

    def stage_two(u, y, r2, words, q, j0, n):
        for a, b in FAR:
            spot = in_plane(q, a, b)
            p1, p2 = plane_of(q, spot)
            remote(
                y.at[pl.ds(j0, n), p1, p2],
                r2.at[pl.ds(j0, n), a * 4 + b, pl.ds(0, words)],
                s.sendb.at[int(u == E)], s.recvb.at[u], spot,
            )
        p1, p2 = plane_of(q, pos)
        for j in range(j0, j0 + n):
            r2[j, 0, 0:words] = y[j, p1, p2]

    for u, unit in enumerate(units):
        phase(f"two{u}")
        ring_sum(u, *unit)
        if u == 1:
            stage_two(0, s.y, s.r2, 9, *units[0])
        if u > 0:
            stage_two(u, s.y, s.r2, 9, *unit)
        if u == 1:
            stage_two(E, s.yE, s.r2E, 2, *eunit)

    r2v = s.r2.reshape(SLOTS, 16, 24, 128)
    r2ve = s.r2E.reshape(SLOTS, 16, 8, 128)
    squares = jnp.zeros((24, 128), F32)
    squares_e = jnp.zeros((8, 128), F32)
    phase("sum_e")
    q, j0, n = eunit
    got(s.r2E.at[pl.ds(j0, n), pl.ds(1, 15), pl.ds(0, 2)], s.recvb.at[E])
    for j in range(j0, j0 + n):
        total = r2ve[j, 0].astype(F32)
        for k in range(1, 16):
            total = total + r2ve[j, k].astype(F32)
        s.gE[j] = total
        squares_e = squares_e + total * total

    for u, (q, j0, n) in enumerate(units):
        phase(f"sum{u}")
        got(s.r2.at[pl.ds(j0, n), pl.ds(1, 15), pl.ds(0, 9)], s.recvb.at[u])
        for j in range(j0, j0 + n):
            total = r2v[j, 0].astype(F32)
            for k in range(1, 16):
                total = total + r2v[j, k].astype(F32)
            s.g[j] = total
            squares = squares + total * total
    phase("squares")
    rows = lax.broadcasted_iota(jnp.int32, (24, 128), 0)
    rows_e = lax.broadcasted_iota(jnp.int32, (8, 128), 0)
    squares = jnp.sum(jnp.where(rows < 18, squares, 0.0), axis=0, keepdims=True)
    squares = squares + jnp.sum(jnp.where(rows_e < 4, squares_e, 0.0), axis=0, keepdims=True)
    s.na[core] = squares
    remote(s.na.at[core], s.na.at[core], s.nsend.at[0], s.nrecv.at[0], partner)
    phase("norm_a")
    got(s.na.at[other], s.nrecv.at[0])
    pz, py, px = pos[:3]
    mine = s.nb.at[pz, py, px]
    s.nb[pz, py, px] = s.na[0] + s.na[1]
    for spot in around:
        remote(mine, mine, s.nsend.at[1], s.nrecv.at[1], spot)
    sent(s.st.at[core], s.dsend.at[0])
    sent(s.ste.at[core], s.dsend.at[1])
    sent(s.r1.at[pl.ds(0, count), pl.ds(1, 3)], s.senda.at[0])
    sent(s.r2.at[pl.ds(0, count), pl.ds(1, 15), pl.ds(0, 9)], s.sendb.at[0])
    sent(s.r2E.at[pl.ds(0, count), pl.ds(1, 15), pl.ds(0, 2)], s.sendb.at[1])
    phase("norm_b")
    got(s.nw, s.nrecv.at[1])
    level = [s.nb[k // 16, k // 4 % 4, k % 4] for k in range(64)]
    while len(level) > 1:
        level = [a + b for a, b in zip(level[::2], level[1::2])]
    total = level[0]
    grad_norm = jnp.sqrt(jnp.sum(total, axis=1, keepdims=True))
    clip = jnp.minimum(jnp.float32(1.0), max_norm / (grad_norm + 1e-06))
    o_norm[...] = jnp.broadcast_to(grad_norm, (1, 128))

    z2 = s.zz.reshape(SLOTS, 24, 128)
    z2e = s.zE.reshape(SLOTS, 8, 128)

    def update(u, g, reg, zz, z2, dirs, v, words, q, j0, n):
        for j in range(j0, j0 + n):
            direction, fresh = adamw_update(g[j], clip, reg[0, j], reg[1, j], reg[2, j])
            dirs[0, j] = direction
            dirs[1, j] = fresh
            z2[j] = fresh.astype(BF16)
        p1, p2 = plane_of(q, pos)
        for a, b in FAR:
            remote(
                zz.at[pl.ds(j0, n), pl.ds(0, words)],
                v.at[pl.ds(j0, n), p1, p2],
                s.senda.at[int(u == E)], s.recva.at[u], in_plane(q, a, b),
            )
        for j in range(j0, j0 + n):
            v[j, p1, p2] = zz[j, 0:words]

    order = list(range(count)) + [E]
    phase("update")
    for u in order:
        if u == E:
            update(E, s.gE, s.regE, s.zE, z2e, s.dirsE, s.vE, 2, *eunit)
        else:
            update(u, s.g, s.reg, s.zz, z2, s.dirs, s.v, 9, *units[u])

    phase("outs")
    for k in range(2):
        for j in range(count):
            s.os[k, j, 0:9] = s.dirs[k, j, 9 * other : 9 * other + 9]
            s.osE[k, j, 0:2] = s.dirsE[k, j, 2 * other : 2 * other + 2]
    remote(s.os, s.orr, s.dsend.at[0], s.drecv.at[0], partner)
    remote(s.osE, s.orrE, s.dsend.at[1], s.drecv.at[1], partner)
    for k, (out, oute) in enumerate(((o_dir, o_dire), (o_mst, o_mste))):
        for j in range(count):
            out[pl.ds(first + j, 9, stride=9), :] = s.dirs[k, j, 9 * core : 9 * core + 9]
            oute[pl.ds(first + j, 2, stride=9), :] = s.dirsE[k, j, 2 * core : 2 * core + 2]

    def ring(u, q, j0, n):
        got(s.r2.at[pl.ds(j0, n), pl.ds(1, 15), pl.ds(0, 9)], s.recva.at[u])
        place = s.w.at[(pl.ds(first + j0, n),) + cut(q, pos[q])]
        for d in (1, 3, 2):
            remote(s.v.at[pl.ds(j0, n)], place, s.sendb.at[0], s.recvq.at[u, d - 1], at(q, d))
        remote(s.v.at[pl.ds(j0, n)], place, s.sendc.at[0], s.recvc.at[u], partner)
        for j in range(j0, j0 + n):
            s.w[(first + j,) + cut(q, pos[q])] = s.v[j]

    for u in range(count):
        phase(f"ring{u}")
        ring(u, *units[u])

    phase("ring_e")
    got(s.r2E.at[pl.ds(0, count), pl.ds(1, 15), pl.ds(0, 2)], s.recva.at[E])
    v2e = s.vE.reshape(SLOTS, 64, 128)
    for j in range(count):
        s.wz[j, slab] = v2e[j]
    mixed = jnp.dot(
        jnp.concatenate([ev[TILES + 2], ev[TILES + 3]], axis=1),
        jnp.concatenate([s.wz[j] for j in range(count)], axis=1),
        preferred_element_type=F32,
    )
    for k in range(8):
        for j in range(count):
            s.ep[k, j] = mixed[2 * k : 2 * k + 2, j * 128 : j * 128 + 128]
    mine = pl.ds(first, count)
    for spot in beside:
        remote(
            s.ep.at[spot[0] * 2 + spot[3], pl.ds(0, count)], s.er.at[pos[0], mine],
            s.sendc.at[1], s.recvc.at[E], spot,
        )
    for j in range(count):
        s.er[pos[0], first + j] = s.ep[slot, j]

    phase("outs2")
    got(s.orr, s.drecv.at[0])
    got(s.orrE, s.drecv.at[1])
    for k, (out, oute) in enumerate(((o_dir, o_dire), (o_mst, o_mste))):
        for j in range(ocount):
            out[pl.ds(ofirst + j, 9, stride=9), :] = s.orr[k, j, 0:9]
            oute[pl.ds(ofirst + j, 2, stride=9), :] = s.orrE[k, j, 0:2]

    loaded(s.nxt, 7)
    w2 = s.w.reshape(TILES, 1152, 128)

    def own(u):
        phase(f"own{u}")
        q, j0, n = units[u]
        for d in (1, 3, 2):
            got(s.v.at[pl.ds(j0, n)], s.recvq.at[u, d - 1])
            quarter = s.w.at[(pl.ds(first + j0, n),) + cut(q, at(q, 4 - d)[q])]
            remote(quarter, quarter, s.sendc.at[0], s.recvc.at[u], partner)

    def theirs(u):
        phase(f"theirs{u}")
        got(s.w.at[ofirst + u], s.recvc.at[u])

    def product(tiles):
        phase(f"product{tiles[0]}")
        whole = jnp.concatenate([w2[k] for k in tiles], axis=1)
        halves = 2 if len(tiles) < 3 else 1
        for h in range(halves):
            some = slice(h * 256, h * 256 + 512 // halves)
            mixed = jnp.dot(s.nxt[some, :], whole, preferred_element_type=F32).astype(BF16)
            for i, k in enumerate(tiles):
                o_np[some, k * 128 : k * 128 + 128] = mixed[:, i * 128 : i * 128 + 128]

    def embed_out():
        phase("embed_out")
        got(s.ed.at[pl.ds(0, 3 * count + 4 * ocount)], s.recvc.at[E])
        for k in range(TILES):
            total = s.er[0, k] + s.er[1, k] + s.er[2, k] + s.er[3, k]
            o_ne[:, k * 128 : k * 128 + 128] = total.astype(BF16)

    def many(base, *tiles):
        product([base + k for k in tiles])

    own(0)
    own(1)
    if count == 5:
        many(first, 0, 1)
        theirs(0)
        theirs(1)
        many(ofirst, 0, 1)
        own(3)
        own(4)
        own(2)
        many(first, 2, 3, 4)
        embed_out()
        theirs(2)
        theirs(3)
        many(ofirst, 2, 3)
    else:
        own(2)
        many(first, 0, 1, 2)
        theirs(0)
        theirs(1)
        many(ofirst, 0, 1)
        own(3)
        many(first, 3)
        embed_out()
        theirs(3)
        theirs(4)
        many(ofirst, 3, 4)
        theirs(2)
        many(ofirst, 2)

    phase("drain")
    sent(s.eb.at[:, pl.ds(0, 7)], s.dsend.at[2])
    sent(s.os, s.dsend.at[0])
    sent(s.osE, s.dsend.at[1])
    sent(s.ps.at[pl.ds(0, ocount)], s.psend)
    sent(s.na.at[core], s.nsend.at[0])
    sent(s.nw, s.nsend.at[1])
    sent(s.r2.at[pl.ds(0, count), pl.ds(1, 15), pl.ds(0, 9)], s.senda.at[0])
    sent(s.r2E.at[pl.ds(0, count), pl.ds(1, 15), pl.ds(0, 2)], s.senda.at[1])
    sent(s.r1.at[pl.ds(0, count), pl.ds(1, 3)], s.sendb.at[0])
    sent(s.w.at[pl.ds(first, count)], s.sendc.at[0])
    sent(s.ed.at[pl.ds(0, 7 * count)], s.sendc.at[1])
    phase(None)


class Names:
    pass


class Phase:
    def __init__(self):
        self.open = None

    def __call__(self, name):
        if self.open is not None:
            self.open.__exit__(None, None, None)
            self.open = None
        if name is not None and PHASES:
            self.open = jax.named_scope(name)
            self.open.__enter__()


DMA = pltpu.SemaphoreType.DMA
SCRATCH = dict(
    att=pltpu.VMEM((512, 1152), BF16),
    attT=pltpu.VMEM((1152, 512), BF16),
    cot=pltpu.VMEM((512, 1152), BF16),
    nxt=pltpu.VMEM((512, 1152), BF16),
    ecot=pltpu.VMEM((2, 1152), BF16),
    now=pltpu.SMEM((2,), F32),
    later=pltpu.SMEM((2,), F32),
    st=pltpu.VMEM((2, 3, 81, 128), F32),
    ste=pltpu.VMEM((2, 3, 18, 128), F32),
    ps=pltpu.VMEM((SLOTS, 1152, 128), BF16),
    pr=pltpu.VMEM((SLOTS, 1152, 128), BF16),
    x=pltpu.VMEM((SLOTS, 4, 4, 4, 9, 2, 128), BF16),
    r1=pltpu.VMEM((SLOTS, 4, 4, 4, 9, 2, 128), BF16),
    y=pltpu.VMEM((SLOTS, 4, 4, 9, 2, 128), BF16),
    yE=pltpu.VMEM((SLOTS, 4, 4, 2, 2, 128), BF16),
    r2=pltpu.VMEM((SLOTS, 16, 12, 2, 128), BF16),
    r2E=pltpu.VMEM((SLOTS, 16, 4, 2, 128), BF16),
    reg=pltpu.VMEM((3, SLOTS, 24, 128), F32),
    regE=pltpu.VMEM((3, SLOTS, 8, 128), F32),
    g=pltpu.VMEM((SLOTS, 24, 128), F32),
    gE=pltpu.VMEM((SLOTS, 8, 128), F32),
    dirs=pltpu.VMEM((2, SLOTS, 24, 128), F32),
    dirsE=pltpu.VMEM((2, SLOTS, 8, 128), F32),
    zz=pltpu.VMEM((SLOTS, 12, 2, 128), BF16),
    zE=pltpu.VMEM((SLOTS, 4, 2, 128), BF16),
    v=pltpu.VMEM((SLOTS, 4, 4, 9, 2, 128), BF16),
    vE=pltpu.VMEM((SLOTS, 4, 4, 2, 2, 128), BF16),
    w=pltpu.VMEM((TILES, 4, 4, 4, 9, 2, 128), BF16),
    os=pltpu.VMEM((2, SLOTS, 16, 128), F32),
    osE=pltpu.VMEM((2, SLOTS, 8, 128), F32),
    orr=pltpu.VMEM((2, SLOTS, 16, 128), F32),
    orrE=pltpu.VMEM((2, SLOTS, 8, 128), F32),
    eb=pltpu.VMEM((TILES + 4, 8, 2, 128), BF16),
    ef=pltpu.VMEM((256, 640), F32),
    wz=pltpu.VMEM((SLOTS, 256, 128), BF16),
    ep=pltpu.VMEM((8, SLOTS, 2, 128), F32),
    er=pltpu.VMEM((4, TILES, 2, 128), F32),
    ed=pltpu.VMEM((36, 2, 128), F32),
    na=pltpu.VMEM((2, 1, 128), F32),
    nb=pltpu.VMEM((4, 4, 4, 1, 128), F32),
    nw=pltpu.VMEM((63, 1, 128), F32),
    load_sem=DMA((8,)),
    dsend=DMA((3,)),
    drecv=DMA((3,)),
    psend=DMA(()),
    senda=DMA((2,)),
    sendb=DMA((2,)),
    sendc=DMA((2,)),
    recvq=DMA((5, 3)),
    recva=DMA((6,)),
    recvb=DMA((6,)),
    recvc=DMA((6,)),
    nsend=DMA((2,)),
    nrecv=DMA((2,)),
)


def kernel(*refs):
    hbm, outs, scratch = refs[:12], refs[12:19], refs[19:]
    s = Names()
    for name, ref in zip(SCRATCH, scratch, strict=True):
        setattr(s, name, ref)
    core = lax.axis_index("c")
    for k in (0, 1):

        @pl.when(core == k)
        def _():
            body(k, hbm, outs, s)


def write_out(*refs):
    sems = refs[14]
    copies = [pltpu.make_async_copy(refs[k], refs[7 + k], sems.at[k]) for k in range(7)]
    for copy in copies:
        copy.start()
    for copy in copies:
        copy.wait()


def shards(
    attended, proj_cot, timesteps, embed_cot, master_proj, moment_proj, second_proj,
    master_embed, moment_embed, squared_moment_layer, attended_next, timesteps_next,
):
    flat = [a.reshape(-1, 128) for a in (master_proj, moment_proj, second_proj)]
    flat_e = [a.reshape(-1, 128) for a in (master_embed, moment_embed, squared_moment_layer)]
    anywhere = pl.BlockSpec(memory_space=pl.ANY)
    large = pl.BlockSpec(memory_space=pltpu.HBM)
    vmem = pl.BlockSpec(memory_space=pltpu.VMEM)
    shape = jax.ShapeDtypeStruct
    results = (
        shape((512, 1152), BF16), shape((2, 1152), BF16), shape((81, 128), F32),
        shape((18, 128), F32), shape((81, 128), F32), shape((18, 128), F32), shape((1, 128), F32),
    )
    inside = pl.pallas_call(
        kernel,
        out_shape=[pltpu.VMEM(r.shape, r.dtype) for r in results],
        in_specs=[large] * 12,
        out_specs=[vmem] * 7,
        scratch_shapes=list(SCRATCH.values()),
        compiler_params=pltpu.CompilerParams(
            collective_id=0, has_side_effects=True, vmem_limit_bytes=60 * 2**20
        ),
        name="step",
    )(attended, proj_cot, attended_next, *flat, *flat_e, timesteps, timesteps_next, embed_cot)
    nproj, nembed, d, de, m, mste, norm = pl.pallas_call(
        write_out,
        out_shape=results,
        in_specs=[vmem] * 7,
        out_specs=[large] * 7,
        scratch_shapes=[DMA((7,))],
        compiler_params=pltpu.CompilerParams(vmem_limit_bytes=8 * 2**20),
        name="write_out",
    )(*inside)
    return (
        nproj, nembed, d.reshape(-1), de.reshape(-1), m.reshape(-1), mste.reshape(-1), norm[0, 0],
    )


def solution(mesh):
    finer = Mesh(mesh.devices.reshape(4, 4, 4, 2), AXES)
    dp = P(AXES)
    wide = P(AXES, None)
    return jax.shard_map(
        shards,
        mesh=finer,
        in_specs=(wide, wide, dp, wide, dp, dp, dp, dp, dp, dp, wide, dp),
        out_specs=(wide, wide, dp, dp, dp, dp, P()),
        check_vma=False,
    )
```

```python
import functools
import math

import jax
import jax.numpy as jnp
from jax import lax
from jax.experimental import pallas as pl
from jax.experimental.pallas import tpu as pltpu
from jax.sharding import Mesh
from jax.sharding import PartitionSpec as P

AXES = ("z", "y", "x", "c")
MESH = pl.DeviceIdType.MESH
F32 = jnp.float32
BF16 = jnp.bfloat16

beta_one = 0.9
beta_two = 0.999
step_count = 1000.0
learn_rate = 0.0001
shrink_factor = 0.01
epsilon = 1e-08
max_norm = 1.0

TILES = 9
MINE = {0: (0, 5), 1: (5, 4)}
UNITS = {
    0: ((0, 0, 1), (1, 1, 1), (2, 2, 1), (0, 3, 1), (1, 4, 1)),
    1: ((0, 0, 1), (1, 1, 1), (2, 2, 1), (2, 3, 1)),
}
E = 5
AROUND = [
    (a, b, c) for a in (2, 1, 3, 0) for b in (2, 1, 3, 0) for c in (2, 1, 3, 0) if (a, b, c) != (0, 0, 0)
]
FAR = [(a, b) for a in (2, 1, 3, 0) for b in (2, 1, 3, 0) if (a, b) != (0, 0)]
EUNIT = {0: (0, 0, 5), 1: (0, 0, 4)}
SLOTS = 5
LATE = {0: (7, 8), 1: (2,)}
PHASES = False


def adamw_update(gradient, clip, master, moment, second):
    scaled = clip * gradient
    first_new = beta_one * moment + (1.0 - beta_one) * scaled
    second_new = beta_two * second + (1.0 - beta_two) * scaled * scaled
    first_hat = first_new / (1.0 - beta_one**step_count)
    second_hat = second_new / (1.0 - beta_two**step_count)
    direction = first_hat / (jnp.sqrt(second_hat) + epsilon)
    freshened_values = master - learn_rate * (direction + shrink_factor * master)
    return (direction, freshened_values)


def body(core, hbm, outs, sc):
    (att_h, cot_h, nxt_h, mp_h, op_h, sp_h, me_h, oe_h, se_h, tn_h, tx_h, ec_h) = hbm
    (o_np, o_ne, o_dir, o_dire, o_mst, o_mste, o_norm) = outs[:7]
    s = sc
    pos = [lax.axis_index(a) for a in AXES]
    other = 1 - core
    first, count = MINE[core]
    ofirst, ocount = MINE[other]
    units = UNITS[core]
    eunit = EUNIT[core]

    def at(axis, d):
        spot = list(pos)
        spot[axis] = lax.rem(pos[axis] + d, 4)
        return spot

    def in_plane(q, a, b):
        i, j = [k for k in range(3) if k != q]
        spot = list(pos)
        spot[i] = lax.rem(pos[i] + a, 4)
        spot[j] = lax.rem(pos[j] + b, 4)
        return spot

    def plane_of(q, spot):
        return [spot[k] for k in range(3) if k != q]

    def cut(q, p):
        index = [slice(None)] * 3
        index[q] = p
        return tuple(index)

    partner = tuple(pos[:3]) + (other,)

    def remote(src, dst, send, recv, spot):
        copy = pltpu.make_async_remote_copy(
            src_ref=src, dst_ref=dst, send_sem=send, recv_sem=recv,
            device_id=tuple(spot), device_id_type=MESH,
        )
        copy.start()

    def got(ref, sem):
        pltpu.make_async_remote_copy(
            src_ref=ref, dst_ref=ref, send_sem=sem, recv_sem=sem,
            device_id=partner, device_id_type=MESH,
        ).wait_recv()

    def sent(ref, sem):
        pltpu.make_async_remote_copy(
            src_ref=ref, dst_ref=ref, send_sem=sem, recv_sem=sem,
            device_id=partner, device_id_type=MESH,
        ).wait_send()

    phase = Phase()
    phase("start")
    def load(src, dst, k):
        pltpu.make_async_copy(src, dst, s.load_sem.at[k]).start()

    def loaded(ref, k):
        pltpu.make_async_copy(ref, ref, s.load_sem.at[k]).wait()

    load(tn_h, s.now, 0)
    load(tx_h, s.later, 1)
    load(ec_h, s.ecot, 2)
    load(att_h, s.att, 3)
    load(cot_h, s.cot, 4)

    phase("signal")
    barrier = pltpu.get_barrier_semaphore()
    around = [
        tuple(lax.rem(pos[k] + d[k], 4) for k in range(3)) + (pos[3],) for d in AROUND
    ]
    beside = [tuple(at(0, d)[:3]) + (c,) for d in range(4) for c in (core, other)][1:]
    rings = [tuple(at(q, d)) for q in range(3) for d in (2, 1, 3)]
    everyone = rings + [spot for spot in beside if spot[3] == other]
    for spot in everyone:
        pl.semaphore_signal(barrier, inc=1, device_id=spot, device_id_type=MESH)

    def paired(tiles):
        return [tiles[k : k + 2] for k in range(0, len(tiles), 2)]

    def terms(tiles):
        cols = s.cot[:, tiles[0] * 128 : (tiles[-1] + 1) * 128]
        return [
            jnp.dot(s.attT[h * 576 : h * 576 + 576, :], cols, preferred_element_type=F32)
            for h in range(2)
        ]

    phase("freqs")
    loaded(s.now, 0)
    loaded(s.later, 1)
    loaded(s.ecot, 2)
    ladder = lax.broadcasted_iota(jnp.int32, (8, 128), 1).astype(F32)
    line = lax.broadcasted_iota(jnp.int32, (8, 128), 0)
    freqs = jnp.exp(-math.log(10000.0) * ladder / 128)
    moments = jnp.where(
        line == 0, s.now[0], jnp.where(line == 1, s.now[1], jnp.where(line == 2, s.later[0], s.later[1]))
    )
    phases = (moments * 1000.0) * freqs
    waves = [jnp.cos(phases), jnp.sin(phases)]
    slot = pos[0] * 2 + core
    for k in range(TILES):
        s.eb[k, slot] = s.ecot[:, k * 128 : k * 128 + 128]
    for k in range(2):
        s.eb[TILES + k, slot] = waves[k][0:2].astype(BF16)
        s.eb[TILES + 2 + k, slot] = waves[k][2:4].astype(BF16)
    s.wz[...] = jnp.zeros(s.wz.shape, BF16)

    phase("load")
    loaded(s.att, 3)
    s.attT[...] = jnp.transpose(s.att[...], (1, 0))
    loaded(s.cot, 4)
    for k, src in enumerate((mp_h, op_h, sp_h)):
        load(src, s.st.at[core, k], 5)
    for k, src in enumerate((me_h, oe_h, se_h)):
        load(src, s.ste.at[core, k], 6)
    load(nxt_h, s.nxt, 7)

    for k, tiles in enumerate(paired(list(range(ofirst, ofirst + ocount)))):
        phase(f"partner_terms{k}")
        parts = terms(tiles)
        for i, t in enumerate(tiles):
            for h in range(2):
                s.ps[t - ofirst, h * 576 : h * 576 + 576] = parts[h][:, i * 128 : i * 128 + 128].astype(BF16)
        if k == 0:
            phase("barrier")
            pl.semaphore_wait(barrier, len(everyone))
            for spot in beside:
                remote(s.eb.at[:, slot], s.eb.at[:, slot], s.dsend.at[2], s.drecv.at[2], spot)
        for t in tiles:
            remote(s.ps.at[t - ofirst], s.pr.at[t - ofirst], s.psend, s.recvc.at[t - ofirst], partner)
    for k, src in enumerate((mp_h, op_h, sp_h)):
        remote(src, s.st.at[core, k], s.dsend.at[0], s.drecv.at[0], partner)
    for k, src in enumerate((me_h, oe_h, se_h)):
        remote(src, s.ste.at[core, k], s.dsend.at[1], s.drecv.at[1], partner)

    x2 = s.x.reshape(SLOTS, 1152, 128)

    def stage_one(u, x, r1, q, j0, n):
        for d in (1, 3, 2):
            spot = at(q, d)
            remote(
                x.at[(pl.ds(j0, n),) + cut(q, spot[q])],
                r1.at[pl.ds(j0, n), d],
                s.senda.at[int(u == E)], s.recva.at[u], spot,
            )

    def keep_one(x, r1, q, j0, n):
        for j in range(j0, j0 + n):
            r1[j, 0] = x[(j,) + cut(q, pos[q])]

    groups = paired(list(range(first, first + count)))
    parts = {0: terms(groups[0])}
    for g, tiles in enumerate(groups):
        phase(f"own_terms{g}")
        for t in tiles:
            got(s.pr.at[t - first], s.recvc.at[t - first])
        if g + 1 < len(groups):
            parts[g + 1] = terms(groups[g + 1])
        for i, t in enumerate(tiles):
            j = t - first
            for h in range(2):
                part = parts[g][h][:, i * 128 : i * 128 + 128]
                x2[j, h * 576 : h * 576 + 576] = (part + s.pr[j, h * 576 : h * 576 + 576].astype(F32)).astype(BF16)
        for t in tiles:
            stage_one(t - first, s.x, s.r1, *units[t - first])

    phase("keep")
    for unit in units:
        keep_one(s.x, s.r1, *unit)

    phase("embed")
    ev = s.eb.reshape(TILES + 4, 16, 128)
    y2e = s.yE.reshape(SLOTS, 64, 128)
    got(s.eb.at[:, pl.ds(0, 7)], s.drecv.at[2])
    s.ef[:, 0 : count * 128] = lax.dot_general(
        jnp.concatenate([ev[TILES], ev[TILES + 1]], axis=1),
        jnp.concatenate([ev[first + j] for j in range(count)], axis=1),
        (((0,), (0,)), ((), ())), preferred_element_type=F32,
    )
    slab = pl.ds(pl.multiple_of(pos[0] * 64, 64), 64)
    for j in range(count):
        y2e[j] = s.ef[slab, j * 128 : j * 128 + 128].astype(BF16)

    phase("state")
    loaded(s.st.at[core], 5)
    loaded(s.ste.at[core], 6)
    got(s.st.at[other], s.drecv.at[0])
    got(s.ste.at[other], s.drecv.at[1])
    for k in range(3):
        for j in range(count):
            t = first + j
            for half in range(2):
                s.reg[k, j, 9 * half : 9 * half + 9] = s.st[half, k, pl.ds(t, 9, stride=9), :]
                s.regE[k, j, 2 * half : 2 * half + 2] = s.ste[half, k, pl.ds(t, 2, stride=9), :]

    r1v = s.r1.reshape(SLOTS, 4, 288, 128)
    y2 = s.y.reshape(SLOTS, 288, 128)

    def ring_sum(u, q, j0, n):
        got(s.r1.at[pl.ds(j0, n), pl.ds(1, 3)], s.recva.at[u])
        for j in range(j0, j0 + n):
            total = r1v[j, 0].astype(F32)
            for d in (1, 2, 3):
                total = total + r1v[j, d].astype(F32)
            y2[j] = total.astype(BF16)

    def stage_two(u, y, r2, words, q, j0, n):
        for a, b in FAR:
            spot = in_plane(q, a, b)
            p1, p2 = plane_of(q, spot)
            remote(
                y.at[pl.ds(j0, n), p1, p2],
                r2.at[pl.ds(j0, n), a * 4 + b, pl.ds(0, words)],
                s.sendb.at[int(u == E)], s.recvb.at[u], spot,
            )
        p1, p2 = plane_of(q, pos)
        for j in range(j0, j0 + n):
            r2[j, 0, 0:words] = y[j, p1, p2]

    for u, unit in enumerate(units):
        phase(f"two{u}")
        ring_sum(u, *unit)
        if u == 1:
            stage_two(0, s.y, s.r2, 9, *units[0])
        if u > 0:
            stage_two(u, s.y, s.r2, 9, *unit)
        if u == 1:
            stage_two(E, s.yE, s.r2E, 2, *eunit)

    r2v = s.r2.reshape(SLOTS, 16, 24, 128)
    r2ve = s.r2E.reshape(SLOTS, 16, 8, 128)
    squares = jnp.zeros((24, 128), F32)
    squares_e = jnp.zeros((8, 128), F32)
    phase("sum_e")
    q, j0, n = eunit
    got(s.r2E.at[pl.ds(j0, n), pl.ds(1, 15), pl.ds(0, 2)], s.recvb.at[E])
    for j in range(j0, j0 + n):
        total = r2ve[j, 0].astype(F32)
        for k in range(1, 16):
            total = total + r2ve[j, k].astype(F32)
        s.gE[j] = total
        squares_e = squares_e + total * total

    for u, (q, j0, n) in enumerate(units):
        phase(f"sum{u}")
        got(s.r2.at[pl.ds(j0, n), pl.ds(1, 15), pl.ds(0, 9)], s.recvb.at[u])
        for j in range(j0, j0 + n):
            total = r2v[j, 0].astype(F32)
            for k in range(1, 16):
                total = total + r2v[j, k].astype(F32)
            s.g[j] = total
            squares = squares + total * total
    phase("squares")
    rows = lax.broadcasted_iota(jnp.int32, (24, 128), 0)
    rows_e = lax.broadcasted_iota(jnp.int32, (8, 128), 0)
    squares = jnp.sum(jnp.where(rows < 18, squares, 0.0), axis=0, keepdims=True)
    squares = squares + jnp.sum(jnp.where(rows_e < 4, squares_e, 0.0), axis=0, keepdims=True)
    s.na[core] = squares
    remote(s.na.at[core], s.na.at[core], s.nsend.at[0], s.nrecv.at[0], partner)
    phase("norm_a")
    got(s.na.at[other], s.nrecv.at[0])
    pz, py, px = pos[:3]
    mine = s.nb.at[pz, py, px]
    s.nb[pz, py, px] = s.na[0] + s.na[1]
    for spot in around:
        remote(mine, mine, s.nsend.at[1], s.nrecv.at[1], spot)
    sent(s.st.at[core], s.dsend.at[0])
    sent(s.ste.at[core], s.dsend.at[1])
    sent(s.r1.at[pl.ds(0, count), pl.ds(1, 3)], s.senda.at[0])
    sent(s.r2.at[pl.ds(0, count), pl.ds(1, 15), pl.ds(0, 9)], s.sendb.at[0])
    sent(s.r2E.at[pl.ds(0, count), pl.ds(1, 15), pl.ds(0, 2)], s.sendb.at[1])
    phase("norm_b")
    got(s.nw, s.nrecv.at[1])
    level = [s.nb[k // 16, k // 4 % 4, k % 4] for k in range(64)]
    while len(level) > 1:
        level = [a + b for a, b in zip(level[::2], level[1::2])]
    total = level[0]
    grad_norm = jnp.sqrt(jnp.sum(total, axis=1, keepdims=True))
    clip = jnp.minimum(jnp.float32(1.0), max_norm / (grad_norm + 1e-06))
    o_norm[...] = jnp.broadcast_to(grad_norm, (1, 128))

    z2 = s.zz.reshape(SLOTS, 24, 128)
    z2e = s.zE.reshape(SLOTS, 8, 128)

    def update(u, g, reg, zz, z2, dirs, v, words, q, j0, n):
        for j in range(j0, j0 + n):
            direction, fresh = adamw_update(g[j], clip, reg[0, j], reg[1, j], reg[2, j])
            dirs[0, j] = direction
            dirs[1, j] = fresh
            z2[j] = fresh.astype(BF16)
        p1, p2 = plane_of(q, pos)
        for a, b in FAR:
            remote(
                zz.at[pl.ds(j0, n), pl.ds(0, words)],
                v.at[pl.ds(j0, n), p1, p2],
                s.senda.at[int(u == E)], s.recva.at[u], in_plane(q, a, b),
            )
        for j in range(j0, j0 + n):
            v[j, p1, p2] = zz[j, 0:words]

    order = list(range(count)) + [E]
    phase("update")
    for u in order:
        if u == E:
            update(E, s.gE, s.regE, s.zE, z2e, s.dirsE, s.vE, 2, *eunit)
        else:
            update(u, s.g, s.reg, s.zz, z2, s.dirs, s.v, 9, *units[u])

    phase("outs")
    for k in range(2):
        for j in range(count):
            s.os[k, j, 0:9] = s.dirs[k, j, 9 * other : 9 * other + 9]
            s.osE[k, j, 0:2] = s.dirsE[k, j, 2 * other : 2 * other + 2]
    remote(s.os, s.orr, s.dsend.at[0], s.drecv.at[0], partner)
    remote(s.osE, s.orrE, s.dsend.at[1], s.drecv.at[1], partner)
    for k, (out, oute) in enumerate(((o_dir, o_dire), (o_mst, o_mste))):
        for j in range(count):
            out[pl.ds(first + j, 9, stride=9), :] = s.dirs[k, j, 9 * core : 9 * core + 9]
            oute[pl.ds(first + j, 2, stride=9), :] = s.dirsE[k, j, 2 * core : 2 * core + 2]

    def ring(u, q, j0, n):
        got(s.r2.at[pl.ds(j0, n), pl.ds(1, 15), pl.ds(0, 9)], s.recva.at[u])
        place = s.w.at[(pl.ds(first + j0, n),) + cut(q, pos[q])]
        for d in (1, 3, 2):
            remote(s.v.at[pl.ds(j0, n)], place, s.sendb.at[0], s.recvq.at[u, d - 1], at(q, d))
        remote(s.v.at[pl.ds(j0, n)], place, s.sendc.at[0], s.recvc.at[u], partner)
        for j in range(j0, j0 + n):
            s.w[(first + j,) + cut(q, pos[q])] = s.v[j]

    for u in range(count):
        phase(f"ring{u}")
        ring(u, *units[u])

    phase("ring_e")
    got(s.r2E.at[pl.ds(0, count), pl.ds(1, 15), pl.ds(0, 2)], s.recva.at[E])
    v2e = s.vE.reshape(SLOTS, 64, 128)
    for j in range(count):
        s.wz[j, slab] = v2e[j]
    mixed = jnp.dot(
        jnp.concatenate([ev[TILES + 2], ev[TILES + 3]], axis=1),
        jnp.concatenate([s.wz[j] for j in range(count)], axis=1),
        preferred_element_type=F32,
    )
    for k in range(8):
        for j in range(count):
            s.ep[k, j] = mixed[2 * k : 2 * k + 2, j * 128 : j * 128 + 128]
    mine = pl.ds(first, count)
    for spot in beside:
        remote(
            s.ep.at[spot[0] * 2 + spot[3], pl.ds(0, count)], s.er.at[pos[0], mine],
            s.sendc.at[1], s.recvc.at[E], spot,
        )
    for j in range(count):
        s.er[pos[0], first + j] = s.ep[slot, j]

    phase("outs2")
    got(s.orr, s.drecv.at[0])
    got(s.orrE, s.drecv.at[1])
    for k, (out, oute) in enumerate(((o_dir, o_dire), (o_mst, o_mste))):
        for j in range(ocount):
            out[pl.ds(ofirst + j, 9, stride=9), :] = s.orr[k, j, 0:9]
            oute[pl.ds(ofirst + j, 2, stride=9), :] = s.orrE[k, j, 0:2]

    loaded(s.nxt, 7)
    w2 = s.w.reshape(TILES, 1152, 128)

    def own(u):
        phase(f"own{u}")
        q, j0, n = units[u]
        for d in (1, 3, 2):
            got(s.v.at[pl.ds(j0, n)], s.recvq.at[u, d - 1])
            quarter = s.w.at[(pl.ds(first + j0, n),) + cut(q, at(q, 4 - d)[q])]
            remote(quarter, quarter, s.sendc.at[0], s.recvc.at[u], partner)

    def theirs(u):
        phase(f"theirs{u}")
        got(s.w.at[ofirst + u], s.recvc.at[u])

    def product(tiles):
        phase(f"product{tiles[0]}")
        whole = jnp.concatenate([w2[k] for k in tiles], axis=1)
        halves = 2 if len(tiles) < 3 else 1
        for h in range(halves):
            some = slice(h * 256, h * 256 + 512 // halves)
            mixed = jnp.dot(s.nxt[some, :], whole, preferred_element_type=F32).astype(BF16)
            for i, k in enumerate(tiles):
                o_np[some, k * 128 : k * 128 + 128] = mixed[:, i * 128 : i * 128 + 128]

    def embed_out():
        phase("embed_out")
        got(s.ed.at[pl.ds(0, 3 * count + 4 * ocount)], s.recvc.at[E])
        for k in range(TILES):
            total = s.er[0, k] + s.er[1, k] + s.er[2, k] + s.er[3, k]
            o_ne[:, k * 128 : k * 128 + 128] = total.astype(BF16)

    def many(base, *tiles):
        product([base + k for k in tiles])

    own(0)
    own(1)
    if count == 5:
        many(first, 0, 1)
        theirs(0)
        theirs(1)
        many(ofirst, 0, 1)
        own(3)
        own(4)
        own(2)
        many(first, 2, 3, 4)
        embed_out()
        theirs(2)
        theirs(3)
    else:
        own(2)
        many(first, 0, 1, 2)
        theirs(0)
        theirs(1)
        many(ofirst, 0, 1)
        own(3)
        many(first, 3)
        embed_out()
        theirs(3)
        theirs(4)
        many(ofirst, 3, 4)
        theirs(2)

    phase("drain")
    sent(s.eb.at[:, pl.ds(0, 7)], s.dsend.at[2])
    sent(s.os, s.dsend.at[0])
    sent(s.osE, s.dsend.at[1])
    sent(s.ps.at[pl.ds(0, ocount)], s.psend)
    sent(s.na.at[core], s.nsend.at[0])
    sent(s.nw, s.nsend.at[1])
    sent(s.r2.at[pl.ds(0, count), pl.ds(1, 15), pl.ds(0, 9)], s.senda.at[0])
    sent(s.r2E.at[pl.ds(0, count), pl.ds(1, 15), pl.ds(0, 2)], s.senda.at[1])
    sent(s.r1.at[pl.ds(0, count), pl.ds(1, 3)], s.sendb.at[0])
    sent(s.w.at[pl.ds(first, count)], s.sendc.at[0])
    sent(s.ed.at[pl.ds(0, 7 * count)], s.sendc.at[1])
    phase(None)


class Names:
    pass


class Phase:
    def __init__(self):
        self.open = None

    def __call__(self, name):
        if self.open is not None:
            self.open.__exit__(None, None, None)
            self.open = None
        if name is not None and PHASES:
            self.open = jax.named_scope(name)
            self.open.__enter__()


DMA = pltpu.SemaphoreType.DMA
SCRATCH = dict(
    att=pltpu.VMEM((512, 1152), BF16),
    attT=pltpu.VMEM((1152, 512), BF16),
    cot=pltpu.VMEM((512, 1152), BF16),
    ecot=pltpu.VMEM((2, 1152), BF16),
    now=pltpu.SMEM((2,), F32),
    later=pltpu.SMEM((2,), F32),
    st=pltpu.VMEM((2, 3, 81, 128), F32),
    ste=pltpu.VMEM((2, 3, 18, 128), F32),
    ps=pltpu.VMEM((SLOTS, 1152, 128), BF16),
    pr=pltpu.VMEM((SLOTS, 1152, 128), BF16),
    x=pltpu.VMEM((SLOTS, 4, 4, 4, 9, 2, 128), BF16),
    r1=pltpu.VMEM((SLOTS, 4, 4, 4, 9, 2, 128), BF16),
    y=pltpu.VMEM((SLOTS, 4, 4, 9, 2, 128), BF16),
    yE=pltpu.VMEM((SLOTS, 4, 4, 2, 2, 128), BF16),
    r2=pltpu.VMEM((SLOTS, 16, 12, 2, 128), BF16),
    r2E=pltpu.VMEM((SLOTS, 16, 4, 2, 128), BF16),
    reg=pltpu.VMEM((3, SLOTS, 24, 128), F32),
    regE=pltpu.VMEM((3, SLOTS, 8, 128), F32),
    g=pltpu.VMEM((SLOTS, 24, 128), F32),
    gE=pltpu.VMEM((SLOTS, 8, 128), F32),
    dirs=pltpu.VMEM((2, SLOTS, 24, 128), F32),
    dirsE=pltpu.VMEM((2, SLOTS, 8, 128), F32),
    zz=pltpu.VMEM((SLOTS, 12, 2, 128), BF16),
    zE=pltpu.VMEM((SLOTS, 4, 2, 128), BF16),
    v=pltpu.VMEM((SLOTS, 4, 4, 9, 2, 128), BF16),
    vE=pltpu.VMEM((SLOTS, 4, 4, 2, 2, 128), BF16),
    os=pltpu.VMEM((2, SLOTS, 16, 128), F32),
    osE=pltpu.VMEM((2, SLOTS, 8, 128), F32),
    orr=pltpu.VMEM((2, SLOTS, 16, 128), F32),
    orrE=pltpu.VMEM((2, SLOTS, 8, 128), F32),
    eb=pltpu.VMEM((TILES + 4, 8, 2, 128), BF16),
    ef=pltpu.VMEM((256, 640), F32),
    wz=pltpu.VMEM((SLOTS, 256, 128), BF16),
    ep=pltpu.VMEM((8, SLOTS, 2, 128), F32),
    er=pltpu.VMEM((4, TILES, 2, 128), F32),
    ed=pltpu.VMEM((36, 2, 128), F32),
    na=pltpu.VMEM((2, 1, 128), F32),
    nb=pltpu.VMEM((4, 4, 4, 1, 128), F32),
    nw=pltpu.VMEM((63, 1, 128), F32),
    load_sem=DMA((8,)),
    dsend=DMA((3,)),
    drecv=DMA((3,)),
    psend=DMA(()),
    senda=DMA((2,)),
    sendb=DMA((2,)),
    sendc=DMA((2,)),
    recvq=DMA((5, 3)),
    recva=DMA((6,)),
    recvb=DMA((6,)),
    recvc=DMA((6,)),
    nsend=DMA((2,)),
    nrecv=DMA((2,)),
)


def kernel(*refs):
    hbm, outs, scratch = refs[:12], refs[12:21], refs[21:]
    s = Names()
    for name, ref in zip(SCRATCH, scratch, strict=True):
        setattr(s, name, ref)
    s.w, s.nxt = outs[7:]
    core = lax.axis_index("c")
    for k in (0, 1):

        @pl.when(core == k)
        def _():
            body(k, hbm, outs, s)


def write_out(*refs):
    ins, outs, (sems, late_sem, buffer) = refs[:9], refs[9:16], refs[16:]
    proj, w, nxt = ins[0], ins[7].reshape(TILES, 1152, 128), ins[8]
    small = [pltpu.make_async_copy(ins[k], outs[k], sems.at[k]) for k in range(1, 7)]
    core = lax.axis_index("c")
    for k in (0, 1):

        @pl.when(core == k)
        def _():
            low, high = LATE[k][0] * 128, (LATE[k][-1] + 1) * 128
            done = [cols for cols in (slice(0, low), slice(high, 1152)) if cols.start < cols.stop]
            copies = [
                pltpu.make_async_copy(proj.at[:, cols], outs[0].at[:, cols], sems.at[7 * i])
                for i, cols in enumerate(done)
            ] + small
            for copy in copies:
                copy.start()
            whole = jnp.concatenate([w[tile] for tile in LATE[k]], axis=1)
            for h in range(2):
                some = slice(h * 256, h * 256 + 256)
                buffer[some, 0 : high - low] = jnp.dot(
                    nxt[some, :], whole, preferred_element_type=F32
                ).astype(BF16)
            last = pltpu.make_async_copy(
                buffer.at[:, 0 : high - low], outs[0].at[:, low:high], late_sem
            )
            last.start()
            for copy in copies + [last]:
                copy.wait()


def shards(
    attended, proj_cot, timesteps, embed_cot, master_proj, moment_proj, second_proj,
    master_embed, moment_embed, squared_moment_layer, attended_next, timesteps_next,
):
    flat = [a.reshape(-1, 128) for a in (master_proj, moment_proj, second_proj)]
    flat_e = [a.reshape(-1, 128) for a in (master_embed, moment_embed, squared_moment_layer)]
    anywhere = pl.BlockSpec(memory_space=pl.ANY)
    large = pl.BlockSpec(memory_space=pltpu.HBM)
    vmem = pl.BlockSpec(memory_space=pltpu.VMEM)
    shape = jax.ShapeDtypeStruct
    results = (
        shape((512, 1152), BF16), shape((2, 1152), BF16), shape((81, 128), F32),
        shape((18, 128), F32), shape((81, 128), F32), shape((18, 128), F32), shape((1, 128), F32),
    )
    passed = (shape((TILES, 4, 4, 4, 9, 2, 128), BF16), shape((512, 1152), BF16))
    inside = pl.pallas_call(
        kernel,
        out_shape=[pltpu.VMEM(r.shape, r.dtype) for r in results + passed],
        in_specs=[large] * 12,
        out_specs=[vmem] * 9,
        scratch_shapes=list(SCRATCH.values()),
        compiler_params=pltpu.CompilerParams(
            collective_id=0, has_side_effects=True, vmem_limit_bytes=58 * 2**20
        ),
        name="step",
    )(attended, proj_cot, attended_next, *flat, *flat_e, timesteps, timesteps_next, embed_cot)
    nproj, nembed, d, de, m, mste, norm = pl.pallas_call(
        write_out,
        out_shape=results,
        in_specs=[vmem] * 9,
        out_specs=[large] * 7,
        scratch_shapes=[DMA((8,)), DMA(()), pltpu.VMEM((512, 256), BF16)],
        compiler_params=pltpu.CompilerParams(vmem_limit_bytes=8 * 2**20),
        name="write_out",
    )(*inside)
    return (
        nproj, nembed, d.reshape(-1), de.reshape(-1), m.reshape(-1), mste.reshape(-1), norm[0, 0],
    )


def solution(mesh):
    finer = Mesh(mesh.devices.reshape(4, 4, 4, 2), AXES)
    dp = P(AXES)
    wide = P(AXES, None)
    return jax.shard_map(
        shards,
        mesh=finer,
        in_specs=(wide, wide, dp, wide, dp, dp, dp, dp, dp, dp, wide, dp),
        out_specs=(wide, wide, dp, dp, dp, dp, P()),
        check_vma=False,
    )
```

```python
import functools
import math

import jax
import jax.numpy as jnp
from jax import lax
from jax.experimental import pallas as pl
from jax.experimental.pallas import tpu as pltpu
from jax.sharding import Mesh
from jax.sharding import PartitionSpec as P

AXES = ("z", "y", "x", "c")
MESH = pl.DeviceIdType.MESH
F32 = jnp.float32
BF16 = jnp.bfloat16

beta_one = 0.9
beta_two = 0.999
step_count = 1000.0
learn_rate = 0.0001
shrink_factor = 0.01
epsilon = 1e-08
max_norm = 1.0

TILES = 9
MINE = {0: (0, 5), 1: (5, 4)}
UNITS = {
    0: ((0, 0, 1), (1, 1, 1), (2, 2, 1), (0, 3, 1), (1, 4, 1)),
    1: ((0, 0, 1), (1, 1, 1), (2, 2, 1), (2, 3, 1)),
}
E = 5
AROUND = [
    (a, b, c) for a in (2, 1, 3, 0) for b in (2, 1, 3, 0) for c in (2, 1, 3, 0) if (a, b, c) != (0, 0, 0)
]
FAR = [(a, b) for a in (2, 1, 3, 0) for b in (2, 1, 3, 0) if (a, b) != (0, 0)]
EUNIT = {0: (0, 0, 5), 1: (0, 0, 4)}
SLOTS = 5
LATE = {0: (7, 8), 1: (2, 4)}
PHASES = False


def adamw_update(gradient, clip, master, moment, second):
    scaled = clip * gradient
    first_new = beta_one * moment + (1.0 - beta_one) * scaled
    second_new = beta_two * second + (1.0 - beta_two) * scaled * scaled
    first_hat = first_new / (1.0 - beta_one**step_count)
    second_hat = second_new / (1.0 - beta_two**step_count)
    direction = first_hat / (jnp.sqrt(second_hat) + epsilon)
    freshened_values = master - learn_rate * (direction + shrink_factor * master)
    return (direction, freshened_values)


def body(core, hbm, outs, sc):
    (att_h, cot_h, nxt_h, mp_h, op_h, sp_h, me_h, oe_h, se_h, tn_h, tx_h, ec_h) = hbm
    (o_np, o_ne, o_dir, o_dire, o_mst, o_mste, o_norm) = outs[:7]
    s = sc
    pos = [lax.axis_index(a) for a in AXES]
    other = 1 - core
    first, count = MINE[core]
    ofirst, ocount = MINE[other]
    units = UNITS[core]
    eunit = EUNIT[core]

    def at(axis, d):
        spot = list(pos)
        spot[axis] = lax.rem(pos[axis] + d, 4)
        return spot

    def in_plane(q, a, b):
        i, j = [k for k in range(3) if k != q]
        spot = list(pos)
        spot[i] = lax.rem(pos[i] + a, 4)
        spot[j] = lax.rem(pos[j] + b, 4)
        return spot

    def plane_of(q, spot):
        return [spot[k] for k in range(3) if k != q]

    def cut(q, p):
        index = [slice(None)] * 3
        index[q] = p
        return tuple(index)

    partner = tuple(pos[:3]) + (other,)

    def remote(src, dst, send, recv, spot):
        copy = pltpu.make_async_remote_copy(
            src_ref=src, dst_ref=dst, send_sem=send, recv_sem=recv,
            device_id=tuple(spot), device_id_type=MESH,
        )
        copy.start()

    def got(ref, sem):
        pltpu.make_async_remote_copy(
            src_ref=ref, dst_ref=ref, send_sem=sem, recv_sem=sem,
            device_id=partner, device_id_type=MESH,
        ).wait_recv()

    def sent(ref, sem):
        pltpu.make_async_remote_copy(
            src_ref=ref, dst_ref=ref, send_sem=sem, recv_sem=sem,
            device_id=partner, device_id_type=MESH,
        ).wait_send()

    phase = Phase()
    phase("start")
    def load(src, dst, k):
        pltpu.make_async_copy(src, dst, s.load_sem.at[k]).start()

    def loaded(ref, k):
        pltpu.make_async_copy(ref, ref, s.load_sem.at[k]).wait()

    load(tn_h, s.now, 0)
    load(tx_h, s.later, 1)
    load(ec_h, s.ecot, 2)
    load(att_h, s.att, 3)
    load(cot_h, s.cot, 4)

    phase("signal")
    barrier = pltpu.get_barrier_semaphore()
    around = [
        tuple(lax.rem(pos[k] + d[k], 4) for k in range(3)) + (pos[3],) for d in AROUND
    ]
    beside = [tuple(at(0, d)[:3]) + (c,) for d in range(4) for c in (core, other)][1:]
    rings = [tuple(at(q, d)) for q in range(3) for d in (2, 1, 3)]
    everyone = rings + [spot for spot in beside if spot[3] == other]
    for spot in everyone:
        pl.semaphore_signal(barrier, inc=1, device_id=spot, device_id_type=MESH)

    def paired(tiles):
        return [tiles[k : k + 2] for k in range(0, len(tiles), 2)]

    def terms(tiles):
        cols = s.cot[:, tiles[0] * 128 : (tiles[-1] + 1) * 128]
        return [
            jnp.dot(s.attT[h * 576 : h * 576 + 576, :], cols, preferred_element_type=F32)
            for h in range(2)
        ]

    phase("freqs")
    loaded(s.now, 0)
    loaded(s.later, 1)
    loaded(s.ecot, 2)
    ladder = lax.broadcasted_iota(jnp.int32, (8, 128), 1).astype(F32)
    line = lax.broadcasted_iota(jnp.int32, (8, 128), 0)
    freqs = jnp.exp(-math.log(10000.0) * ladder / 128)
    moments = jnp.where(
        line == 0, s.now[0], jnp.where(line == 1, s.now[1], jnp.where(line == 2, s.later[0], s.later[1]))
    )
    phases = (moments * 1000.0) * freqs
    waves = [jnp.cos(phases), jnp.sin(phases)]
    slot = pos[0] * 2 + core
    for k in range(TILES):
        s.eb[k, slot] = s.ecot[:, k * 128 : k * 128 + 128]
    for k in range(2):
        s.eb[TILES + k, slot] = waves[k][0:2].astype(BF16)
        s.eb[TILES + 2 + k, slot] = waves[k][2:4].astype(BF16)
    s.wz[...] = jnp.zeros(s.wz.shape, BF16)

    phase("load")
    loaded(s.att, 3)
    s.attT[...] = jnp.transpose(s.att[...], (1, 0))
    loaded(s.cot, 4)
    for k, src in enumerate((mp_h, op_h, sp_h)):
        load(src, s.st.at[core, k], 5)
    for k, src in enumerate((me_h, oe_h, se_h)):
        load(src, s.ste.at[core, k], 6)
    load(nxt_h, s.nxt, 7)

    for k, tiles in enumerate(paired(list(range(ofirst, ofirst + ocount)))):
        phase(f"partner_terms{k}")
        parts = terms(tiles)
        for i, t in enumerate(tiles):
            for h in range(2):
                s.ps[t - ofirst, h * 576 : h * 576 + 576] = parts[h][:, i * 128 : i * 128 + 128].astype(BF16)
        if k == 0:
            phase("barrier")
            pl.semaphore_wait(barrier, len(everyone))
            for spot in beside:
                remote(s.eb.at[:, slot], s.eb.at[:, slot], s.dsend.at[2], s.drecv.at[2], spot)
        for t in tiles:
            remote(s.ps.at[t - ofirst], s.pr.at[t - ofirst], s.psend, s.recvc.at[t - ofirst], partner)
    for k, src in enumerate((mp_h, op_h, sp_h)):
        remote(src, s.st.at[core, k], s.dsend.at[0], s.drecv.at[0], partner)
    for k, src in enumerate((me_h, oe_h, se_h)):
        remote(src, s.ste.at[core, k], s.dsend.at[1], s.drecv.at[1], partner)

    x2 = s.x.reshape(SLOTS, 1152, 128)

    def stage_one(u, x, r1, q, j0, n):
        for d in (1, 3, 2):
            spot = at(q, d)
            remote(
                x.at[(pl.ds(j0, n),) + cut(q, spot[q])],
                r1.at[pl.ds(j0, n), d],
                s.senda, s.recva.at[u], spot,
            )

    def keep_one(x, r1, q, j0, n):
        for j in range(j0, j0 + n):
            r1[j, 0] = x[(j,) + cut(q, pos[q])]

    groups = paired(list(range(first, first + count)))
    parts = {0: terms(groups[0])}
    for g, tiles in enumerate(groups):
        phase(f"own_terms{g}")
        for t in tiles:
            got(s.pr.at[t - first], s.recvc.at[t - first])
        if g + 1 < len(groups):
            parts[g + 1] = terms(groups[g + 1])
        for i, t in enumerate(tiles):
            j = t - first
            for h in range(2):
                part = parts[g][h][:, i * 128 : i * 128 + 128]
                x2[j, h * 576 : h * 576 + 576] = (part + s.pr[j, h * 576 : h * 576 + 576].astype(F32)).astype(BF16)
        for t in tiles:
            stage_one(t - first, s.x, s.r1, *units[t - first])

    phase("keep")
    for unit in units:
        keep_one(s.x, s.r1, *unit)

    phase("embed")
    ev = s.eb.reshape(TILES + 4, 16, 128)
    y2e = s.yE.reshape(SLOTS, 64, 128)
    got(s.eb.at[:, pl.ds(0, 7)], s.drecv.at[2])
    s.ef[:, 0 : count * 128] = lax.dot_general(
        jnp.concatenate([ev[TILES], ev[TILES + 1]], axis=1),
        jnp.concatenate([ev[first + j] for j in range(count)], axis=1),
        (((0,), (0,)), ((), ())), preferred_element_type=F32,
    )
    slab = pl.ds(pl.multiple_of(pos[0] * 64, 64), 64)
    for j in range(count):
        y2e[j] = s.ef[slab, j * 128 : j * 128 + 128].astype(BF16)

    phase("state")
    loaded(s.st.at[core], 5)
    loaded(s.ste.at[core], 6)
    got(s.st.at[other], s.drecv.at[0])
    got(s.ste.at[other], s.drecv.at[1])
    for k in range(3):
        for j in range(count):
            t = first + j
            for half in range(2):
                s.reg[k, j, 9 * half : 9 * half + 9] = s.st[half, k, pl.ds(t, 9, stride=9), :]
                s.regE[k, j, 2 * half : 2 * half + 2] = s.ste[half, k, pl.ds(t, 2, stride=9), :]

    r1v = s.r1.reshape(SLOTS, 4, 288, 128)
    y2 = s.y.reshape(SLOTS, 288, 128)

    def ring_sum(u, q, j0, n):
        got(s.r1.at[pl.ds(j0, n), pl.ds(1, 3)], s.recva.at[u])
        for j in range(j0, j0 + n):
            total = r1v[j, 0].astype(F32)
            for d in (1, 2, 3):
                total = total + r1v[j, d].astype(F32)
            y2[j] = total.astype(BF16)

    def stage_two(u, y, r2, words, q, j0, n):
        for a, b in FAR:
            spot = in_plane(q, a, b)
            p1, p2 = plane_of(q, spot)
            remote(
                y.at[pl.ds(j0, n), p1, p2],
                r2.at[pl.ds(j0, n), a * 4 + b, pl.ds(0, words)],
                s.sende if u == E else s.sendb, s.recva.at[E] if u == E else s.recvb.at[u], spot,
            )
        p1, p2 = plane_of(q, pos)
        for j in range(j0, j0 + n):
            r2[j, 0, 0:words] = y[j, p1, p2]

    for u, unit in enumerate(units):
        phase(f"two{u}")
        ring_sum(u, *unit)
        if u == 1:
            stage_two(0, s.y, s.r2, 9, *units[0])
        if u > 0:
            stage_two(u, s.y, s.r2, 9, *unit)
        if u == 1:
            stage_two(E, s.yE, s.r2E, 2, *eunit)

    r2v = s.r2.reshape(SLOTS, 16, 24, 128)
    r2ve = s.r2E.reshape(SLOTS, 16, 8, 128)
    squares = jnp.zeros((24, 128), F32)
    squares_e = jnp.zeros((8, 128), F32)
    phase("sum_e")
    q, j0, n = eunit
    got(s.r2E.at[pl.ds(j0, n), pl.ds(1, 15), pl.ds(0, 2)], s.recva.at[E])
    for j in range(j0, j0 + n):
        total = r2ve[j, 0].astype(F32)
        for k in range(1, 16):
            total = total + r2ve[j, k].astype(F32)
        s.gE[j] = total
        squares_e = squares_e + total * total

    for u, (q, j0, n) in enumerate(units):
        phase(f"sum{u}")
        got(s.r2.at[pl.ds(j0, n), pl.ds(1, 15), pl.ds(0, 9)], s.recvb.at[u])
        for j in range(j0, j0 + n):
            total = r2v[j, 0].astype(F32)
            for k in range(1, 16):
                total = total + r2v[j, k].astype(F32)
            s.g[j] = total
            squares = squares + total * total
    phase("squares")
    rows = lax.broadcasted_iota(jnp.int32, (24, 128), 0)
    rows_e = lax.broadcasted_iota(jnp.int32, (8, 128), 0)
    squares = jnp.sum(jnp.where(rows < 18, squares, 0.0), axis=0, keepdims=True)
    squares = squares + jnp.sum(jnp.where(rows_e < 4, squares_e, 0.0), axis=0, keepdims=True)
    s.na[core] = squares
    remote(s.na.at[core], s.na.at[core], s.nsend.at[0], s.nrecv.at[0], partner)
    phase("norm_a")
    got(s.na.at[other], s.nrecv.at[0])
    pz, py, px = pos[:3]
    mine = s.nb.at[pz, py, px]
    s.nb[pz, py, px] = s.na[0] + s.na[1]
    for spot in around:
        remote(mine, mine, s.nsend.at[1], s.nrecv.at[1], spot)
    sent(s.st.at[core], s.dsend.at[0])
    sent(s.ste.at[core], s.dsend.at[1])
    sent(s.r1.at[pl.ds(0, count), pl.ds(1, 3)], s.senda)
    sent(s.r2.at[pl.ds(0, count), pl.ds(1, 15), pl.ds(0, 9)], s.sendb)
    sent(s.r2E.at[pl.ds(0, count), pl.ds(1, 15), pl.ds(0, 2)], s.sende)
    sent(s.eb.at[:, pl.ds(0, 7)], s.dsend.at[2])
    phase("norm_b")
    got(s.nw, s.nrecv.at[1])
    level = [s.nb[k // 16, k // 4 % 4, k % 4] for k in range(64)]
    while len(level) > 1:
        level = [a + b for a, b in zip(level[::2], level[1::2])]
    total = level[0]
    grad_norm = jnp.sqrt(jnp.sum(total, axis=1, keepdims=True))
    clip = jnp.minimum(jnp.float32(1.0), max_norm / (grad_norm + 1e-06))
    o_norm[...] = jnp.broadcast_to(grad_norm, (1, 128))

    z2 = s.zz.reshape(SLOTS, 24, 128)
    z2e = s.zE.reshape(SLOTS, 8, 128)

    def update(u, g, reg, zz, z2, dirs, v, words, q, j0, n):
        for j in range(j0, j0 + n):
            direction, fresh = adamw_update(g[j], clip, reg[0, j], reg[1, j], reg[2, j])
            dirs[0, j] = direction
            dirs[1, j] = fresh
            z2[j] = fresh.astype(BF16)
        p1, p2 = plane_of(q, pos)
        for a, b in FAR:
            remote(
                zz.at[pl.ds(j0, n), pl.ds(0, words)],
                v.at[pl.ds(j0, n), p1, p2],
                s.sende if u == E else s.senda, s.recva.at[u], in_plane(q, a, b),
            )
        for j in range(j0, j0 + n):
            v[j, p1, p2] = zz[j, 0:words]

    order = list(range(count)) + [E]
    phase("update")
    for u in order:
        if u == E:
            update(E, s.gE, s.regE, s.zE, z2e, s.dirsE, s.vE, 2, *eunit)
        else:
            update(u, s.g, s.reg, s.zz, z2, s.dirs, s.v, 9, *units[u])

    phase("outs")
    for k in range(2):
        for j in range(count):
            s.os[k, j, 0:9] = s.dirs[k, j, 9 * other : 9 * other + 9]
            s.osE[k, j, 0:2] = s.dirsE[k, j, 2 * other : 2 * other + 2]
    remote(s.os, s.orr, s.dsend.at[0], s.drecv.at[0], partner)
    remote(s.osE, s.orrE, s.dsend.at[1], s.drecv.at[1], partner)
    for k, (out, oute) in enumerate(((o_dir, o_dire), (o_mst, o_mste))):
        for j in range(count):
            out[pl.ds(first + j, 9, stride=9), :] = s.dirs[k, j, 9 * core : 9 * core + 9]
            oute[pl.ds(first + j, 2, stride=9), :] = s.dirsE[k, j, 2 * core : 2 * core + 2]

    def ring(u, q, j0, n):
        got(s.r2.at[pl.ds(j0, n), pl.ds(1, 15), pl.ds(0, 9)], s.recva.at[u])
        place = s.w.at[(pl.ds(first + j0, n),) + cut(q, pos[q])]
        for d in (1, 3, 2):
            remote(s.v.at[pl.ds(j0, n)], place, s.sendb, s.recvq.at[u, int(d == 2)], at(q, d))
        remote(s.v.at[pl.ds(j0, n)], place, s.sendc, s.recvc.at[u], partner)
        for j in range(j0, j0 + n):
            s.w[(first + j,) + cut(q, pos[q])] = s.v[j]

    for u in range(count):
        phase(f"ring{u}")
        ring(u, *units[u])

    phase("ring_e")
    got(s.r2E.at[pl.ds(0, count), pl.ds(1, 15), pl.ds(0, 2)], s.recva.at[E])
    v2e = s.vE.reshape(SLOTS, 64, 128)
    for j in range(count):
        s.wz[j, slab] = v2e[j]
    mixed = jnp.dot(
        jnp.concatenate([ev[TILES + 2], ev[TILES + 3]], axis=1),
        jnp.concatenate([s.wz[j] for j in range(count)], axis=1),
        preferred_element_type=F32,
    )
    for k in range(8):
        for j in range(count):
            s.ep[k, j] = mixed[2 * k : 2 * k + 2, j * 128 : j * 128 + 128]
    mine = pl.ds(first, count)
    for spot in beside:
        remote(
            s.ep.at[spot[0] * 2 + spot[3], pl.ds(0, count)], s.er.at[pos[0], mine],
            s.dsend.at[2], s.drecv.at[2], spot,
        )
    for j in range(count):
        s.er[pos[0], first + j] = s.ep[slot, j]

    phase("outs2")
    got(s.orr, s.drecv.at[0])
    got(s.orrE, s.drecv.at[1])
    for k, (out, oute) in enumerate(((o_dir, o_dire), (o_mst, o_mste))):
        for j in range(ocount):
            out[pl.ds(ofirst + j, 9, stride=9), :] = s.orr[k, j, 0:9]
            oute[pl.ds(ofirst + j, 2, stride=9), :] = s.orrE[k, j, 0:2]

    loaded(s.nxt, 7)
    w2 = s.w.reshape(TILES, 1152, 128)

    def own(u):
        phase(f"own{u}")
        q, j0, n = units[u]
        for k, ds in enumerate(((1, 3), (2,))):
            got(s.r1.at[pl.ds(j0, n), pl.ds(1, len(ds))], s.recvq.at[u, k])
            for d in ds:
                quarter = s.w.at[(pl.ds(first + j0, n),) + cut(q, at(q, 4 - d)[q])]
                remote(quarter, quarter, s.sendc, s.recvc.at[u], partner)

    def theirs(u):
        phase(f"theirs{u}")
        got(s.w.at[ofirst + u], s.recvc.at[u])

    def product(tiles):
        phase(f"product{tiles[0]}")
        whole = jnp.concatenate([w2[k] for k in tiles], axis=1)
        halves = 2 if len(tiles) < 3 else 1
        for h in range(halves):
            some = slice(h * 256, h * 256 + 512 // halves)
            mixed = jnp.dot(s.nxt[some, :], whole, preferred_element_type=F32).astype(BF16)
            for i, k in enumerate(tiles):
                o_np[some, k * 128 : k * 128 + 128] = mixed[:, i * 128 : i * 128 + 128]

    def embed_out():
        phase("embed_out")
        got(s.ed.at[pl.ds(0, 3 * count + 4 * ocount)], s.drecv.at[2])
        for k in range(TILES):
            total = s.er[0, k] + s.er[1, k] + s.er[2, k] + s.er[3, k]
            o_ne[:, k * 128 : k * 128 + 128] = total.astype(BF16)

    def many(base, *tiles):
        product([base + k for k in tiles])

    own(0)
    own(1)
    if count == 5:
        many(first, 0, 1)
        theirs(0)
        theirs(1)
        many(ofirst, 0, 1)
        own(3)
        own(4)
        own(2)
        many(first, 2, 3, 4)
        embed_out()
        theirs(2)
        theirs(3)
    else:
        own(2)
        many(first, 0, 1, 2)
        theirs(0)
        theirs(1)
        many(ofirst, 0, 1)
        own(3)
        many(first, 3)
        embed_out()
        theirs(3)
        many(ofirst, 3)
        theirs(4)
        theirs(2)

    phase("drain")
    sent(s.os, s.dsend.at[0])
    sent(s.osE, s.dsend.at[1])
    sent(s.ps.at[pl.ds(0, ocount)], s.psend)
    sent(s.na.at[core], s.nsend.at[0])
    sent(s.nw, s.nsend.at[1])
    sent(s.r2.at[pl.ds(0, count), pl.ds(1, 15), pl.ds(0, 9)], s.senda)
    sent(s.r2E.at[pl.ds(0, count), pl.ds(1, 15), pl.ds(0, 2)], s.sende)
    sent(s.r1.at[pl.ds(0, count), pl.ds(1, 3)], s.sendb)
    sent(s.w.at[pl.ds(first, count)], s.sendc)
    sent(s.ed.at[pl.ds(0, 7 * count)], s.dsend.at[2])
    phase(None)


class Names:
    pass


class Phase:
    def __init__(self):
        self.open = None

    def __call__(self, name):
        if self.open is not None:
            self.open.__exit__(None, None, None)
            self.open = None
        if name is not None and PHASES:
            self.open = jax.named_scope(name)
            self.open.__enter__()


DMA = pltpu.SemaphoreType.DMA
SCRATCH = dict(
    att=pltpu.VMEM((512, 1152), BF16),
    attT=pltpu.VMEM((1152, 512), BF16),
    cot=pltpu.VMEM((512, 1152), BF16),
    ecot=pltpu.VMEM((2, 1152), BF16),
    now=pltpu.SMEM((2,), F32),
    later=pltpu.SMEM((2,), F32),
    st=pltpu.VMEM((2, 3, 81, 128), F32),
    ste=pltpu.VMEM((2, 3, 18, 128), F32),
    ps=pltpu.VMEM((SLOTS, 1152, 128), BF16),
    pr=pltpu.VMEM((SLOTS, 1152, 128), BF16),
    x=pltpu.VMEM((SLOTS, 4, 4, 4, 9, 2, 128), BF16),
    r1=pltpu.VMEM((SLOTS, 4, 4, 4, 9, 2, 128), BF16),
    y=pltpu.VMEM((SLOTS, 4, 4, 9, 2, 128), BF16),
    yE=pltpu.VMEM((SLOTS, 4, 4, 2, 2, 128), BF16),
    r2=pltpu.VMEM((SLOTS, 16, 12, 2, 128), BF16),
    r2E=pltpu.VMEM((SLOTS, 16, 4, 2, 128), BF16),
    reg=pltpu.VMEM((3, SLOTS, 24, 128), F32),
    regE=pltpu.VMEM((3, SLOTS, 8, 128), F32),
    g=pltpu.VMEM((SLOTS, 24, 128), F32),
    gE=pltpu.VMEM((SLOTS, 8, 128), F32),
    dirs=pltpu.VMEM((2, SLOTS, 24, 128), F32),
    dirsE=pltpu.VMEM((2, SLOTS, 8, 128), F32),
    zz=pltpu.VMEM((SLOTS, 12, 2, 128), BF16),
    zE=pltpu.VMEM((SLOTS, 4, 2, 128), BF16),
    v=pltpu.VMEM((SLOTS, 4, 4, 9, 2, 128), BF16),
    vE=pltpu.VMEM((SLOTS, 4, 4, 2, 2, 128), BF16),
    os=pltpu.VMEM((2, SLOTS, 16, 128), F32),
    osE=pltpu.VMEM((2, SLOTS, 8, 128), F32),
    orr=pltpu.VMEM((2, SLOTS, 16, 128), F32),
    orrE=pltpu.VMEM((2, SLOTS, 8, 128), F32),
    eb=pltpu.VMEM((TILES + 4, 8, 2, 128), BF16),
    ef=pltpu.VMEM((256, 640), F32),
    wz=pltpu.VMEM((SLOTS, 256, 128), BF16),
    ep=pltpu.VMEM((8, SLOTS, 2, 128), F32),
    er=pltpu.VMEM((4, TILES, 2, 128), F32),
    ed=pltpu.VMEM((36, 2, 128), F32),
    na=pltpu.VMEM((2, 1, 128), F32),
    nb=pltpu.VMEM((4, 4, 4, 1, 128), F32),
    nw=pltpu.VMEM((63, 1, 128), F32),
    load_sem=DMA((8,)),
    dsend=DMA((3,)),
    drecv=DMA((3,)),
    psend=DMA(()),
    senda=DMA(()),
    sendb=DMA(()),
    sendc=DMA(()),
    sende=DMA(()),
    recvq=DMA((5, 2)),
    recva=DMA((6,)),
    recvb=DMA((5,)),
    recvc=DMA((5,)),
    nsend=DMA((2,)),
    nrecv=DMA((2,)),
)


def kernel(*refs):
    hbm, outs, scratch = refs[:12], refs[12:21], refs[21:]
    s = Names()
    for name, ref in zip(SCRATCH, scratch, strict=True):
        setattr(s, name, ref)
    s.w, s.nxt = outs[7:]
    core = lax.axis_index("c")
    for k in (0, 1):

        @pl.when(core == k)
        def _():
            body(k, hbm, outs, s)


def write_out(*refs):
    ins, outs, (sems, buffer) = refs[:9], refs[9:16], refs[16:]
    proj, w, nxt = ins[0], ins[7].reshape(TILES, 1152, 128), ins[8]
    small = [pltpu.make_async_copy(ins[k], outs[k], sems.at[k - 1]) for k in range(1, 7)]
    core = lax.axis_index("c")
    for k in (0, 1):

        @pl.when(core == k)
        def _():
            late = LATE[k]
            starts = [0] + [(tile + 1) * 128 for tile in late]
            ends = [tile * 128 for tile in late] + [1152]
            done = [slice(a, b) for a, b in zip(starts, ends) if a < b]
            copies = [
                pltpu.make_async_copy(proj.at[:, cols], outs[0].at[:, cols], sems.at[6 + i])
                for i, cols in enumerate(done)
            ] + small
            for copy in copies:
                copy.start()
            whole = jnp.concatenate([w[tile] for tile in late], axis=1)
            for h in range(2):
                some = slice(h * 256, h * 256 + 256)
                buffer[some, :] = jnp.dot(nxt[some, :], whole, preferred_element_type=F32).astype(BF16)
            for i, tile in enumerate(late):
                last = pltpu.make_async_copy(
                    buffer.at[:, i * 128 : i * 128 + 128],
                    outs[0].at[:, tile * 128 : tile * 128 + 128],
                    sems.at[9 + i],
                )
                last.start()
                copies.append(last)
            for copy in copies:
                copy.wait()


def shards(
    attended, proj_cot, timesteps, embed_cot, master_proj, moment_proj, second_proj,
    master_embed, moment_embed, squared_moment_layer, attended_next, timesteps_next,
):
    flat = [a.reshape(-1, 128) for a in (master_proj, moment_proj, second_proj)]
    flat_e = [a.reshape(-1, 128) for a in (master_embed, moment_embed, squared_moment_layer)]
    anywhere = pl.BlockSpec(memory_space=pl.ANY)
    large = pl.BlockSpec(memory_space=pltpu.HBM)
    vmem = pl.BlockSpec(memory_space=pltpu.VMEM)
    shape = jax.ShapeDtypeStruct
    results = (
        shape((512, 1152), BF16), shape((2, 1152), BF16), shape((81, 128), F32),
        shape((18, 128), F32), shape((81, 128), F32), shape((18, 128), F32), shape((1, 128), F32),
    )
    passed = (shape((TILES, 4, 4, 4, 9, 2, 128), BF16), shape((512, 1152), BF16))
    inside = pl.pallas_call(
        kernel,
        out_shape=[pltpu.VMEM(r.shape, r.dtype) for r in results + passed],
        in_specs=[large] * 12,
        out_specs=[vmem] * 9,
        scratch_shapes=list(SCRATCH.values()),
        compiler_params=pltpu.CompilerParams(
            collective_id=0, has_side_effects=True, vmem_limit_bytes=58 * 2**20
        ),
        name="step",
    )(attended, proj_cot, attended_next, *flat, *flat_e, timesteps, timesteps_next, embed_cot)
    nproj, nembed, d, de, m, mste, norm = pl.pallas_call(
        write_out,
        out_shape=results,
        in_specs=[vmem] * 9,
        out_specs=[large] * 7,
        scratch_shapes=[DMA((11,)), pltpu.VMEM((512, 256), BF16)],
        compiler_params=pltpu.CompilerParams(vmem_limit_bytes=8 * 2**20),
        name="write_out",
    )(*inside)
    return (
        nproj, nembed, d.reshape(-1), de.reshape(-1), m.reshape(-1), mste.reshape(-1), norm[0, 0],
    )


def solution(mesh):
    finer = Mesh(mesh.devices.reshape(4, 4, 4, 2), AXES)
    dp = P(AXES)
    wide = P(AXES, None)
    return jax.shard_map(
        shards,
        mesh=finer,
        in_specs=(wide, wide, dp, wide, dp, dp, dp, dp, dp, dp, wide, dp),
        out_specs=(wide, wide, dp, dp, dp, dp, P()),
        check_vma=False,
    )
```
